32 devices in a mesh: img: 2 (over x), rows: 16 (over z, y, core).
Axes of the slice: x: 2, y: 2, z: 4, core: 2. Of those that a mesh axis runs over, the one named last changes fastest.
Arguments:
- hidden_states: bfloat16 [3, 4096, 1024], P(None, ('img', 'rows')), parts along dimension 1, may hold values from -6 to 6
- cell_of: int32 [2048], replicated, may hold values from 0 to 2047, as said below
- proj_four_weight: bfloat16 [1024, 256], replicated, may hold values from -0.1875 to 0.1875
- proj_four_bias: float32 [256], replicated, may hold values from -3 to 3
- proj_two_weight: bfloat16 [1024, 512], replicated, may hold values from -0.1875 to 0.1875
- proj_two_bias: float32 [512], replicated, may hold values from -3 to 3
- proj_same_weight: bfloat16 [1024, 1024], replicated, may hold values from -0.1875 to 0.1875
- proj_same_bias: float32 [1024], replicated, may hold values from -3 to 3
- up4_weight: bfloat16 [256, 4096], replicated, may hold values from -0.375 to 0.375
- up4_bias: float32 [256], replicated, may hold values from -3 to 3
- up2_weight: bfloat16 [512, 2048], replicated, may hold values from -0.25 to 0.25
- up2_bias: float32 [512], replicated, may hold values from -3 to 3
- join_weight: bfloat16 [3, 3, 256, 256], replicated, may hold values from -0.125 to 0.125
Outputs:
- joined_four: bfloat16 [256, 256, 256], P(('img', 'rows')), parts along dimension 0
- upsampled_two: bfloat16 [128, 128, 512], P(('img', 'rows')), parts along dimension 0
- same_scale: bfloat16 [64, 64, 1024], P(('img', 'rows')), parts along dimension 0
The draws below stay inside these ranges and needn't reach their ends.
There are 2 independent parts, one for each index of `img`. The reference program is written for one: setup_inputs(seed, part) draws one part's arguments, and reference() takes and returns one part's arrays. A program takes and returns all parts, laid end to end along the dimension named above; an argument that names none is the same for every part. Nothing has to cross between parts.
Inputs may be any that keep to these rules, and one draw needn't show every extreme that they name: `cell_of`: a permutation of the cells 0 to 2047; the sequence positions k * 128 to (k + 1) * 128 - 1 hold exactly 8 cells of every block of 128 consecutive cells.
All inputs are finite; a program needn't handle non-finite values.
Results may differ from the reference program's by a relative error of at most 0.0057.
Values may be sent and summed in bfloat16 or wider, within the bound.
No kernel may reach another device: no remote copies, remote signals or barrier semaphores. Data moves between devices by JAX's collectives and lax.ppermute only.
A program may use at most 64 MiB of HBM per device.

```python
import jax
import jax.numpy as jnp

HOOKS = 3
HID = 1024
C_FOUR = 256
C_TWO = 512
C_SAME = 1024
FEAT = 256
GRID_W = 64
TOK_DEV = 128
GRID_H = 32
TOKENS = 2048


def draw_cell_of(key, part):
    tile_count = TOKENS // TOK_DEV
    per_tile = TOK_DEV // tile_count
    first_key, second_key = jax.random.split(jax.random.fold_in(key, 11))
    base_cells = jnp.arange(TOKENS, dtype=jnp.int32).reshape(tile_count, TOK_DEV)
    shuffled = jax.random.permutation(first_key, base_cells, axis=1, independent=True)
    dealt = shuffled.reshape(tile_count, tile_count, per_tile).transpose(1, 0, 2).reshape(tile_count, TOK_DEV)
    return jax.random.permutation(second_key, dealt, axis=1, independent=True).reshape(TOKENS)


def levels(own_key, dims, cuts, smallest, largest):
    def one(position, blocks):
        steps = jax.random.uniform(jax.random.fold_in(jax.random.fold_in(own_key, 6), position), (blocks,), jnp.float32, smallest / len(cuts), largest / len(cuts))
        return jnp.repeat(jnp.exp(steps), dims[position] // blocks).reshape((-1,) + (1,) * (len(dims) - position - 1))

    loudness = one(*cuts[0])
    for cut in cuts[1:]:
        loudness = loudness * one(*cut)
    return loudness


def bell_draw(own_key, shape, spread, most, cuts=(), kind=jnp.bfloat16):
    values = spread * jax.random.normal(own_key, shape, jnp.float32)
    if cuts:
        values = values * levels(own_key, shape, cuts, -0.22, 0.18)
    return jnp.clip(values, -most, most).astype(kind)


def setup_inputs(seed: int = 0, part: int = 0) -> dict:
    splits = jax.random.split(jax.random.key(seed), 14)
    part_keys = jax.random.split(jax.random.fold_in(splits[13], part), 14)
    return {
        "hidden_states": bell_draw(part_keys[0], (HOOKS, TOKENS, HID), 1.0, 6.0, ((1, 16),)),
        "cell_of": draw_cell_of(jax.random.fold_in(splits[13], 71), part),
        "proj_four_weight": bell_draw(splits[2], (HID, C_FOUR), HID ** -0.5, 0.1875),
        "proj_four_bias": bell_draw(splits[3], (C_FOUR,), 0.5, 3.0, (), jnp.float32),
        "proj_two_weight": bell_draw(splits[4], (HID, C_TWO), HID ** -0.5, 0.1875),
        "proj_two_bias": bell_draw(splits[5], (C_TWO,), 0.5, 3.0, (), jnp.float32),
        "proj_same_weight": bell_draw(splits[6], (HID, C_SAME), HID ** -0.5, 0.1875),
        "proj_same_bias": bell_draw(splits[7], (C_SAME,), 0.5, 3.0, (), jnp.float32),
        "up4_weight": bell_draw(splits[8], (C_FOUR, 16 * C_FOUR), C_FOUR ** -0.5, 0.375),
        "up4_bias": bell_draw(splits[9], (C_FOUR,), 0.5, 3.0, (), jnp.float32),
        "up2_weight": bell_draw(splits[10], (C_TWO, 4 * C_TWO), C_TWO ** -0.5, 0.25),
        "up2_bias": bell_draw(splits[11], (C_TWO,), 0.5, 3.0, (), jnp.float32),
        "join_weight": bell_draw(splits[12], (3, 3, C_FOUR, FEAT), (9 * C_FOUR) ** -0.5, 0.125),
    }


def expand(proj, weight, bias_row, factor):
    height, columns, channels = proj.shape
    out_channels = weight.shape[1] // (factor * factor)
    flattened = jnp.dot(proj.reshape(-1, channels), weight, preferred_element_type=jnp.float32)
    flattened = flattened + jnp.tile(bias_row, factor * factor)[None, :]
    result = flattened.astype(jnp.bfloat16).reshape(height, columns, factor, factor, out_channels)
    return result.transpose(0, 2, 1, 3, 4).reshape(height * factor, columns * factor, out_channels)


def convolve(padded, weight, out_rows, out_cols):
    channels = padded.shape[2]
    total = jnp.zeros((out_rows, out_cols, weight.shape[3]), jnp.float32)
    for row_tap in range(3):
        for col_tap in range(3):
            window = padded[row_tap:row_tap + out_rows, col_tap:col_tap + out_cols]
            term = jnp.dot(window.reshape(-1, channels), weight[row_tap, col_tap], preferred_element_type=jnp.float32)
            total = total + term.reshape(out_rows, out_cols, -1)
    return total.astype(jnp.bfloat16)


def reference(hidden_states, cell_of, proj_four_weight, proj_four_bias, proj_two_weight, proj_two_bias, proj_same_weight, proj_same_bias, up4_weight, up4_bias, up2_weight, up2_bias, join_weight):
    grid_tokens = jnp.zeros(hidden_states.shape, jnp.bfloat16).at[:, cell_of, :].set(hidden_states)
    pairs = ((proj_four_weight, proj_four_bias), (proj_two_weight, proj_two_bias), (proj_same_weight, proj_same_bias))
    maps = []
    for hook in range(HOOKS):
        projected = jnp.dot(grid_tokens[hook], pairs[hook][0], preferred_element_type=jnp.float32) + pairs[hook][1]
        maps.append(projected.astype(jnp.bfloat16).reshape(GRID_H, GRID_W, -1))
    upsampled_four = expand(maps[0], up4_weight, up4_bias, 4)
    padded = jnp.pad(upsampled_four, ((1, 1), (1, 1), (0, 0)))
    joined_four = convolve(padded, join_weight, 4 * GRID_H, 4 * GRID_W)
    upsampled_two = expand(maps[1], up2_weight, up2_bias, 2)
    same_scale = maps[2]
    return (joined_four, upsampled_two, same_scale)
```

```python
import functools

import jax
import jax.numpy as jnp
from jax import lax
from jax.experimental import pallas as pl
from jax.experimental.pallas import tpu as pltpu
from jax.sharding import PartitionSpec as P

GRID_W = 64
F32 = jnp.float32
BF16 = jnp.bfloat16
ANY = pl.BlockSpec(memory_space=pl.ANY)
VMEM = pl.BlockSpec(memory_space=pltpu.VMEM)


def in_hbm(x):
    return pltpu.with_memory_space_constraint(x, pltpu.HBM)


def one_hot(mask):
    return jnp.where(mask, 1.0, 0.0).astype(BF16)


def iota(shape, dim):
    return lax.broadcasted_iota(jnp.int32, shape, dim)


def matmul(left, right):
    return jnp.dot(left, right, preferred_element_type=F32)


def column(row, size):
    same = iota((size, size), 0) == iota((size, size), 1)
    return jnp.sum(jnp.where(same, jnp.broadcast_to(row, (size, size)), 0.0), axis=1, keepdims=True)


def landing(table, block, tok_dev, per_peer):
    shards = table.shape[0]
    start = block * tok_dev
    inside = jnp.logical_and(table >= start, table < start + tok_dev)
    before = one_hot(iota((tok_dev, tok_dev), 0) < iota((tok_dev, tok_dev), 1))
    rank = matmul(one_hot(inside), before)
    place = (table - start).astype(F32)
    lane = iota((shards, tok_dev), 1)
    spread = jnp.zeros((shards, tok_dev), F32)
    for k in range(per_peer):
        hit = jnp.logical_and(inside, rank == float(k))
        found = jnp.sum(jnp.where(hit, place, 0.0), axis=1, keepdims=True)
        spread = spread + jnp.where(lax.rem(lane, per_peer) == k, found, 0.0)
    own = lax.div(lane, per_peer) == iota((shards, tok_dev), 0)
    return jnp.sum(jnp.where(own, spread, 0.0), axis=0, keepdims=True).astype(jnp.int32)


def project_kernel(
    hidden, table_hbm, w4, b4, w2, b2, ws, bs, four_v, rest_v, places_v,
    hidden_v, table_v, w4_v, w2_v, ws_v, b4_v, b2_v, bs_v, sems,
):
    copies = [
        pltpu.make_async_copy(src, dst, sems.at[i])
        for i, (src, dst) in enumerate(
            (
                (table_hbm, table_v),
                (hidden.at[0], hidden_v.at[0]),
                (b4, b4_v),
                (w4, w4_v),
                (hidden.at[1], hidden_v.at[1]),
                (b2, b2_v),
                (w2, w2_v),
                (hidden.at[2], hidden_v.at[2]),
                (bs, bs_v),
                (ws, ws_v),
            )
        )
    ]
    for copy in copies:
        copy.start()
    shards, tok_dev = table_v.shape
    per_peer = tok_dev // shards
    me = lax.axis_index("rows")
    copies[0].wait()
    table = table_v[...]
    mine = table_v[pl.ds(me, 1), :]
    block_row = lax.div(mine, tok_dev)
    block_col = column(block_row.astype(F32), tok_dev).astype(jnp.int32)
    square = (tok_dev, tok_dev)
    earlier = jnp.logical_and(block_col == jnp.broadcast_to(block_row, square), iota(square, 0) < iota(square, 1))
    within = jnp.sum(jnp.where(earlier, 1.0, 0.0), axis=0, keepdims=True).astype(jnp.int32)
    slot = block_row * per_peer + within
    order = one_hot(iota(square, 0) == slot)
    order_above = one_hot(iota(square, 0) == slot + per_peer)
    order_below = one_hot(iota(square, 0) == slot - per_peer)

    own = landing(table, me, tok_dev, per_peer)
    above = landing(table, me - 1, tok_dev, per_peer)
    below = landing(table, me + 1, tok_dev, per_peer)
    cell = iota(square, 0)
    col = lax.rem(cell, GRID_W)
    edge = (GRID_W, tok_dev)
    edge_col = iota(edge, 0)
    last = edge_col + (tok_dev - GRID_W)
    places_v[0:tok_dev] = one_hot(cell == own)
    places_v[tok_dev : 2 * tok_dev] = one_hot(jnp.logical_and(cell == own + 1, col != 0))
    places_v[2 * tok_dev : 3 * tok_dev] = one_hot(jnp.logical_and(cell == own - 1, col != GRID_W - 1))
    base = 3 * tok_dev
    for source, target in ((above, last), (below, edge_col)):
        places_v[base : base + GRID_W] = one_hot(target == source)
        places_v[base + GRID_W : base + 2 * GRID_W] = one_hot(jnp.logical_and(target == source + 1, edge_col != 0))
        places_v[base + 2 * GRID_W : base + 3 * GRID_W] = one_hot(
            jnp.logical_and(target == source - 1, edge_col != GRID_W - 1)
        )
        base += 3 * GRID_W

    for copy in copies[1:4]:
        copy.wait()
    c4 = w4_v.shape[1]
    four = (matmul(hidden_v[0], w4_v[...]) + b4_v[...]).astype(BF16)
    four_v[:, 0:c4] = matmul(order, four).astype(BF16)
    four_v[:, c4 : 2 * c4] = matmul(order_above, four).astype(BF16)
    four_v[:, 2 * c4 : 3 * c4] = matmul(order_below, four).astype(BF16)
    for copy in copies[4:7]:
        copy.wait()
    c2 = w2_v.shape[1]
    two = (matmul(hidden_v[1], w2_v[...]) + b2_v[...]).astype(BF16)
    rest_v[:, 0:c2] = matmul(order, two).astype(BF16)
    for copy in copies[7:10]:
        copy.wait()
    same = (matmul(hidden_v[2], ws_v[...]) + bs_v[...]).astype(BF16)
    rest_v[:, c2:] = matmul(order, same).astype(BF16)


def fetch_kernel(w4, b4, wj, w2, b2, w4_v, b4_v, wj_v, w2_v, b2_v, sems):
    pairs = ((w4, w4_v), (b4, b4_v), (wj, wj_v), (w2, w2_v), (b2, b2_v))
    copies = [pltpu.make_async_copy(src, dst, sems.at[i]) for i, (src, dst) in enumerate(pairs)]
    for copy in copies:
        copy.start()
    for copy in copies:
        copy.wait()


def four_kernel(arrived, places, w4, b4, wj, joined, tiles_v, wide_v, acc_v, out_v, sems):
    tok_dev, c4 = arrived.shape[0], arrived.shape[1] // 3
    row_count = tok_dev // GRID_W
    me = lax.axis_index("rows")
    top = jnp.where(me > 0, 1.0, 0.0)
    bottom = jnp.where(me < lax.axis_size("rows") - 1, 1.0, 0.0)
    bias = b4[...]
    feat = c4

    base = 3 * tok_dev
    tiles_v[0:base] = matmul(places[0:base], arrived[:, 0:c4]).astype(BF16)
    tiles_v[base : base + 3 * GRID_W] = matmul(places[base : base + 3 * GRID_W], arrived[:, c4 : 2 * c4]).astype(BF16)
    base += 3 * GRID_W
    tiles_v[base : base + 3 * GRID_W] = matmul(places[base : base + 3 * GRID_W], arrived[:, 2 * c4 :]).astype(BF16)

    left = jnp.where(iota((GRID_W, 1), 0) == 0, 0.0, 1.0)
    right = jnp.where(iota((GRID_W, 1), 0) == GRID_W - 1, 0.0, 1.0)

    def fill(first, stride, rows, tap, to, scale):
        size = rows * GRID_W
        for b in range(4):
            part = matmul(tiles_v[first : first + size], w4[:, (tap * 4 + b) * feat : (tap * 4 + b + 1) * feat]) + bias
            if scale is not None:
                part = part * scale
            for i in range(rows):
                wide_v[pl.ds(to(i) * GRID_W, GRID_W), (b + 1) * feat : (b + 2) * feat] = part[
                    i * GRID_W : (i + 1) * GRID_W
                ].astype(BF16)
        for b, shift, edge, block in ((3, 1, left, 0), (0, 2, right, 5)):
            start = first + shift * stride
            part = matmul(tiles_v[start : start + size], w4[:, (tap * 4 + b) * feat : (tap * 4 + b + 1) * feat]) + bias
            if scale is not None:
                part = part * scale
            for i in range(rows):
                wide_v[pl.ds(to(i) * GRID_W, GRID_W), block * feat : (block + 1) * feat] = (
                    part[i * GRID_W : (i + 1) * GRID_W] * edge
                ).astype(BF16)

    for tap in range(4):
        fill(0, tok_dev, row_count, tap, lambda i, tap=tap: 4 * i + tap + 1, None)
    fill(3 * tok_dev, GRID_W, 1, 3, lambda i: 0, top)
    fill(3 * tok_dev + 3 * GRID_W, GRID_W, 1, 0, lambda i: 4 * row_count + 1, bottom)

    copies = []
    for chunk in range(row_count):
        for b in range(4):
            total = None
            for row_tap in range(3):
                term = matmul(
                    wide_v[(4 * chunk + row_tap) * GRID_W : (4 * chunk + row_tap + 4) * GRID_W, b * feat : (b + 3) * feat],
                    wj[row_tap],
                )
                total = term if total is None else total + term
            for r in range(4):
                for block in range(feat // 128):
                    acc_v[4 * chunk + r, block, pl.ds(b, GRID_W, 4), :] = total[
                        r * GRID_W : (r + 1) * GRID_W, block * 128 : (block + 1) * 128
                    ]
        for r in range(4 * chunk, 4 * chunk + 4):
            for block in range(feat // 128):
                out_v[r, :, block * 128 : (block + 1) * 128] = acc_v[r, block].astype(BF16)
        copy = pltpu.make_async_copy(
            out_v.at[pl.ds(4 * chunk, 4)], joined.at[pl.ds(4 * chunk, 4)], sems.at[chunk]
        )
        copy.start()
        copies.append(copy)
    for copy in copies:
        copy.wait()


def rest_kernel(arrived, places, w2, b2, up_two, same, acc_v, out_v, same_v, sems):
    tok_dev = arrived.shape[0]
    c2 = w2.shape[0]
    row_count = tok_dev // GRID_W
    place = places[0:tok_dev]
    same_v[...] = matmul(place, arrived[:, c2:]).astype(BF16)
    out_same = pltpu.make_async_copy(same_v, same, sems.at[0])
    out_same.start()
    tile = matmul(place, arrived[:, 0:c2]).astype(BF16)
    bias = b2[...]
    copies = []
    for a in range(2):
        for b in range(2):
            part = matmul(tile, w2[:, (a * 2 + b) * c2 : (a * 2 + b + 1) * c2]) + bias
            for i in range(row_count):
                for block in range(c2 // 128):
                    acc_v[2 * i + a, block, pl.ds(b, GRID_W, 2), :] = part[
                        i * GRID_W : (i + 1) * GRID_W, block * 128 : (block + 1) * 128
                    ]
        for i in range(row_count):
            r = 2 * i + a
            for block in range(c2 // 128):
                out_v[r, :, block * 128 : (block + 1) * 128] = acc_v[r, block].astype(BF16)
            copy = pltpu.make_async_copy(out_v.at[r], up_two.at[r], sems.at[1 + r])
            copy.start()
            copies.append(copy)
    out_same.wait()
    for copy in copies:
        copy.wait()


def body(
    hidden_states,
    cell_of,
    proj_four_weight,
    proj_four_bias,
    proj_two_weight,
    proj_two_bias,
    proj_same_weight,
    proj_same_bias,
    up4_weight,
    up4_bias,
    up2_weight,
    up2_bias,
    join_weight,
):
    hooks, tok_dev, hid = hidden_states.shape
    shards = lax.axis_size("rows")
    per_peer = tok_dev // shards
    row_count = tok_dev // GRID_W
    c4, c2, cs = proj_four_weight.shape[1], proj_two_weight.shape[1], proj_same_weight.shape[1]
    feat = join_weight.shape[3]
    table = cell_of.reshape(shards, tok_dev)
    place_rows = 3 * tok_dev + 6 * GRID_W
    shape = jax.ShapeDtypeStruct

    send_four, send_rest, places = pl.pallas_call(
        project_kernel,
        out_shape=(
            pltpu.VMEM((tok_dev, 3 * c4), BF16),
            pltpu.VMEM((tok_dev, c2 + cs), BF16),
            pltpu.VMEM((place_rows, tok_dev), BF16),
        ),
        in_specs=[ANY] * 8,
        out_specs=(VMEM, VMEM, VMEM),
        scratch_shapes=[
            pltpu.VMEM(hidden_states.shape, BF16),
            pltpu.VMEM(table.shape, jnp.int32),
            pltpu.VMEM((hid, c4), BF16),
            pltpu.VMEM((hid, c2), BF16),
            pltpu.VMEM((hid, cs), BF16),
            pltpu.VMEM((1, c4), F32),
            pltpu.VMEM((1, c2), F32),
            pltpu.VMEM((1, cs), F32),
            pltpu.SemaphoreType.DMA((10,)),
        ],
        cost_estimate=pl.CostEstimate(flops=2 * tok_dev * hid * (c4 + c2 + cs), bytes_accessed=5 << 20, transcendentals=0),
        name="project",
        compiler_params=pltpu.CompilerParams(vmem_limit_bytes=12 << 20),
    )(
        in_hbm(hidden_states),
        in_hbm(table),
        in_hbm(proj_four_weight),
        in_hbm(proj_four_bias.reshape(1, -1)),
        in_hbm(proj_two_weight),
        in_hbm(proj_two_bias.reshape(1, -1)),
        in_hbm(proj_same_weight),
        in_hbm(proj_same_bias.reshape(1, -1)),
    )
    exchange = functools.partial(lax.all_to_all, axis_name="rows", split_axis=0, concat_axis=0, tiled=True)
    four = exchange(send_four.reshape(shards, per_peer, 3 * c4)).reshape(tok_dev, 3 * c4)
    rest = exchange(send_rest.reshape(shards, per_peer, c2 + cs)).reshape(tok_dev, c2 + cs)

    weights = (
        up4_weight,
        up4_bias.reshape(1, -1),
        join_weight.reshape(3, 3 * c4, feat),
        up2_weight,
        up2_bias.reshape(1, -1),
    )
    w4, b4, wj, w2, b2 = pl.pallas_call(
        fetch_kernel,
        out_shape=tuple(pltpu.VMEM(w.shape, w.dtype) for w in weights),
        in_specs=[ANY] * 5,
        out_specs=(VMEM,) * 5,
        scratch_shapes=[pltpu.SemaphoreType.DMA((5,))],
        cost_estimate=pl.CostEstimate(flops=1 << 30, bytes_accessed=6 << 20, transcendentals=0),
        name="fetch",
        compiler_params=pltpu.CompilerParams(vmem_limit_bytes=8 << 20),
    )(*(in_hbm(w) for w in weights))

    out_rows = 4 * row_count
    joined = pl.pallas_call(
        four_kernel,
        out_shape=shape((out_rows, 4 * GRID_W, feat), BF16),
        in_specs=[VMEM] * 5,
        out_specs=ANY,
        scratch_shapes=[
            pltpu.VMEM((place_rows, c4), BF16),
            pltpu.VMEM(((out_rows + 2) * GRID_W, 6 * c4), BF16),
            pltpu.VMEM((out_rows, feat // 128, 4 * GRID_W, 128), F32),
            pltpu.VMEM((out_rows, 4 * GRID_W, feat), BF16),
            pltpu.SemaphoreType.DMA((row_count,)),
        ],
        compiler_params=pltpu.CompilerParams(vmem_limit_bytes=24 << 20),
        cost_estimate=pl.CostEstimate(flops=4 << 30, bytes_accessed=4 << 20, transcendentals=0),
        name="join",
    )(four, places, w4, b4, wj)

    upsampled_two, same_scale = pl.pallas_call(
        rest_kernel,
        out_shape=(shape((2 * row_count, 2 * GRID_W, c2), BF16), shape((tok_dev, cs), BF16)),
        in_specs=[VMEM] * 4,
        out_specs=(ANY, ANY),
        scratch_shapes=[
            pltpu.VMEM((2 * row_count, c2 // 128, 2 * GRID_W, 128), F32),
            pltpu.VMEM((2 * row_count, 2 * GRID_W, c2), BF16),
            pltpu.VMEM((tok_dev, cs), BF16),
            pltpu.SemaphoreType.DMA((1 + 2 * row_count,)),
        ],
        compiler_params=pltpu.CompilerParams(vmem_limit_bytes=16 << 20),
        cost_estimate=pl.CostEstimate(flops=1 << 28, bytes_accessed=4 << 20, transcendentals=0),
        name="rest",
    )(rest, places, w2, b2)
    return (joined, upsampled_two, same_scale.reshape(row_count, GRID_W, cs))


def solution(mesh):
    return jax.shard_map(
        body,
        mesh=mesh,
        in_specs=(P(None, ("img", "rows"), None),) + (P(),) * 12,
        out_specs=(P(("img", "rows"), None, None),) * 3,
        check_vma=False,
    )
```

```python
import functools

import jax
import jax.numpy as jnp
from jax import lax
from jax.experimental import pallas as pl
from jax.experimental.pallas import tpu as pltpu
from jax.sharding import PartitionSpec as P

GRID_W = 64
CHUNK = 256
F32 = jnp.float32
BF16 = jnp.bfloat16
ANY = pl.BlockSpec(memory_space=pl.ANY)
VMEM = pl.BlockSpec(memory_space=pltpu.VMEM)


def in_hbm(x):
    return pltpu.with_memory_space_constraint(x, pltpu.HBM)


def one_hot(mask):
    return jnp.where(mask, 1.0, 0.0).astype(BF16)


def iota(shape, dim):
    return lax.broadcasted_iota(jnp.int32, shape, dim)


def matmul(left, right):
    return jnp.dot(left, right, preferred_element_type=F32)


def column(row, size):
    same = iota((size, size), 0) == iota((size, size), 1)
    return jnp.sum(jnp.where(same, jnp.broadcast_to(row, (size, size)), 0.0), axis=1, keepdims=True)


def landing(table, block, tok_dev, per_peer):
    shards = table.shape[0]
    start = block * tok_dev
    inside = jnp.logical_and(table >= start, table < start + tok_dev)
    before = one_hot(iota((tok_dev, tok_dev), 0) < iota((tok_dev, tok_dev), 1))
    rank = matmul(one_hot(inside), before)
    place = (table - start).astype(F32)
    lane = iota((shards, tok_dev), 1)
    spread = jnp.zeros((shards, tok_dev), F32)
    for k in range(per_peer):
        hit = jnp.logical_and(inside, rank == float(k))
        found = jnp.sum(jnp.where(hit, place, 0.0), axis=1, keepdims=True)
        spread = spread + jnp.where(lax.rem(lane, per_peer) == k, found, 0.0)
    own = lax.div(lane, per_peer) == iota((shards, tok_dev), 0)
    return jnp.sum(jnp.where(own, spread, 0.0), axis=0, keepdims=True).astype(jnp.int32)


def project_kernel(
    hidden, table_hbm, w4, b4, w2, b2, ws, bs, send, places_v,
    hidden_v, table_v, w4_v, w2_v, ws_v, b4_v, b2_v, bs_v, send_v, sems, out_sems,
):
    chunks = ws.shape[1] // CHUNK
    pairs = [
        (table_hbm, table_v),
        (hidden.at[0], hidden_v.at[0]),
        (b4, b4_v),
        (w4, w4_v),
        (hidden.at[1], hidden_v.at[1]),
        (b2, b2_v),
        (w2, w2_v),
        (hidden.at[2], hidden_v.at[2]),
        (bs, bs_v),
    ] + [(ws.at[:, pl.ds(i * CHUNK, CHUNK)], ws_v.at[i]) for i in range(chunks)]
    copies = [pltpu.make_async_copy(src, dst, sems.at[i]) for i, (src, dst) in enumerate(pairs)]
    for copy in copies:
        copy.start()
    shards, tok_dev = table_v.shape
    per_peer = tok_dev // shards
    me = lax.axis_index("rows")
    copies[0].wait()
    table = table_v[...]
    mine = table_v[pl.ds(me, 1), :]
    block_row = lax.div(mine, tok_dev)
    block_col = column(block_row.astype(F32), tok_dev).astype(jnp.int32)
    square = (tok_dev, tok_dev)
    earlier = jnp.logical_and(block_col == jnp.broadcast_to(block_row, square), iota(square, 0) < iota(square, 1))
    within = jnp.sum(jnp.where(earlier, 1.0, 0.0), axis=0, keepdims=True).astype(jnp.int32)
    slot = block_row * per_peer + within
    order = one_hot(iota(square, 0) == slot)
    order_above = one_hot(iota(square, 0) == slot + per_peer)
    order_below = one_hot(iota(square, 0) == slot - per_peer)

    own = landing(table, me, tok_dev, per_peer)
    above = landing(table, me - 1, tok_dev, per_peer)
    below = landing(table, me + 1, tok_dev, per_peer)
    cell = iota(square, 0)
    col = lax.rem(cell, GRID_W)
    edge = (GRID_W, tok_dev)
    edge_col = iota(edge, 0)
    last = edge_col + (tok_dev - GRID_W)
    places_v[0:tok_dev] = one_hot(cell == own)
    places_v[tok_dev : 2 * tok_dev] = one_hot(jnp.logical_and(cell == own + 1, col != 0))
    places_v[2 * tok_dev : 3 * tok_dev] = one_hot(jnp.logical_and(cell == own - 1, col != GRID_W - 1))
    base = 3 * tok_dev
    for source, target in ((above, last), (below, edge_col)):
        places_v[base : base + GRID_W] = one_hot(target == source)
        places_v[base + GRID_W : base + 2 * GRID_W] = one_hot(jnp.logical_and(target == source + 1, edge_col != 0))
        places_v[base + 2 * GRID_W : base + 3 * GRID_W] = one_hot(
            jnp.logical_and(target == source - 1, edge_col != GRID_W - 1)
        )
        base += 3 * GRID_W

    for copy in copies[1:4]:
        copy.wait()
    c4 = w4_v.shape[1]
    four = (matmul(hidden_v[0], w4_v[...]) + b4_v[...]).astype(BF16)
    send_v[:, 0:c4] = matmul(order, four).astype(BF16)
    send_v[:, c4 : 2 * c4] = matmul(order_above, four).astype(BF16)
    send_v[:, 2 * c4 : 3 * c4] = matmul(order_below, four).astype(BF16)
    for copy in copies[4:7]:
        copy.wait()
    c2 = w2_v.shape[1]
    two = (matmul(hidden_v[1], w2_v[...]) + b2_v[...]).astype(BF16)
    send_v[:, 3 * c4 : 3 * c4 + c2] = matmul(order, two).astype(BF16)
    done = 3 * c4 + c2
    outs = [(0, done)] + [(done + i * CHUNK, CHUNK) for i in range(chunks)]
    stores = [
        pltpu.make_async_copy(send_v.at[:, pl.ds(at, size)], send.at[:, pl.ds(at, size)], out_sems.at[i])
        for i, (at, size) in enumerate(outs)
    ]
    stores[0].start()
    for copy in copies[7:9]:
        copy.wait()
    for i in range(chunks):
        copies[9 + i].wait()
        same = (matmul(hidden_v[2], ws_v[i]) + bs_v[:, i * CHUNK : (i + 1) * CHUNK]).astype(BF16)
        send_v[:, done + i * CHUNK : done + (i + 1) * CHUNK] = matmul(order, same).astype(BF16)
        stores[1 + i].start()
    for store in stores:
        store.wait()


def fetch_kernel(w4, b4, b2, w4_v, b4_v, b2_v, sems):
    pairs = ((w4, w4_v), (b4, b4_v), (b2, b2_v))
    copies = [pltpu.make_async_copy(src, dst, sems.at[i]) for i, (src, dst) in enumerate(pairs)]
    for copy in copies:
        copy.start()
    for copy in copies:
        copy.wait()


def finish_kernel(
    arrived, places, w4, b4, b2, wj_hbm, w2_hbm, joined, up_two, same,
    wj, w2, tiles_v, wide_v, acc_v, out_v, acc_two_v, two_v, same_v, weight_sems, sems, rest_sems,
):
    weights = [
        pltpu.make_async_copy(src, dst, weight_sems.at[i]) for i, (src, dst) in enumerate(((wj_hbm, wj), (w2_hbm, w2)))
    ]
    for copy in weights:
        copy.start()
    tok_dev, c4 = arrived.shape[0], w4.shape[0]
    c2 = w2.shape[0]
    row_count = tok_dev // GRID_W
    place = places[0:tok_dev]
    same_v[...] = matmul(place, arrived[:, 3 * c4 + c2 :]).astype(BF16)
    stores = [pltpu.make_async_copy(same_v, same, rest_sems.at[0])]
    stores[0].start()
    widen(arrived, places, w4, b4, tiles_v, wide_v)
    weights[0].wait()
    for chunk in range(row_count):
        stores.append(convolve(chunk, wide_v, wj, joined, acc_v, out_v, sems))
        if chunk == 0:
            weights[1].wait()
            stores += expand_two(arrived, place, w2, b2, 3 * c4, up_two, acc_two_v, two_v, rest_sems)
    for store in stores:
        store.wait()


def widen(arrived, places, w4, b4, tiles_v, wide_v):
    tok_dev, c4 = arrived.shape[0], w4.shape[0]
    row_count = tok_dev // GRID_W
    me = lax.axis_index("rows")
    top = jnp.where(me > 0, 1.0, 0.0)
    bottom = jnp.where(me < lax.axis_size("rows") - 1, 1.0, 0.0)
    bias = b4[...]
    feat = c4

    base = 3 * tok_dev
    tiles_v[0:base] = matmul(places[0:base], arrived[:, 0:c4]).astype(BF16)
    tiles_v[base : base + 3 * GRID_W] = matmul(places[base : base + 3 * GRID_W], arrived[:, c4 : 2 * c4]).astype(BF16)
    base += 3 * GRID_W
    tiles_v[base : base + 3 * GRID_W] = matmul(places[base : base + 3 * GRID_W], arrived[:, 2 * c4 : 3 * c4]).astype(BF16)

    left = jnp.where(iota((GRID_W, 1), 0) == 0, 0.0, 1.0)
    right = jnp.where(iota((GRID_W, 1), 0) == GRID_W - 1, 0.0, 1.0)

    def fill(first, stride, rows, tap, to, scale):
        size = rows * GRID_W
        for b in range(4):
            part = matmul(tiles_v[first : first + size], w4[:, (tap * 4 + b) * feat : (tap * 4 + b + 1) * feat]) + bias
            if scale is not None:
                part = part * scale
            for i in range(rows):
                wide_v[pl.ds(to(i) * GRID_W, GRID_W), (b + 1) * feat : (b + 2) * feat] = part[
                    i * GRID_W : (i + 1) * GRID_W
                ].astype(BF16)
        for b, shift, edge, block in ((3, 1, left, 0), (0, 2, right, 5)):
            start = first + shift * stride
            part = matmul(tiles_v[start : start + size], w4[:, (tap * 4 + b) * feat : (tap * 4 + b + 1) * feat]) + bias
            if scale is not None:
                part = part * scale
            for i in range(rows):
                wide_v[pl.ds(to(i) * GRID_W, GRID_W), block * feat : (block + 1) * feat] = (
                    part[i * GRID_W : (i + 1) * GRID_W] * edge
                ).astype(BF16)

    for tap in range(4):
        fill(0, tok_dev, row_count, tap, lambda i, tap=tap: 4 * i + tap + 1, None)
    fill(3 * tok_dev, GRID_W, 1, 3, lambda i: 0, top)
    fill(3 * tok_dev + 3 * GRID_W, GRID_W, 1, 0, lambda i: 4 * row_count + 1, bottom)


def convolve(chunk, wide_v, wj, joined, acc_v, out_v, sems):
    feat = wj.shape[2]
    for b in range(4):
        total = None
        for row_tap in range(3):
            first = (4 * chunk + row_tap) * GRID_W
            term = matmul(wide_v[first : first + 4 * GRID_W, b * feat : (b + 3) * feat], wj[row_tap])
            total = term if total is None else total + term
        for r in range(4):
            for block in range(feat // 128):
                acc_v[4 * chunk + r, block, pl.ds(b, GRID_W, 4), :] = total[
                    r * GRID_W : (r + 1) * GRID_W, block * 128 : (block + 1) * 128
                ]
    for r in range(4 * chunk, 4 * chunk + 4):
        for block in range(feat // 128):
            out_v[r, :, block * 128 : (block + 1) * 128] = acc_v[r, block].astype(BF16)
    rows = pl.ds(4 * chunk, 4)
    store = pltpu.make_async_copy(out_v.at[rows], joined.at[rows], sems.at[chunk])
    store.start()
    return store


def expand_two(arrived, place, w2, b2, at, up_two, acc_v, out_v, sems):
    c2 = w2.shape[0]
    row_count = arrived.shape[0] // GRID_W
    tile = matmul(place, arrived[:, at : at + c2]).astype(BF16)
    bias = b2[...]
    stores = []
    for a in range(2):
        for b in range(2):
            part = matmul(tile, w2[:, (a * 2 + b) * c2 : (a * 2 + b + 1) * c2]) + bias
            for i in range(row_count):
                for block in range(c2 // 128):
                    acc_v[2 * i + a, block, pl.ds(b, GRID_W, 2), :] = part[
                        i * GRID_W : (i + 1) * GRID_W, block * 128 : (block + 1) * 128
                    ]
        for i in range(row_count):
            r = 2 * i + a
            for block in range(c2 // 128):
                out_v[r, :, block * 128 : (block + 1) * 128] = acc_v[r, block].astype(BF16)
            store = pltpu.make_async_copy(out_v.at[r], up_two.at[r], sems.at[1 + r])
            store.start()
            stores.append(store)
    return stores


def body(
    hidden_states,
    cell_of,
    proj_four_weight,
    proj_four_bias,
    proj_two_weight,
    proj_two_bias,
    proj_same_weight,
    proj_same_bias,
    up4_weight,
    up4_bias,
    up2_weight,
    up2_bias,
    join_weight,
):
    hooks, tok_dev, hid = hidden_states.shape
    shards = lax.axis_size("rows")
    per_peer = tok_dev // shards
    row_count = tok_dev // GRID_W
    c4, c2, cs = proj_four_weight.shape[1], proj_two_weight.shape[1], proj_same_weight.shape[1]
    feat = join_weight.shape[3]
    table = cell_of.reshape(shards, tok_dev)
    place_rows = 3 * tok_dev + 6 * GRID_W
    shape = jax.ShapeDtypeStruct

    total = 3 * c4 + c2 + cs
    biases = [bias.reshape(1, -1) for bias in (proj_four_bias, proj_two_bias, proj_same_bias)]
    inputs = (
        hidden_states,
        table,
        proj_four_weight,
        biases[0],
        proj_two_weight,
        biases[1],
        proj_same_weight,
        biases[2],
    )
    send, places = pl.pallas_call(
        project_kernel,
        out_shape=(pltpu.HBM((tok_dev, total), BF16), pltpu.VMEM((place_rows, tok_dev), BF16)),
        in_specs=[ANY] * 8,
        out_specs=(ANY, VMEM),
        scratch_shapes=[
            pltpu.VMEM(hidden_states.shape, BF16),
            pltpu.VMEM(table.shape, jnp.int32),
            pltpu.VMEM((hid, c4), BF16),
            pltpu.VMEM((hid, c2), BF16),
            pltpu.VMEM((cs // CHUNK, hid, CHUNK), BF16),
            pltpu.VMEM((1, c4), F32),
            pltpu.VMEM((1, c2), F32),
            pltpu.VMEM((1, cs), F32),
            pltpu.VMEM((tok_dev, total), BF16),
            pltpu.SemaphoreType.DMA((9 + cs // CHUNK,)),
            pltpu.SemaphoreType.DMA((1 + cs // CHUNK,)),
        ],
        compiler_params=pltpu.CompilerParams(vmem_limit_bytes=12 << 20),
        cost_estimate=pl.CostEstimate(flops=2 * tok_dev * hid * (c4 + c2 + cs), bytes_accessed=5 << 20, transcendentals=0),
        name="project",
    )(*(in_hbm(x) for x in inputs))
    arrived = lax.all_to_all(
        send.reshape(shards, per_peer, total), "rows", split_axis=0, concat_axis=0, tiled=True
    ).reshape(tok_dev, total)

    weights = (up4_weight, up4_bias.reshape(1, -1), up2_bias.reshape(1, -1))
    w4, b4, b2 = pl.pallas_call(
        fetch_kernel,
        out_shape=tuple(pltpu.VMEM(w.shape, w.dtype) for w in weights),
        in_specs=[ANY] * 3,
        out_specs=(VMEM,) * 3,
        scratch_shapes=[pltpu.SemaphoreType.DMA((3,))],
        cost_estimate=pl.CostEstimate(flops=1 << 30, bytes_accessed=2 << 20, transcendentals=0),
        name="fetch",
        compiler_params=pltpu.CompilerParams(vmem_limit_bytes=4 << 20),
    )(*(in_hbm(w) for w in weights))

    out_rows = 4 * row_count
    joined, upsampled_two, same_scale = pl.pallas_call(
        finish_kernel,
        out_shape=(
            shape((out_rows, 4 * GRID_W, feat), BF16),
            shape((2 * row_count, 2 * GRID_W, c2), BF16),
            shape((tok_dev, cs), BF16),
        ),
        in_specs=[VMEM] * 5 + [ANY] * 2,
        out_specs=(ANY, ANY, ANY),
        scratch_shapes=[
            pltpu.VMEM((3, 3 * c4, feat), BF16),
            pltpu.VMEM(up2_weight.shape, BF16),
            pltpu.VMEM((place_rows, c4), BF16),
            pltpu.VMEM(((out_rows + 2) * GRID_W, 6 * c4), BF16),
            pltpu.VMEM((out_rows, feat // 128, 4 * GRID_W, 128), F32),
            pltpu.VMEM((out_rows, 4 * GRID_W, feat), BF16),
            pltpu.VMEM((2 * row_count, c2 // 128, 2 * GRID_W, 128), F32),
            pltpu.VMEM((2 * row_count, 2 * GRID_W, c2), BF16),
            pltpu.VMEM((tok_dev, cs), BF16),
            pltpu.SemaphoreType.DMA((2,)),
            pltpu.SemaphoreType.DMA((row_count,)),
            pltpu.SemaphoreType.DMA((1 + 2 * row_count,)),
        ],
        compiler_params=pltpu.CompilerParams(vmem_limit_bytes=24 << 20),
        cost_estimate=pl.CostEstimate(flops=4 << 30, bytes_accessed=4 << 20, transcendentals=0),
        name="finish",
    )(arrived, places, w4, b4, b2, in_hbm(join_weight.reshape(3, 3 * c4, feat)), in_hbm(up2_weight))
    return (joined, upsampled_two, same_scale.reshape(row_count, GRID_W, cs))


def solution(mesh):
    return jax.shard_map(
        body,
        mesh=mesh,
        in_specs=(P(None, ("img", "rows"), None),) + (P(),) * 12,
        out_specs=(P(("img", "rows"), None, None),) * 3,
        check_vma=False,
    )
```

```python
import functools

import jax
import jax.numpy as jnp
from jax import lax
from jax.experimental import pallas as pl
from jax.experimental.pallas import tpu as pltpu
from jax.sharding import PartitionSpec as P


GRID_W = 64
CHUNK = 256
F32 = jnp.float32
BF16 = jnp.bfloat16
ANY = pl.BlockSpec(memory_space=pl.ANY)
VMEM = pl.BlockSpec(memory_space=pltpu.VMEM)


def in_hbm(x):
    return pltpu.with_memory_space_constraint(x, pltpu.HBM)


def one_hot(mask):
    return jnp.where(mask, 1.0, 0.0).astype(BF16)


def iota(shape, dim):
    return lax.broadcasted_iota(jnp.int32, shape, dim)


def matmul(left, right):
    return jnp.dot(left, right, preferred_element_type=F32)


def column(row, size):
    same = iota((size, size), 0) == iota((size, size), 1)
    return jnp.sum(jnp.where(same, jnp.broadcast_to(row, (size, size)), 0.0), axis=1, keepdims=True)


def low_part(shards):
    return 1 << ((shards.bit_length()) // 2)


def landing(table, block, tok_dev, per_peer, flip=0):
    shards = table.shape[0]
    start = block * tok_dev
    inside = jnp.logical_and(table >= start, table < start + tok_dev)
    before = one_hot(iota((tok_dev, tok_dev), 0) < iota((tok_dev, tok_dev), 1))
    rank = matmul(one_hot(inside), before)
    place = (table - start).astype(F32)
    lane = iota((shards, tok_dev), 1)
    spread = jnp.zeros((shards, tok_dev), F32)
    for k in range(per_peer):
        hit = jnp.logical_and(inside, rank == float(k))
        found = jnp.sum(jnp.where(hit, place, 0.0), axis=1, keepdims=True)
        spread = spread + jnp.where(lax.rem(lane, per_peer) == k, found, 0.0)
    own = lax.div(lane, per_peer) == jnp.bitwise_xor(iota((shards, tok_dev), 0), flip)
    return jnp.sum(jnp.where(own, spread, 0.0), axis=0, keepdims=True).astype(jnp.int32)


def start_all(pairs, sems):
    copies = [pltpu.make_async_copy(src, dst, sems.at[i]) for i, (src, dst) in enumerate(pairs)]
    for copy in copies:
        copy.start()
    return copies


def project_kernel(
    hidden, table_hbm, w4, b4, w2, b2, send, places_v, order_v,
    hidden_v, table_v, w4_v, w2_v, b4_v, b2_v, send_v, sems, out_sems,
):
    copies = start_all(
        [
            (table_hbm, table_v),
            (hidden.at[0], hidden_v.at[0]),
            (b4, b4_v),
            (w4, w4_v),
            (hidden.at[1], hidden_v.at[1]),
            (b2, b2_v),
            (w2, w2_v),
        ],
        sems,
    )
    shards, tok_dev = table_v.shape
    per_peer = tok_dev // shards
    me = lax.axis_index("rows")
    copies[0].wait()
    table = table_v[...]
    mine = table_v[pl.ds(me, 1), :]
    block_row = lax.div(mine, tok_dev)
    block_col = column(block_row.astype(F32), tok_dev).astype(jnp.int32)
    square = (tok_dev, tok_dev)
    earlier = jnp.logical_and(block_col == jnp.broadcast_to(block_row, square), iota(square, 0) < iota(square, 1))
    within = jnp.sum(jnp.where(earlier, 1.0, 0.0), axis=0, keepdims=True).astype(jnp.int32)
    slot = block_row * per_peer + within
    order = one_hot(iota(square, 0) == slot)
    order_above = one_hot(iota(square, 0) == slot + per_peer)
    order_below = one_hot(iota(square, 0) == slot - per_peer)

    low = low_part(shards)
    apart = jnp.bitwise_xor(block_row, me)
    turn = lax.rem(apart, low) * (shards // low) + lax.div(apart, low)
    order_v[...] = one_hot(iota(square, 0) == turn * per_peer + within)

    own = landing(table, me, tok_dev, per_peer)
    above = landing(table, me - 1, tok_dev, per_peer)
    below = landing(table, me + 1, tok_dev, per_peer)
    cell = iota(square, 0)
    col = lax.rem(cell, GRID_W)
    edge = (GRID_W, tok_dev)
    edge_col = iota(edge, 0)
    last = edge_col + (tok_dev - GRID_W)
    places_v[0:tok_dev] = one_hot(cell == own)
    places_v[tok_dev : 2 * tok_dev] = one_hot(jnp.logical_and(cell == own + 1, col != 0))
    places_v[2 * tok_dev : 3 * tok_dev] = one_hot(jnp.logical_and(cell == own - 1, col != GRID_W - 1))
    base = 3 * tok_dev
    for source, target in ((above, last), (below, edge_col)):
        places_v[base : base + GRID_W] = one_hot(target == source)
        places_v[base + GRID_W : base + 2 * GRID_W] = one_hot(jnp.logical_and(target == source + 1, edge_col != 0))
        places_v[base + 2 * GRID_W : base + 3 * GRID_W] = one_hot(
            jnp.logical_and(target == source - 1, edge_col != GRID_W - 1)
        )
        base += 3 * GRID_W

    places_v[base : base + tok_dev] = one_hot(cell == landing(table, me, tok_dev, per_peer, me))

    for copy in copies[1:4]:
        copy.wait()
    c4 = w4_v.shape[1]
    four = (matmul(hidden_v[0], w4_v[...]) + b4_v[...]).astype(BF16)
    send_v[:, 0:c4] = matmul(order, four).astype(BF16)
    send_v[:, c4 : 2 * c4] = matmul(order_above, four).astype(BF16)
    send_v[:, 2 * c4 : 3 * c4] = matmul(order_below, four).astype(BF16)
    cuts = (slice(0, 3 * c4), slice(3 * c4, send_v.shape[1]))
    stores = [
        pltpu.make_async_copy(send_v.at[:, cut], send.at[:, cut], out_sems.at[i]) for i, cut in enumerate(cuts)
    ]
    stores[0].start()
    for copy in copies[4:7]:
        copy.wait()
    two = (matmul(hidden_v[1], w2_v[...]) + b2_v[...]).astype(BF16)
    send_v[:, 3 * c4 :] = matmul(order, two).astype(BF16)
    stores[1].start()
    for store in stores:
        store.wait()


def same_kernel(hidden, ws, bs, order, *refs):
    count = len(refs) - 4
    outs, (hidden_v, ws_v, bs_v, sems) = refs[:count], refs[count:]
    chunks = ws.shape[1] // CHUNK
    copies = start_all(
        [(hidden.at[2], hidden_v), (bs, bs_v)]
        + [(ws.at[:, pl.ds(i * CHUNK, CHUNK)], ws_v.at[i]) for i in range(chunks)],
        sems,
    )
    copies[0].wait()
    copies[1].wait()
    rows = outs[0].shape[0]
    for i in range(chunks):
        cut = slice(i * CHUNK, (i + 1) * CHUNK)
        copies[2 + i].wait()
        same = (matmul(hidden_v[...], ws_v[i]) + bs_v[:, cut]).astype(BF16)
        sent = matmul(order[...], same).astype(BF16)
        for k, out in enumerate(outs):
            out[:, cut] = sent[k * rows : (k + 1) * rows]


def turn_kernel(low_count, *refs):
    lows, highs = refs[:low_count], refs[low_count:]
    rows = lows[0].shape[0] // len(highs)
    for h, high in enumerate(highs):
        for k, low in enumerate(lows):
            high[k * rows : (k + 1) * rows] = low[h * rows : (h + 1) * rows]


def fetch_kernel(w4, b4, b2, w4_v, b4_v, b2_v, sems):
    for copy in start_all([(w4, w4_v), (b4, b4_v), (b2, b2_v)], sems):
        copy.wait()


def finish_kernel(
    arrived, places, w4, b4, b2, wj_hbm, w2_hbm, joined, up_two,
    wj, w2, tiles_v, wide_v, acc_v, out_v, acc_two_v, two_v, weight_sems, sems, two_sems,
):
    weights = start_all([(wj_hbm, wj), (w2_hbm, w2)], weight_sems)
    tok_dev, c4 = arrived.shape[0], w4.shape[0]
    row_count = tok_dev // GRID_W
    place = places[0:tok_dev]
    stores = []
    widen(arrived, places, w4, b4, tiles_v, wide_v)
    weights[0].wait()
    for chunk in range(row_count):
        stores.append(convolve(chunk, wide_v, wj, joined, acc_v, out_v, sems))
        if chunk == 0:
            weights[1].wait()
            stores += expand_two(arrived, place, w2, b2, 3 * c4, up_two, acc_two_v, two_v, two_sems)
    for store in stores:
        store.wait()


def widen(arrived, places, w4, b4, tiles_v, wide_v):
    tok_dev, c4 = arrived.shape[0], w4.shape[0]
    row_count = tok_dev // GRID_W
    me = lax.axis_index("rows")
    top = jnp.where(me > 0, 1.0, 0.0)
    bottom = jnp.where(me < lax.axis_size("rows") - 1, 1.0, 0.0)
    bias = b4[...]
    feat = c4

    base = 3 * tok_dev
    tiles_v[0:base] = matmul(places[0:base], arrived[:, 0:c4]).astype(BF16)
    tiles_v[base : base + 3 * GRID_W] = matmul(places[base : base + 3 * GRID_W], arrived[:, c4 : 2 * c4]).astype(BF16)
    base += 3 * GRID_W
    tiles_v[base : base + 3 * GRID_W] = matmul(places[base : base + 3 * GRID_W], arrived[:, 2 * c4 : 3 * c4]).astype(BF16)

    left = jnp.where(iota((GRID_W, 1), 0) == 0, 0.0, 1.0)
    right = jnp.where(iota((GRID_W, 1), 0) == GRID_W - 1, 0.0, 1.0)

    def fill(first, stride, rows, tap, to, scale):
        size = rows * GRID_W
        for b in range(4):
            part = matmul(tiles_v[first : first + size], w4[:, (tap * 4 + b) * feat : (tap * 4 + b + 1) * feat]) + bias
            if scale is not None:
                part = part * scale
            for i in range(rows):
                wide_v[pl.ds(to(i) * GRID_W, GRID_W), (b + 1) * feat : (b + 2) * feat] = part[
                    i * GRID_W : (i + 1) * GRID_W
                ].astype(BF16)
        for b, shift, edge, block in ((3, 1, left, 0), (0, 2, right, 5)):
            start = first + shift * stride
            part = matmul(tiles_v[start : start + size], w4[:, (tap * 4 + b) * feat : (tap * 4 + b + 1) * feat]) + bias
            if scale is not None:
                part = part * scale
            for i in range(rows):
                wide_v[pl.ds(to(i) * GRID_W, GRID_W), block * feat : (block + 1) * feat] = (
                    part[i * GRID_W : (i + 1) * GRID_W] * edge
                ).astype(BF16)

    for tap in range(4):
        fill(0, tok_dev, row_count, tap, lambda i, tap=tap: 4 * i + tap + 1, None)
    fill(3 * tok_dev, GRID_W, 1, 3, lambda i: 0, top)
    fill(3 * tok_dev + 3 * GRID_W, GRID_W, 1, 0, lambda i: 4 * row_count + 1, bottom)


def convolve(chunk, wide_v, wj, joined, acc_v, out_v, sems):
    feat = wj.shape[2]
    for b in range(4):
        total = None
        for row_tap in range(3):
            first = (4 * chunk + row_tap) * GRID_W
            term = matmul(wide_v[first : first + 4 * GRID_W, b * feat : (b + 3) * feat], wj[row_tap])
            total = term if total is None else total + term
        for r in range(4):
            for block in range(feat // 128):
                acc_v[4 * chunk + r, block, pl.ds(b, GRID_W, 4), :] = total[
                    r * GRID_W : (r + 1) * GRID_W, block * 128 : (block + 1) * 128
                ]
    for r in range(4 * chunk, 4 * chunk + 4):
        for block in range(feat // 128):
            out_v[r, :, block * 128 : (block + 1) * 128] = acc_v[r, block].astype(BF16)
    rows = pl.ds(4 * chunk, 4)
    store = pltpu.make_async_copy(out_v.at[rows], joined.at[rows], sems.at[chunk])
    store.start()
    return store


def expand_two(arrived, place, w2, b2, at, up_two, acc_v, out_v, sems):
    c2 = w2.shape[0]
    row_count = arrived.shape[0] // GRID_W
    tile = matmul(place, arrived[:, at : at + c2]).astype(BF16)
    bias = b2[...]
    stores = []
    for a in range(2):
        for b in range(2):
            part = matmul(tile, w2[:, (a * 2 + b) * c2 : (a * 2 + b + 1) * c2]) + bias
            for i in range(row_count):
                for block in range(c2 // 128):
                    acc_v[2 * i + a, block, pl.ds(b, GRID_W, 2), :] = part[
                        i * GRID_W : (i + 1) * GRID_W, block * 128 : (block + 1) * 128
                    ]
        for i in range(row_count):
            r = 2 * i + a
            for block in range(c2 // 128):
                out_v[r, :, block * 128 : (block + 1) * 128] = acc_v[r, block].astype(BF16)
            store = pltpu.make_async_copy(out_v.at[r], up_two.at[r], sems.at[r])
            store.start()
            stores.append(store)
    return stores


def place_kernel(places, *refs):
    arrived, same, rows_v = refs[:-2], refs[-2], refs[-1]
    rows = arrived[0].shape[0]
    for h, piece in enumerate(arrived):
        rows_v[h * rows : (h + 1) * rows] = piece[...]
    tok_dev = rows_v.shape[0]
    same[...] = matmul(places[places.shape[0] - tok_dev :], rows_v[...]).astype(BF16)


def body(
    hidden_states,
    cell_of,
    proj_four_weight,
    proj_four_bias,
    proj_two_weight,
    proj_two_bias,
    proj_same_weight,
    proj_same_bias,
    up4_weight,
    up4_bias,
    up2_weight,
    up2_bias,
    join_weight,
):
    _, tok_dev, hid = hidden_states.shape
    shards = lax.axis_size("rows")
    per_peer = tok_dev // shards
    row_count = tok_dev // GRID_W
    c4, c2, cs = proj_four_weight.shape[1], proj_two_weight.shape[1], proj_same_weight.shape[1]
    feat = join_weight.shape[3]
    table = cell_of.reshape(shards, tok_dev)
    place_rows = 4 * tok_dev + 6 * GRID_W
    shape = jax.ShapeDtypeStruct

    total = 3 * c4 + c2
    low = low_part(shards)
    high = shards // low
    biases = [bias.reshape(1, -1) for bias in (proj_four_bias, proj_two_bias, proj_same_bias)]
    inputs = (hidden_states, table, proj_four_weight, biases[0], proj_two_weight, biases[1])
    send, places, order = pl.pallas_call(
        project_kernel,
        out_shape=(
            pltpu.HBM((tok_dev, total), BF16),
            pltpu.VMEM((place_rows, tok_dev), BF16),
            pltpu.VMEM((tok_dev, tok_dev), BF16),
        ),
        in_specs=[ANY] * 6,
        out_specs=(ANY, VMEM, VMEM),
        scratch_shapes=[
            pltpu.VMEM((2, tok_dev, hid), BF16),
            pltpu.VMEM(table.shape, jnp.int32),
            pltpu.VMEM((hid, c4), BF16),
            pltpu.VMEM((hid, c2), BF16),
            pltpu.VMEM((1, c4), F32),
            pltpu.VMEM((1, c2), F32),
            pltpu.VMEM((tok_dev, total), BF16),
            pltpu.SemaphoreType.DMA((7,)),
            pltpu.SemaphoreType.DMA((2,)),
        ],
        compiler_params=pltpu.CompilerParams(vmem_limit_bytes=8 << 20),
        cost_estimate=pl.CostEstimate(flops=2 * tok_dev * hid * (c4 + c2), bytes_accessed=2 << 20, transcendentals=0),
        name="project",
    )(*(in_hbm(x) for x in inputs))
    arrived = lax.all_to_all(
        send.reshape(shards, per_peer, total), "rows", split_axis=0, concat_axis=0, tiled=True
    ).reshape(tok_dev, total)
    sent = pl.pallas_call(
        same_kernel,
        out_shape=(shape((high * per_peer, cs), BF16),) * low,
        in_specs=[ANY, ANY, ANY, VMEM],
        out_specs=(VMEM,) * low,
        scratch_shapes=[
            pltpu.VMEM((tok_dev, hid), BF16),
            pltpu.VMEM((cs // CHUNK, hid, CHUNK), BF16),
            pltpu.VMEM((1, cs), F32),
            pltpu.SemaphoreType.DMA((2 + cs // CHUNK,)),
        ],
        compiler_params=pltpu.CompilerParams(vmem_limit_bytes=8 << 20),
        cost_estimate=pl.CostEstimate(flops=2 * tok_dev * hid * cs, bytes_accessed=3 << 20, transcendentals=0),
        name="same",
    )(in_hbm(hidden_states), in_hbm(proj_same_weight), in_hbm(biases[2]), order)

    def swap(piece, step):
        return lax.ppermute(piece, "rows", [(i, i ^ step) for i in range(shards)])

    crossed = [sent[0]] + [swap(sent[k], k) for k in range(1, low)]
    turned = pl.pallas_call(
        functools.partial(turn_kernel, low),
        out_shape=(shape((low * per_peer, cs), BF16),) * high,
        in_specs=[VMEM] * low,
        out_specs=(VMEM,) * high,
        compiler_params=pltpu.CompilerParams(vmem_limit_bytes=4 << 20),
        cost_estimate=pl.CostEstimate(flops=1 << 26, bytes_accessed=1 << 20, transcendentals=0),
        name="turn",
    )(*crossed)
    landed = [turned[0]] + [swap(turned[h], h * low) for h in range(1, high)]

    weights = (up4_weight, up4_bias.reshape(1, -1), up2_bias.reshape(1, -1))
    w4, b4, b2 = pl.pallas_call(
        fetch_kernel,
        out_shape=tuple(pltpu.VMEM(w.shape, w.dtype) for w in weights),
        in_specs=[ANY] * 3,
        out_specs=(VMEM,) * 3,
        scratch_shapes=[pltpu.SemaphoreType.DMA((3,))],
        cost_estimate=pl.CostEstimate(flops=1 << 30, bytes_accessed=2 << 20, transcendentals=0),
        compiler_params=pltpu.CompilerParams(vmem_limit_bytes=4 << 20),
        name="fetch",
    )(*(in_hbm(w) for w in weights))

    out_rows = 4 * row_count
    joined, upsampled_two = pl.pallas_call(
        finish_kernel,
        out_shape=(
            shape((out_rows, 4 * GRID_W, feat), BF16),
            shape((2 * row_count, 2 * GRID_W, c2), BF16),
        ),
        in_specs=[VMEM] * 5 + [ANY] * 2,
        out_specs=(ANY, ANY),
        scratch_shapes=[
            pltpu.VMEM((3, 3 * c4, feat), BF16),
            pltpu.VMEM(up2_weight.shape, BF16),
            pltpu.VMEM((place_rows, c4), BF16),
            pltpu.VMEM(((out_rows + 2) * GRID_W, 6 * c4), BF16),
            pltpu.VMEM((out_rows, feat // 128, 4 * GRID_W, 128), F32),
            pltpu.VMEM((out_rows, 4 * GRID_W, feat), BF16),
            pltpu.VMEM((2 * row_count, c2 // 128, 2 * GRID_W, 128), F32),
            pltpu.VMEM((2 * row_count, 2 * GRID_W, c2), BF16),
            pltpu.SemaphoreType.DMA((2,)),
            pltpu.SemaphoreType.DMA((row_count,)),
            pltpu.SemaphoreType.DMA((2 * row_count,)),
        ],
        compiler_params=pltpu.CompilerParams(vmem_limit_bytes=24 << 20),
        cost_estimate=pl.CostEstimate(flops=4 << 30, bytes_accessed=4 << 20, transcendentals=0),
        name="finish",
    )(arrived, places, w4, b4, b2, in_hbm(join_weight.reshape(3, 3 * c4, feat)), in_hbm(up2_weight))
    same_scale = pl.pallas_call(
        place_kernel,
        out_shape=shape((tok_dev, cs), BF16),
        in_specs=[VMEM] * (1 + high),
        out_specs=VMEM,
        scratch_shapes=[pltpu.VMEM((tok_dev, cs), BF16)],
        compiler_params=pltpu.CompilerParams(vmem_limit_bytes=4 << 20),
        cost_estimate=pl.CostEstimate(flops=1 << 26, bytes_accessed=1 << 20, transcendentals=0),
        name="place",
    )(places, *landed)
    return (joined, upsampled_two, same_scale.reshape(row_count, GRID_W, cs))


def solution(mesh):
    return jax.shard_map(
        body,
        mesh=mesh,
        in_specs=(P(None, ("img", "rows"), None),) + (P(),) * 12,
        out_specs=(P(("img", "rows"), None, None),) * 3,
        check_vma=False,
    )
```

```python
import functools

import jax
import jax.numpy as jnp
from jax import lax
from jax.experimental import pallas as pl
from jax.experimental.pallas import tpu as pltpu
from jax.sharding import PartitionSpec as P


GRID_W = 64
CHUNK = 256
F32 = jnp.float32
BF16 = jnp.bfloat16
ANY = pl.BlockSpec(memory_space=pl.ANY)
VMEM = pl.BlockSpec(memory_space=pltpu.VMEM)


def in_hbm(x):
    return pltpu.with_memory_space_constraint(x, pltpu.HBM)


def one_hot(mask):
    return jnp.where(mask, 1.0, 0.0).astype(BF16)


def iota(shape, dim):
    return lax.broadcasted_iota(jnp.int32, shape, dim)


def matmul(left, right):
    return jnp.dot(left, right, preferred_element_type=F32)


def column(row, size):
    same = iota((size, size), 0) == iota((size, size), 1)
    return jnp.sum(jnp.where(same, jnp.broadcast_to(row, (size, size)), 0.0), axis=1, keepdims=True)


def low_part(shards):
    return 1 << ((shards.bit_length()) // 2)


def landing(table, block, tok_dev, per_peer, flip=0):
    shards = table.shape[0]
    start = block * tok_dev
    inside = jnp.logical_and(table >= start, table < start + tok_dev)
    before = one_hot(iota((tok_dev, tok_dev), 0) < iota((tok_dev, tok_dev), 1))
    rank = matmul(one_hot(inside), before)
    place = (table - start).astype(F32)
    lane = iota((shards, tok_dev), 1)
    spread = jnp.zeros((shards, tok_dev), F32)
    for k in range(per_peer):
        hit = jnp.logical_and(inside, rank == float(k))
        found = jnp.sum(jnp.where(hit, place, 0.0), axis=1, keepdims=True)
        spread = spread + jnp.where(lax.rem(lane, per_peer) == k, found, 0.0)
    own = lax.div(lane, per_peer) == jnp.bitwise_xor(iota((shards, tok_dev), 0), flip)
    return jnp.sum(jnp.where(own, spread, 0.0), axis=0, keepdims=True).astype(jnp.int32)


def start_all(pairs, sems):
    copies = [pltpu.make_async_copy(src, dst, sems.at[i]) for i, (src, dst) in enumerate(pairs)]
    for copy in copies:
        copy.start()
    return copies


def project_kernel(low, hidden, table_hbm, w4, b4, w2, b2, ws, bs, send, places_v, *refs):
    sent = refs[:low]
    hidden_v, table_v, w4_v, w2_v, ws_v, b4_v, b2_v, bs_v, send_v, sems, out_sem = refs[low:]
    chunks = ws.shape[1] // CHUNK
    copies = start_all(
        [
            (table_hbm, table_v),
            (hidden.at[0], hidden_v.at[0]),
            (b4, b4_v),
            (w4, w4_v),
            (hidden.at[1], hidden_v.at[1]),
            (b2, b2_v),
            (w2, w2_v),
            (hidden.at[2], hidden_v.at[2]),
            (bs, bs_v),
        ]
        + [(ws.at[:, pl.ds(i * CHUNK, CHUNK)], ws_v.at[i]) for i in range(chunks)],
        sems,
    )
    shards, tok_dev = table_v.shape
    per_peer = tok_dev // shards
    me = lax.axis_index("rows")
    copies[0].wait()
    table = table_v[...]
    mine = table_v[pl.ds(me, 1), :]
    block_row = lax.div(mine, tok_dev)
    block_col = column(block_row.astype(F32), tok_dev).astype(jnp.int32)
    square = (tok_dev, tok_dev)
    earlier = jnp.logical_and(block_col == jnp.broadcast_to(block_row, square), iota(square, 0) < iota(square, 1))
    within = jnp.sum(jnp.where(earlier, 1.0, 0.0), axis=0, keepdims=True).astype(jnp.int32)
    slot = block_row * per_peer + within
    order = one_hot(iota(square, 0) == slot)
    order_above = one_hot(iota(square, 0) == slot + per_peer)
    order_below = one_hot(iota(square, 0) == slot - per_peer)

    apart = jnp.bitwise_xor(block_row, me)
    turn = lax.rem(apart, low) * (shards // low) + lax.div(apart, low)
    order_turn = one_hot(iota(square, 0) == turn * per_peer + within)

    own = landing(table, me, tok_dev, per_peer)
    above = landing(table, me - 1, tok_dev, per_peer)
    below = landing(table, me + 1, tok_dev, per_peer)
    cell = iota(square, 0)
    col = lax.rem(cell, GRID_W)
    edge = (GRID_W, tok_dev)
    edge_col = iota(edge, 0)
    last = edge_col + (tok_dev - GRID_W)
    places_v[0:tok_dev] = one_hot(cell == own)
    places_v[tok_dev : 2 * tok_dev] = one_hot(jnp.logical_and(cell == own + 1, col != 0))
    places_v[2 * tok_dev : 3 * tok_dev] = one_hot(jnp.logical_and(cell == own - 1, col != GRID_W - 1))
    base = 3 * tok_dev
    for source, target in ((above, last), (below, edge_col)):
        places_v[base : base + GRID_W] = one_hot(target == source)
        places_v[base + GRID_W : base + 2 * GRID_W] = one_hot(jnp.logical_and(target == source + 1, edge_col != 0))
        places_v[base + 2 * GRID_W : base + 3 * GRID_W] = one_hot(
            jnp.logical_and(target == source - 1, edge_col != GRID_W - 1)
        )
        base += 3 * GRID_W

    places_v[base : base + tok_dev] = one_hot(cell == landing(table, me, tok_dev, per_peer, me))

    for copy in copies[1:4]:
        copy.wait()
    c4 = w4_v.shape[1]
    four = (matmul(hidden_v[0], w4_v[...]) + b4_v[...]).astype(BF16)
    send_v[:, 0:c4] = matmul(order, four).astype(BF16)
    send_v[:, c4 : 2 * c4] = matmul(order_above, four).astype(BF16)
    send_v[:, 2 * c4 : 3 * c4] = matmul(order_below, four).astype(BF16)
    store = pltpu.make_async_copy(send_v, send, out_sem)
    store.start()
    c2 = w2_v.shape[1]
    for copy in copies[4:7]:
        copy.wait()
    hand_out(order_turn, matmul(hidden_v[1], w2_v[...]) + b2_v[...], sent, 0)
    for copy in copies[7:9]:
        copy.wait()
    for i in range(chunks):
        copies[9 + i].wait()
        same = matmul(hidden_v[2], ws_v[i]) + bs_v[:, i * CHUNK : (i + 1) * CHUNK]
        hand_out(order_turn, same, sent, c2 + i * CHUNK)
    store.wait()


def hand_out(order, projected, sent, at):
    moved = matmul(order, projected.astype(BF16)).astype(BF16)
    rows = sent[0].shape[0]
    for k, out in enumerate(sent):
        out[:, at : at + moved.shape[1]] = moved[k * rows : (k + 1) * rows]


def turn_kernel(low_count, *refs):
    lows, highs = refs[:low_count], refs[low_count:]
    rows = lows[0].shape[0] // len(highs)
    for h, high in enumerate(highs):
        for k, low in enumerate(lows):
            high[k * rows : (k + 1) * rows] = low[h * rows : (h + 1) * rows]


def fetch_kernel(w4, b4, b2, w4_v, b4_v, b2_v, sems):
    for copy in start_all([(w4, w4_v), (b4, b4_v), (b2, b2_v)], sems):
        copy.wait()


def join_kernel(
    arrived, places, w4, b4, wj_hbm, w2_hbm, joined, w2,
    wj, tiles_v, wide_v, acc_v, out_v, weight_sems, sems,
):
    weights = start_all([(wj_hbm, wj), (w2_hbm, w2)], weight_sems)
    widen(arrived, places, w4, b4, tiles_v, wide_v)
    weights[0].wait()
    stores = [
        convolve(chunk, wide_v, wj, joined, acc_v, out_v, sems) for chunk in range(arrived.shape[0] // GRID_W)
    ]
    weights[1].wait()
    for store in stores:
        store.wait()


def widen(arrived, places, w4, b4, tiles_v, wide_v):
    tok_dev, c4 = arrived.shape[0], w4.shape[0]
    row_count = tok_dev // GRID_W
    me = lax.axis_index("rows")
    top = jnp.where(me > 0, 1.0, 0.0)
    bottom = jnp.where(me < lax.axis_size("rows") - 1, 1.0, 0.0)
    bias = b4[...]
    feat = c4

    base = 3 * tok_dev
    tiles_v[0:base] = matmul(places[0:base], arrived[:, 0:c4]).astype(BF16)
    tiles_v[base : base + 3 * GRID_W] = matmul(places[base : base + 3 * GRID_W], arrived[:, c4 : 2 * c4]).astype(BF16)
    base += 3 * GRID_W
    tiles_v[base : base + 3 * GRID_W] = matmul(places[base : base + 3 * GRID_W], arrived[:, 2 * c4 : 3 * c4]).astype(BF16)

    left = jnp.where(iota((GRID_W, 1), 0) == 0, 0.0, 1.0)
    right = jnp.where(iota((GRID_W, 1), 0) == GRID_W - 1, 0.0, 1.0)

    def fill(first, stride, rows, tap, to, scale):
        size = rows * GRID_W
        for b in range(4):
            part = matmul(tiles_v[first : first + size], w4[:, (tap * 4 + b) * feat : (tap * 4 + b + 1) * feat]) + bias
            if scale is not None:
                part = part * scale
            for i in range(rows):
                wide_v[pl.ds(to(i) * GRID_W, GRID_W), (b + 1) * feat : (b + 2) * feat] = part[
                    i * GRID_W : (i + 1) * GRID_W
                ].astype(BF16)
        for b, shift, edge, block in ((3, 1, left, 0), (0, 2, right, 5)):
            start = first + shift * stride
            part = matmul(tiles_v[start : start + size], w4[:, (tap * 4 + b) * feat : (tap * 4 + b + 1) * feat]) + bias
            if scale is not None:
                part = part * scale
            for i in range(rows):
                wide_v[pl.ds(to(i) * GRID_W, GRID_W), block * feat : (block + 1) * feat] = (
                    part[i * GRID_W : (i + 1) * GRID_W] * edge
                ).astype(BF16)

    for tap in range(4):
        fill(0, tok_dev, row_count, tap, lambda i, tap=tap: 4 * i + tap + 1, None)
    fill(3 * tok_dev, GRID_W, 1, 3, lambda i: 0, top)
    fill(3 * tok_dev + 3 * GRID_W, GRID_W, 1, 0, lambda i: 4 * row_count + 1, bottom)


def convolve(chunk, wide_v, wj, joined, acc_v, out_v, sems):
    feat = wj.shape[2]
    for b in range(4):
        total = None
        for row_tap in range(3):
            first = (4 * chunk + row_tap) * GRID_W
            term = matmul(wide_v[first : first + 4 * GRID_W, b * feat : (b + 3) * feat], wj[row_tap])
            total = term if total is None else total + term
        for r in range(4):
            for block in range(feat // 128):
                acc_v[4 * chunk + r, block, pl.ds(b, GRID_W, 4), :] = total[
                    r * GRID_W : (r + 1) * GRID_W, block * 128 : (block + 1) * 128
                ]
    for r in range(4 * chunk, 4 * chunk + 4):
        for block in range(feat // 128):
            out_v[r, :, block * 128 : (block + 1) * 128] = acc_v[r, block].astype(BF16)
    rows = pl.ds(4 * chunk, 4)
    store = pltpu.make_async_copy(out_v.at[rows], joined.at[rows], sems.at[chunk])
    store.start()
    return store


def rest_kernel(places, w2, b2, *refs):
    arrived, (up_two, same, rows_v, acc_v, out_v, same_v, sems, same_sem) = refs[:-8], refs[-8:]
    rows = arrived[0].shape[0]
    for h, piece in enumerate(arrived):
        rows_v[h * rows : (h + 1) * rows] = piece[...]
    tok_dev = rows_v.shape[0]
    c2 = w2.shape[0]
    row_count = tok_dev // GRID_W
    place = places[places.shape[0] - tok_dev :]
    same_v[...] = matmul(place, rows_v[:, c2:]).astype(BF16)
    stores = [pltpu.make_async_copy(same_v, same, same_sem)]
    stores[0].start()
    tile = matmul(place, rows_v[:, 0:c2]).astype(BF16)
    bias = b2[...]
    for a in range(2):
        for b in range(2):
            part = matmul(tile, w2[:, (a * 2 + b) * c2 : (a * 2 + b + 1) * c2]) + bias
            for i in range(row_count):
                for block in range(c2 // 128):
                    acc_v[2 * i + a, block, pl.ds(b, GRID_W, 2), :] = part[
                        i * GRID_W : (i + 1) * GRID_W, block * 128 : (block + 1) * 128
                    ]
        for i in range(row_count):
            r = 2 * i + a
            for block in range(c2 // 128):
                out_v[r, :, block * 128 : (block + 1) * 128] = acc_v[r, block].astype(BF16)
            store = pltpu.make_async_copy(out_v.at[r], up_two.at[r], sems.at[r])
            store.start()
            stores.append(store)
    for store in stores:
        store.wait()


def body(
    hidden_states,
    cell_of,
    proj_four_weight,
    proj_four_bias,
    proj_two_weight,
    proj_two_bias,
    proj_same_weight,
    proj_same_bias,
    up4_weight,
    up4_bias,
    up2_weight,
    up2_bias,
    join_weight,
):
    _, tok_dev, hid = hidden_states.shape
    shards = lax.axis_size("rows")
    per_peer = tok_dev // shards
    row_count = tok_dev // GRID_W
    c4, c2, cs = proj_four_weight.shape[1], proj_two_weight.shape[1], proj_same_weight.shape[1]
    feat = join_weight.shape[3]
    table = cell_of.reshape(shards, tok_dev)
    place_rows = 4 * tok_dev + 6 * GRID_W
    shape = jax.ShapeDtypeStruct

    low = low_part(shards)
    high = shards // low
    biases = [bias.reshape(1, -1) for bias in (proj_four_bias, proj_two_bias, proj_same_bias)]
    inputs = (
        hidden_states,
        table,
        proj_four_weight,
        biases[0],
        proj_two_weight,
        biases[1],
        proj_same_weight,
        biases[2],
    )
    send, places, *sent = pl.pallas_call(
        functools.partial(project_kernel, low),
        out_shape=(pltpu.HBM((tok_dev, 3 * c4), BF16), pltpu.VMEM((place_rows, tok_dev), BF16))
        + (pltpu.VMEM((high * per_peer, c2 + cs), BF16),) * low,
        in_specs=[ANY] * 8,
        out_specs=(ANY,) + (VMEM,) * (1 + low),
        scratch_shapes=[
            pltpu.VMEM(hidden_states.shape, BF16),
            pltpu.VMEM(table.shape, jnp.int32),
            pltpu.VMEM((hid, c4), BF16),
            pltpu.VMEM((hid, c2), BF16),
            pltpu.VMEM((cs // CHUNK, hid, CHUNK), BF16),
            pltpu.VMEM((1, c4), F32),
            pltpu.VMEM((1, c2), F32),
            pltpu.VMEM((1, cs), F32),
            pltpu.VMEM((tok_dev, 3 * c4), BF16),
            pltpu.SemaphoreType.DMA((9 + cs // CHUNK,)),
            pltpu.SemaphoreType.DMA,
        ],
        compiler_params=pltpu.CompilerParams(vmem_limit_bytes=10 << 20),
        cost_estimate=pl.CostEstimate(flops=2 * tok_dev * hid * (c4 + c2 + cs), bytes_accessed=5 << 20, transcendentals=0),
        name="project",
    )(*(in_hbm(x) for x in inputs))

    def swap(piece, step):
        return lax.ppermute(piece, "rows", [(i, i ^ step) for i in range(shards)])

    crossed = [sent[0]] + [swap(sent[k], k) for k in range(1, low)]
    arrived = lax.all_to_all(
        send.reshape(shards, per_peer, 3 * c4), "rows", split_axis=0, concat_axis=0, tiled=True
    ).reshape(tok_dev, 3 * c4)
    turned = pl.pallas_call(
        functools.partial(turn_kernel, low),
        out_shape=(shape((low * per_peer, c2 + cs), BF16),) * high,
        in_specs=[VMEM] * low,
        out_specs=(VMEM,) * high,
        compiler_params=pltpu.CompilerParams(vmem_limit_bytes=4 << 20),
        cost_estimate=pl.CostEstimate(flops=1 << 26, bytes_accessed=1 << 20, transcendentals=0),
        name="turn",
    )(*crossed)
    landed = [turned[0]] + [swap(turned[h], h * low) for h in range(1, high)]

    weights = (up4_weight, up4_bias.reshape(1, -1), up2_bias.reshape(1, -1))
    w4, b4, b2 = pl.pallas_call(
        fetch_kernel,
        out_shape=tuple(pltpu.VMEM(w.shape, w.dtype) for w in weights),
        in_specs=[ANY] * 3,
        out_specs=(VMEM,) * 3,
        scratch_shapes=[pltpu.SemaphoreType.DMA((3,))],
        cost_estimate=pl.CostEstimate(flops=1 << 30, bytes_accessed=2 << 20, transcendentals=0),
        compiler_params=pltpu.CompilerParams(vmem_limit_bytes=4 << 20),
        name="fetch",
    )(*(in_hbm(w) for w in weights))

    out_rows = 4 * row_count
    joined, w2 = pl.pallas_call(
        join_kernel,
        out_shape=(
            shape((out_rows, 4 * GRID_W, feat), BF16),
            pltpu.VMEM(up2_weight.shape, BF16),
        ),
        in_specs=[VMEM] * 4 + [ANY] * 2,
        out_specs=(ANY, VMEM),
        scratch_shapes=[
            pltpu.VMEM((3, 3 * c4, feat), BF16),
            pltpu.VMEM((place_rows, c4), BF16),
            pltpu.VMEM(((out_rows + 2) * GRID_W, 6 * c4), BF16),
            pltpu.VMEM((out_rows, feat // 128, 4 * GRID_W, 128), F32),
            pltpu.VMEM((out_rows, 4 * GRID_W, feat), BF16),
            pltpu.SemaphoreType.DMA((2,)),
            pltpu.SemaphoreType.DMA((row_count,)),
        ],
        compiler_params=pltpu.CompilerParams(vmem_limit_bytes=20 << 20),
        cost_estimate=pl.CostEstimate(flops=4 << 30, bytes_accessed=4 << 20, transcendentals=0),
        name="join",
    )(arrived, places, w4, b4, in_hbm(join_weight.reshape(3, 3 * c4, feat)), in_hbm(up2_weight))
    upsampled_two, same_scale = pl.pallas_call(
        rest_kernel,
        out_shape=(shape((2 * row_count, 2 * GRID_W, c2), BF16), shape((tok_dev, cs), BF16)),
        in_specs=[VMEM] * (3 + high),
        out_specs=(ANY, ANY),
        scratch_shapes=[
            pltpu.VMEM((tok_dev, c2 + cs), BF16),
            pltpu.VMEM((2 * row_count, c2 // 128, 2 * GRID_W, 128), F32),
            pltpu.VMEM((2 * row_count, 2 * GRID_W, c2), BF16),
            pltpu.VMEM((tok_dev, cs), BF16),
            pltpu.SemaphoreType.DMA((2 * row_count,)),
            pltpu.SemaphoreType.DMA,
        ],
        compiler_params=pltpu.CompilerParams(vmem_limit_bytes=8 << 20),
        cost_estimate=pl.CostEstimate(flops=1 << 30, bytes_accessed=4 << 20, transcendentals=0),
        name="rest",
    )(places, w2, b2, *landed)
    return (joined, upsampled_two, same_scale.reshape(row_count, GRID_W, cs))


def solution(mesh):
    return jax.shard_map(
        body,
        mesh=mesh,
        in_specs=(P(None, ("img", "rows"), None),) + (P(),) * 12,
        out_specs=(P(("img", "rows"), None, None),) * 3,
        check_vma=False,
    )
```

```python
import functools

import jax
import jax.numpy as jnp
from jax import lax
from jax.experimental import pallas as pl
from jax.experimental.pallas import tpu as pltpu
from jax.sharding import PartitionSpec as P


GRID_W = 64
CHUNK = 512
F32 = jnp.float32
BF16 = jnp.bfloat16
ANY = pl.BlockSpec(memory_space=pl.ANY)
VMEM = pl.BlockSpec(memory_space=pltpu.VMEM)


def in_hbm(x):
    return pltpu.with_memory_space_constraint(x, pltpu.HBM)


def one_hot(mask):
    return jnp.where(mask, 1.0, 0.0).astype(BF16)


def iota(shape, dim):
    return lax.broadcasted_iota(jnp.int32, shape, dim)


def matmul(left, right):
    return jnp.dot(left, right, preferred_element_type=F32)


def column(row, size):
    same = iota((size, size), 0) == iota((size, size), 1)
    return jnp.sum(jnp.where(same, jnp.broadcast_to(row, (size, size)), 0.0), axis=1, keepdims=True)


def low_part(shards):
    return 1 << ((shards.bit_length()) // 2)


def landing(table, block, tok_dev, per_peer, flip=0):
    shards = table.shape[0]
    start = block * tok_dev
    inside = jnp.logical_and(table >= start, table < start + tok_dev)
    before = one_hot(iota((tok_dev, tok_dev), 0) < iota((tok_dev, tok_dev), 1))
    rank = matmul(one_hot(inside), before)
    place = (table - start).astype(F32)
    lane = iota((shards, tok_dev), 1)
    spread = jnp.zeros((shards, tok_dev), F32)
    for k in range(per_peer):
        hit = jnp.logical_and(inside, rank == float(k))
        found = jnp.sum(jnp.where(hit, place, 0.0), axis=1, keepdims=True)
        spread = spread + jnp.where(lax.rem(lane, per_peer) == k, found, 0.0)
    own = lax.div(lane, per_peer) == jnp.bitwise_xor(iota((shards, tok_dev), 0), flip)
    return jnp.sum(jnp.where(own, spread, 0.0), axis=0, keepdims=True).astype(jnp.int32)


def start_all(pairs, sems):
    copies = [pltpu.make_async_copy(src, dst, sems.at[i]) for i, (src, dst) in enumerate(pairs)]
    for copy in copies:
        copy.start()
    return copies


def project_kernel(low, hidden, table_hbm, w4, b4, w2, b2, ws, bs, send, places_v, *refs):
    sent = refs[:low]
    hidden_v, table_v, w4_v, w2_v, ws_v, b4_v, b2_v, bs_v, send_v, sems, out_sem = refs[low:]
    chunks = ws.shape[1] // CHUNK
    copies = start_all(
        [
            (table_hbm, table_v),
            (hidden.at[0], hidden_v.at[0]),
            (b4, b4_v),
            (w4, w4_v),
            (hidden.at[1], hidden_v.at[1]),
            (b2, b2_v),
            (w2, w2_v),
            (hidden.at[2], hidden_v.at[2]),
            (bs, bs_v),
        ]
        + [(ws.at[:, pl.ds(i * CHUNK, CHUNK)], ws_v.at[i]) for i in range(chunks)],
        sems,
    )
    shards, tok_dev = table_v.shape
    per_peer = tok_dev // shards
    me = lax.axis_index("rows")
    copies[0].wait()
    table = table_v[...]
    mine = table_v[pl.ds(me, 1), :]
    block_row = lax.div(mine, tok_dev)
    block_col = column(block_row.astype(F32), tok_dev).astype(jnp.int32)
    square = (tok_dev, tok_dev)
    earlier = jnp.logical_and(block_col == jnp.broadcast_to(block_row, square), iota(square, 0) < iota(square, 1))
    within = jnp.sum(jnp.where(earlier, 1.0, 0.0), axis=0, keepdims=True).astype(jnp.int32)
    slot = block_row * per_peer + within
    order = one_hot(iota(square, 0) == slot)

    apart = jnp.bitwise_xor(block_row, me)
    turn = lax.rem(apart, low) * (shards // low) + lax.div(apart, low)
    order_turn = one_hot(iota(square, 0) == turn * per_peer + within)

    own = landing(table, me, tok_dev, per_peer)
    above = landing(table, me - 1, tok_dev, per_peer)
    below = landing(table, me + 1, tok_dev, per_peer)
    cell = iota(square, 0)
    col = lax.rem(cell, GRID_W)
    edge = (GRID_W, tok_dev)
    edge_col = iota(edge, 0)
    last = edge_col + (tok_dev - GRID_W)
    places_v[0:tok_dev] = one_hot(cell == own)
    places_v[tok_dev : 2 * tok_dev] = one_hot(jnp.logical_and(cell == own + 1, col != 0))
    places_v[2 * tok_dev : 3 * tok_dev] = one_hot(jnp.logical_and(cell == own - 1, col != GRID_W - 1))
    base = 3 * tok_dev
    for source, target in ((above, last), (below, edge_col)):
        places_v[base : base + GRID_W] = one_hot(target == source)
        places_v[base + GRID_W : base + 2 * GRID_W] = one_hot(jnp.logical_and(target == source + 1, edge_col != 0))
        places_v[base + 2 * GRID_W : base + 3 * GRID_W] = one_hot(
            jnp.logical_and(target == source - 1, edge_col != GRID_W - 1)
        )
        base += 3 * GRID_W

    places_v[base : base + tok_dev] = one_hot(cell == landing(table, me, tok_dev, per_peer, me))

    c4, c2 = w4_v.shape[1], w2_v.shape[1]
    copies[1].wait()
    rows_four = matmul(order, hidden_v[0]).astype(BF16)
    copies[2].wait()
    copies[3].wait()
    four = (matmul(rows_four, w4_v[...]) + b4_v[...]).astype(BF16)
    blank = jnp.zeros((per_peer, c4), BF16)
    send_v[:, 0:c4] = four
    send_v[0:per_peer, c4 : 2 * c4] = blank
    send_v[per_peer:, c4 : 2 * c4] = four[: tok_dev - per_peer]
    send_v[: tok_dev - per_peer, 2 * c4 :] = four[per_peer:]
    send_v[tok_dev - per_peer :, 2 * c4 :] = blank
    store = pltpu.make_async_copy(send_v, send, out_sem)
    store.start()
    copies[4].wait()
    rows_two = matmul(order_turn, hidden_v[1]).astype(BF16)
    copies[5].wait()
    copies[6].wait()
    hand_out(matmul(rows_two, w2_v[...]) + b2_v[...], sent, 0)
    copies[7].wait()
    rows_same = matmul(order_turn, hidden_v[2]).astype(BF16)
    copies[8].wait()
    for i in range(chunks):
        copies[9 + i].wait()
        same = matmul(rows_same, ws_v[i]) + bs_v[:, i * CHUNK : (i + 1) * CHUNK]
        hand_out(same, sent, c2 + i * CHUNK)
    store.wait()


def hand_out(projected, sent, at):
    moved = projected.astype(BF16)
    rows = sent[0].shape[0]
    for k, out in enumerate(sent):
        out[:, at : at + moved.shape[1]] = moved[k * rows : (k + 1) * rows]


def turn_kernel(low_count, *refs):
    lows, highs = refs[:low_count], refs[low_count:]
    rows = lows[0].shape[0] // len(highs)
    for h, high in enumerate(highs):
        for k, low in enumerate(lows):
            high[k * rows : (k + 1) * rows] = low[h * rows : (h + 1) * rows]


def fetch_kernel(w4, b4, b2, w4_v, b4_v, b2_v, sems):
    for copy in start_all([(w4, w4_v), (b4, b4_v), (b2, b2_v)], sems):
        copy.wait()


def join_kernel(
    arrived, places, w4, b4, wj_hbm, w2_hbm, joined, w2,
    wj, tiles_v, wide_v, acc_v, out_v, weight_sems, sems,
):
    weights = [pltpu.make_async_copy(wj_hbm, wj, weight_sems.at[0]), pltpu.make_async_copy(w2_hbm, w2, weight_sems.at[1])]
    weights[0].start()
    widen(arrived, places, w4, b4, tiles_v, wide_v)
    weights[0].wait()
    weights[1].start()
    stores = [
        convolve(chunk, wide_v, wj, joined, acc_v, out_v, sems) for chunk in range(arrived.shape[0] // GRID_W)
    ]
    weights[1].wait()
    for store in stores:
        store.wait()


def widen(arrived, places, w4, b4, tiles_v, wide_v):
    tok_dev, c4 = arrived.shape[0], w4.shape[0]
    row_count = tok_dev // GRID_W
    me = lax.axis_index("rows")
    top = jnp.where(me > 0, 1.0, 0.0)
    bottom = jnp.where(me < lax.axis_size("rows") - 1, 1.0, 0.0)
    bias = b4[...]
    feat = c4

    base = 3 * tok_dev
    tiles_v[0:base] = matmul(places[0:base], arrived[:, 0:c4]).astype(BF16)
    tiles_v[base : base + 3 * GRID_W] = matmul(places[base : base + 3 * GRID_W], arrived[:, c4 : 2 * c4]).astype(BF16)
    base += 3 * GRID_W
    tiles_v[base : base + 3 * GRID_W] = matmul(places[base : base + 3 * GRID_W], arrived[:, 2 * c4 : 3 * c4]).astype(BF16)

    left = jnp.where(iota((GRID_W, 1), 0) == 0, 0.0, 1.0)
    right = jnp.where(iota((GRID_W, 1), 0) == GRID_W - 1, 0.0, 1.0)

    def fill(first, stride, rows, tap, to, scale):
        size = rows * GRID_W
        for b in range(4):
            part = matmul(tiles_v[first : first + size], w4[:, (tap * 4 + b) * feat : (tap * 4 + b + 1) * feat]) + bias
            if scale is not None:
                part = part * scale
            for i in range(rows):
                wide_v[pl.ds(to(i) * GRID_W, GRID_W), (b + 1) * feat : (b + 2) * feat] = part[
                    i * GRID_W : (i + 1) * GRID_W
                ].astype(BF16)
        for b, shift, edge, block in ((3, 1, left, 0), (0, 2, right, 5)):
            start = first + shift * stride
            part = matmul(tiles_v[start : start + size], w4[:, (tap * 4 + b) * feat : (tap * 4 + b + 1) * feat]) + bias
            if scale is not None:
                part = part * scale
            for i in range(rows):
                wide_v[pl.ds(to(i) * GRID_W, GRID_W), block * feat : (block + 1) * feat] = (
                    part[i * GRID_W : (i + 1) * GRID_W] * edge
                ).astype(BF16)

    for tap in range(4):
        fill(0, tok_dev, row_count, tap, lambda i, tap=tap: 4 * i + tap + 1, None)
    fill(3 * tok_dev, GRID_W, 1, 3, lambda i: 0, top)
    fill(3 * tok_dev + 3 * GRID_W, GRID_W, 1, 0, lambda i: 4 * row_count + 1, bottom)


def convolve(chunk, wide_v, wj, joined, acc_v, out_v, sems):
    feat = wj.shape[2]
    for b in range(4):
        total = None
        for row_tap in range(3):
            first = (4 * chunk + row_tap) * GRID_W
            term = matmul(wide_v[first : first + 4 * GRID_W, b * feat : (b + 3) * feat], wj[row_tap])
            total = term if total is None else total + term
        for r in range(4):
            for block in range(feat // 128):
                acc_v[4 * chunk + r, block, pl.ds(b, GRID_W, 4), :] = total[
                    r * GRID_W : (r + 1) * GRID_W, block * 128 : (block + 1) * 128
                ]
    for r in range(4 * chunk, 4 * chunk + 4):
        for block in range(feat // 128):
            out_v[r, :, block * 128 : (block + 1) * 128] = acc_v[r, block].astype(BF16)
    rows = pl.ds(4 * chunk, 4)
    store = pltpu.make_async_copy(out_v.at[rows], joined.at[rows], sems.at[chunk])
    store.start()
    return store


def rest_kernel(places, w2, b2, *refs):
    arrived, (up_two, same, rows_v, acc_v, out_v, same_v, sems, same_sem) = refs[:-8], refs[-8:]
    rows = arrived[0].shape[0]
    for h, piece in enumerate(arrived):
        rows_v[h * rows : (h + 1) * rows] = piece[...]
    tok_dev = rows_v.shape[0]
    c2 = w2.shape[0]
    row_count = tok_dev // GRID_W
    place = places[places.shape[0] - tok_dev :]
    same_v[...] = matmul(place, rows_v[:, c2:]).astype(BF16)
    stores = [pltpu.make_async_copy(same_v, same, same_sem)]
    stores[0].start()
    tile = matmul(place, rows_v[:, 0:c2]).astype(BF16)
    bias = b2[...]
    for a in range(2):
        for b in range(2):
            part = matmul(tile, w2[:, (a * 2 + b) * c2 : (a * 2 + b + 1) * c2]) + bias
            for i in range(row_count):
                for block in range(c2 // 128):
                    acc_v[2 * i + a, block, pl.ds(b, GRID_W, 2), :] = part[
                        i * GRID_W : (i + 1) * GRID_W, block * 128 : (block + 1) * 128
                    ]
        for i in range(row_count):
            r = 2 * i + a
            for block in range(c2 // 128):
                out_v[r, :, block * 128 : (block + 1) * 128] = acc_v[r, block].astype(BF16)
            store = pltpu.make_async_copy(out_v.at[r], up_two.at[r], sems.at[r])
            store.start()
            stores.append(store)
    for store in stores:
        store.wait()


def body(
    hidden_states,
    cell_of,
    proj_four_weight,
    proj_four_bias,
    proj_two_weight,
    proj_two_bias,
    proj_same_weight,
    proj_same_bias,
    up4_weight,
    up4_bias,
    up2_weight,
    up2_bias,
    join_weight,
):
    _, tok_dev, hid = hidden_states.shape
    shards = lax.axis_size("rows")
    per_peer = tok_dev // shards
    row_count = tok_dev // GRID_W
    c4, c2, cs = proj_four_weight.shape[1], proj_two_weight.shape[1], proj_same_weight.shape[1]
    feat = join_weight.shape[3]
    table = cell_of.reshape(shards, tok_dev)
    place_rows = 4 * tok_dev + 6 * GRID_W
    shape = jax.ShapeDtypeStruct

    low = low_part(shards)
    high = shards // low
    biases = [bias.reshape(1, -1) for bias in (proj_four_bias, proj_two_bias, proj_same_bias)]
    inputs = (
        hidden_states,
        table,
        proj_four_weight,
        biases[0],
        proj_two_weight,
        biases[1],
        proj_same_weight,
        biases[2],
    )
    send, places, *sent = pl.pallas_call(
        functools.partial(project_kernel, low),
        out_shape=(pltpu.HBM((tok_dev, 3 * c4), BF16), pltpu.VMEM((place_rows, tok_dev), BF16))
        + (pltpu.VMEM((high * per_peer, c2 + cs), BF16),) * low,
        in_specs=[ANY] * 8,
        out_specs=(ANY,) + (VMEM,) * (1 + low),
        scratch_shapes=[
            pltpu.VMEM(hidden_states.shape, BF16),
            pltpu.VMEM(table.shape, jnp.int32),
            pltpu.VMEM((hid, c4), BF16),
            pltpu.VMEM((hid, c2), BF16),
            pltpu.VMEM((cs // CHUNK, hid, CHUNK), BF16),
            pltpu.VMEM((1, c4), F32),
            pltpu.VMEM((1, c2), F32),
            pltpu.VMEM((1, cs), F32),
            pltpu.VMEM((tok_dev, 3 * c4), BF16),
            pltpu.SemaphoreType.DMA((9 + cs // CHUNK,)),
            pltpu.SemaphoreType.DMA,
        ],
        compiler_params=pltpu.CompilerParams(vmem_limit_bytes=10 << 20),
        cost_estimate=pl.CostEstimate(flops=2 * tok_dev * hid * (c4 + c2 + cs), bytes_accessed=5 << 20, transcendentals=0),
        name="project",
    )(*(in_hbm(x) for x in inputs))

    def swap(piece, step):
        return lax.ppermute(piece, "rows", [(i, i ^ step) for i in range(shards)])

    crossed = [sent[0]] + [swap(sent[k], k) for k in range(1, low)]
    arrived = lax.all_to_all(
        send.reshape(shards, per_peer, 3 * c4), "rows", split_axis=0, concat_axis=0, tiled=True
    ).reshape(tok_dev, 3 * c4)
    turned = pl.pallas_call(
        functools.partial(turn_kernel, low),
        out_shape=(shape((low * per_peer, c2 + cs), BF16),) * high,
        in_specs=[VMEM] * low,
        out_specs=(VMEM,) * high,
        compiler_params=pltpu.CompilerParams(vmem_limit_bytes=4 << 20),
        cost_estimate=pl.CostEstimate(flops=1 << 26, bytes_accessed=1 << 20, transcendentals=0),
        name="turn",
    )(*crossed)
    landed = [turned[0]] + [swap(turned[h], h * low) for h in range(1, high)]

    weights = (up4_weight, up4_bias.reshape(1, -1), up2_bias.reshape(1, -1))
    w4, b4, b2 = pl.pallas_call(
        fetch_kernel,
        out_shape=tuple(pltpu.VMEM(w.shape, w.dtype) for w in weights),
        in_specs=[ANY] * 3,
        out_specs=(VMEM,) * 3,
        scratch_shapes=[pltpu.SemaphoreType.DMA((3,))],
        cost_estimate=pl.CostEstimate(flops=1 << 30, bytes_accessed=2 << 20, transcendentals=0),
        compiler_params=pltpu.CompilerParams(vmem_limit_bytes=4 << 20),
        name="fetch",
    )(*(in_hbm(w) for w in weights))

    out_rows = 4 * row_count
    joined, w2 = pl.pallas_call(
        join_kernel,
        out_shape=(
            shape((out_rows, 4 * GRID_W, feat), BF16),
            pltpu.VMEM(up2_weight.shape, BF16),
        ),
        in_specs=[VMEM] * 4 + [ANY] * 2,
        out_specs=(ANY, VMEM),
        scratch_shapes=[
            pltpu.VMEM((3, 3 * c4, feat), BF16),
            pltpu.VMEM((place_rows, c4), BF16),
            pltpu.VMEM(((out_rows + 2) * GRID_W, 6 * c4), BF16),
            pltpu.VMEM((out_rows, feat // 128, 4 * GRID_W, 128), F32),
            pltpu.VMEM((out_rows, 4 * GRID_W, feat), BF16),
            pltpu.SemaphoreType.DMA((2,)),
            pltpu.SemaphoreType.DMA((row_count,)),
        ],
        compiler_params=pltpu.CompilerParams(vmem_limit_bytes=20 << 20),
        cost_estimate=pl.CostEstimate(flops=4 << 30, bytes_accessed=4 << 20, transcendentals=0),
        name="join",
    )(arrived, places, w4, b4, in_hbm(join_weight.reshape(3, 3 * c4, feat)), in_hbm(up2_weight))
    upsampled_two, same_scale = pl.pallas_call(
        rest_kernel,
        out_shape=(shape((2 * row_count, 2 * GRID_W, c2), BF16), shape((tok_dev, cs), BF16)),
        in_specs=[VMEM] * (3 + high),
        out_specs=(ANY, ANY),
        scratch_shapes=[
            pltpu.VMEM((tok_dev, c2 + cs), BF16),
            pltpu.VMEM((2 * row_count, c2 // 128, 2 * GRID_W, 128), F32),
            pltpu.VMEM((2 * row_count, 2 * GRID_W, c2), BF16),
            pltpu.VMEM((tok_dev, cs), BF16),
            pltpu.SemaphoreType.DMA((2 * row_count,)),
            pltpu.SemaphoreType.DMA,
        ],
        compiler_params=pltpu.CompilerParams(vmem_limit_bytes=8 << 20),
        cost_estimate=pl.CostEstimate(flops=1 << 30, bytes_accessed=4 << 20, transcendentals=0),
        name="rest",
    )(places, w2, b2, *landed)
    return (joined, upsampled_two, same_scale.reshape(row_count, GRID_W, cs))


def solution(mesh):
    return jax.shard_map(
        body,
        mesh=mesh,
        in_specs=(P(None, ("img", "rows"), None),) + (P(),) * 12,
        out_specs=(P(("img", "rows"), None, None),) * 3,
        check_vma=False,
    )
```

```python
import functools

import jax
import jax.numpy as jnp
from jax import lax
from jax.experimental import pallas as pl
from jax.experimental.pallas import tpu as pltpu
from jax.sharding import PartitionSpec as P


GRID_W = 64
CHUNK = 512
F32 = jnp.float32
BF16 = jnp.bfloat16
ANY = pl.BlockSpec(memory_space=pl.ANY)
VMEM = pl.BlockSpec(memory_space=pltpu.VMEM)


def in_hbm(x):
    return pltpu.with_memory_space_constraint(x, pltpu.HBM)


def one_hot(mask):
    return jnp.where(mask, 1.0, 0.0).astype(BF16)


def iota(shape, dim):
    return lax.broadcasted_iota(jnp.int32, shape, dim)


def matmul(left, right):
    return jnp.dot(left, right, preferred_element_type=F32)


def column(row, size):
    same = iota((size, size), 0) == iota((size, size), 1)
    return jnp.sum(jnp.where(same, jnp.broadcast_to(row, (size, size)), 0.0), axis=1, keepdims=True)


def low_part(shards):
    return 1 << ((shards.bit_length()) // 2)


def landing(table, block, tok_dev, per_peer, seat):
    shards = table.shape[0]
    start = block * tok_dev
    inside = jnp.logical_and(table >= start, table < start + tok_dev)
    before = one_hot(iota((tok_dev, tok_dev), 0) < iota((tok_dev, tok_dev), 1))
    rank = matmul(one_hot(inside), before)
    place = (table - start).astype(F32)
    lane = iota((shards, tok_dev), 1)
    spread = jnp.zeros((shards, tok_dev), F32)
    for k in range(per_peer):
        hit = jnp.logical_and(inside, rank == float(k))
        found = jnp.sum(jnp.where(hit, place, 0.0), axis=1, keepdims=True)
        spread = spread + jnp.where(lax.rem(lane, per_peer) == k, found, 0.0)
    own = lax.div(lane, per_peer) == seat
    return jnp.sum(jnp.where(own, spread, 0.0), axis=0, keepdims=True).astype(jnp.int32)


def start_all(pairs, sems):
    copies = [pltpu.make_async_copy(src, dst, sems.at[i]) for i, (src, dst) in enumerate(pairs)]
    for copy in copies:
        copy.start()
    return copies


def project_kernel(low, hidden, table_hbm, w4, b4, w2, b2, ws, bs, places_v, *refs):
    high = (len(refs) - 9) - low
    sent_four, sent = refs[:high], refs[high : high + low]
    hidden_v, table_v, w4_v, w2_v, ws_v, b4_v, b2_v, bs_v, sems = refs[high + low :]
    chunks = ws.shape[1] // CHUNK
    copies = start_all(
        [
            (table_hbm, table_v),
            (hidden.at[0], hidden_v.at[0]),
            (b4, b4_v),
            (w4, w4_v),
            (hidden.at[1], hidden_v.at[1]),
            (b2, b2_v),
            (w2, w2_v),
            (hidden.at[2], hidden_v.at[2]),
            (bs, bs_v),
        ]
        + [(ws.at[:, pl.ds(i * CHUNK, CHUNK)], ws_v.at[i]) for i in range(chunks)],
        sems,
    )
    shards, tok_dev = table_v.shape
    per_peer = tok_dev // shards
    me = lax.axis_index("rows")
    copies[0].wait()
    table = table_v[...]
    mine = table_v[pl.ds(me, 1), :]
    block_row = lax.div(mine, tok_dev)
    block_col = column(block_row.astype(F32), tok_dev).astype(jnp.int32)
    square = (tok_dev, tok_dev)
    earlier = jnp.logical_and(block_col == jnp.broadcast_to(block_row, square), iota(square, 0) < iota(square, 1))
    within = jnp.sum(jnp.where(earlier, 1.0, 0.0), axis=0, keepdims=True).astype(jnp.int32)
    row = iota(square, 0)
    apart = jnp.bitwise_xor(block_row, me)
    order_low = one_hot(row == (lax.rem(apart, low) * high + lax.div(apart, low)) * per_peer + within)
    orders = [one_hot(row == jnp.bitwise_xor(block_row + step, me) * per_peer + within) for step in (0, 1, -1)]
    order_high = jnp.concatenate(orders, axis=0)

    seat_low = jnp.bitwise_xor(iota((shards, tok_dev), 0), me)
    seat_high = lax.rem(seat_low, low) * high + lax.div(seat_low, low)
    own = landing(table, me, tok_dev, per_peer, seat_high)
    above = landing(table, me - 1, tok_dev, per_peer, seat_high)
    below = landing(table, me + 1, tok_dev, per_peer, seat_high)
    cell = iota(square, 0)
    col = lax.rem(cell, GRID_W)
    edge = (GRID_W, tok_dev)
    edge_col = iota(edge, 0)
    last = edge_col + (tok_dev - GRID_W)
    places_v[0:tok_dev] = one_hot(cell == own)
    places_v[tok_dev : 2 * tok_dev] = one_hot(jnp.logical_and(cell == own + 1, col != 0))
    places_v[2 * tok_dev : 3 * tok_dev] = one_hot(jnp.logical_and(cell == own - 1, col != GRID_W - 1))
    base = 3 * tok_dev
    for source, target in ((above, last), (below, edge_col)):
        places_v[base : base + GRID_W] = one_hot(target == source)
        places_v[base + GRID_W : base + 2 * GRID_W] = one_hot(jnp.logical_and(target == source + 1, edge_col != 0))
        places_v[base + 2 * GRID_W : base + 3 * GRID_W] = one_hot(
            jnp.logical_and(target == source - 1, edge_col != GRID_W - 1)
        )
        base += 3 * GRID_W

    places_v[base : base + tok_dev] = one_hot(cell == landing(table, me, tok_dev, per_peer, seat_low))

    c4, c2 = w4_v.shape[1], w2_v.shape[1]
    for copy in copies[1:4]:
        copy.wait()
    four = (matmul(hidden_v[0], w4_v[...]) + b4_v[...]).astype(BF16)
    moved = matmul(order_high, four)
    for i in range(3):
        hand_out(moved[i * tok_dev : (i + 1) * tok_dev], sent_four, i * c4)
    copies[4].wait()
    rows_two = matmul(order_low, hidden_v[1]).astype(BF16)
    copies[5].wait()
    copies[6].wait()
    hand_out(matmul(rows_two, w2_v[...]) + b2_v[...], sent, 0)
    copies[7].wait()
    rows_same = matmul(order_low, hidden_v[2]).astype(BF16)
    copies[8].wait()
    for i in range(chunks):
        copies[9 + i].wait()
        same = matmul(rows_same, ws_v[i]) + bs_v[:, i * CHUNK : (i + 1) * CHUNK]
        hand_out(same, sent, c2 + i * CHUNK)


def hand_out(projected, sent, at):
    moved = projected.astype(BF16)
    rows = sent[0].shape[0]
    for k, out in enumerate(sent):
        out[:, at : at + moved.shape[1]] = moved[k * rows : (k + 1) * rows]


def turn_kernel(count, *refs):
    arrived, leaving = refs[:count], refs[count:]
    rows = arrived[0].shape[0] // len(leaving)
    for to, message in enumerate(leaving):
        for come, piece in enumerate(arrived):
            message[come * rows : (come + 1) * rows] = piece[to * rows : (to + 1) * rows]


def fetch_kernel(*refs):
    count = len(refs) // 2
    for copy in start_all(list(zip(refs[:count], refs[count:-1])), refs[-1]):
        copy.wait()


def join_kernel(places, w4, b4, wj, *refs):
    pieces, (joined, rows_v, tiles_v, wide_v, acc_v, out_v, sems) = refs[:-7], refs[-7:]
    gather_rows(pieces, rows_v)
    widen(rows_v, places, w4, b4, tiles_v, wide_v)
    stores = [convolve(chunk, wide_v, wj, joined, acc_v, out_v, sems) for chunk in range(rows_v.shape[0] // GRID_W)]
    for store in stores:
        store.wait()


def gather_rows(pieces, rows_v):
    rows = pieces[0].shape[0]
    for i, piece in enumerate(pieces):
        rows_v[i * rows : (i + 1) * rows] = piece[...]


def widen(arrived, places, w4, b4, tiles_v, wide_v):
    tok_dev, c4 = arrived.shape[0], w4.shape[0]
    row_count = tok_dev // GRID_W
    me = lax.axis_index("rows")
    top = jnp.where(me > 0, 1.0, 0.0)
    bottom = jnp.where(me < lax.axis_size("rows") - 1, 1.0, 0.0)
    bias = b4[...]
    feat = c4

    base = 3 * tok_dev
    tiles_v[0:base] = matmul(places[0:base], arrived[:, 0:c4]).astype(BF16)
    tiles_v[base : base + 3 * GRID_W] = matmul(places[base : base + 3 * GRID_W], arrived[:, c4 : 2 * c4]).astype(BF16)
    base += 3 * GRID_W
    tiles_v[base : base + 3 * GRID_W] = matmul(places[base : base + 3 * GRID_W], arrived[:, 2 * c4 : 3 * c4]).astype(BF16)

    left = jnp.where(iota((GRID_W, 1), 0) == 0, 0.0, 1.0)
    right = jnp.where(iota((GRID_W, 1), 0) == GRID_W - 1, 0.0, 1.0)

    def fill(first, stride, rows, tap, to, scale):
        size = rows * GRID_W
        for b in range(4):
            part = matmul(tiles_v[first : first + size], w4[:, (tap * 4 + b) * feat : (tap * 4 + b + 1) * feat]) + bias
            if scale is not None:
                part = part * scale
            for i in range(rows):
                wide_v[pl.ds(to(i) * GRID_W, GRID_W), (b + 1) * feat : (b + 2) * feat] = part[
                    i * GRID_W : (i + 1) * GRID_W
                ].astype(BF16)
        for b, shift, edge, block in ((3, 1, left, 0), (0, 2, right, 5)):
            start = first + shift * stride
            part = matmul(tiles_v[start : start + size], w4[:, (tap * 4 + b) * feat : (tap * 4 + b + 1) * feat]) + bias
            if scale is not None:
                part = part * scale
            for i in range(rows):
                wide_v[pl.ds(to(i) * GRID_W, GRID_W), block * feat : (block + 1) * feat] = (
                    part[i * GRID_W : (i + 1) * GRID_W] * edge
                ).astype(BF16)

    for tap in range(4):
        fill(0, tok_dev, row_count, tap, lambda i, tap=tap: 4 * i + tap + 1, None)
    fill(3 * tok_dev, GRID_W, 1, 3, lambda i: 0, top)
    fill(3 * tok_dev + 3 * GRID_W, GRID_W, 1, 0, lambda i: 4 * row_count + 1, bottom)


def convolve(chunk, wide_v, wj, joined, acc_v, out_v, sems):
    feat = wj.shape[2]
    for b in range(4):
        total = None
        for row_tap in range(3):
            first = (4 * chunk + row_tap) * GRID_W
            term = matmul(wide_v[first : first + 4 * GRID_W, b * feat : (b + 3) * feat], wj[row_tap])
            total = term if total is None else total + term
        for r in range(4):
            for block in range(feat // 128):
                acc_v[4 * chunk + r, block, pl.ds(b, GRID_W, 4), :] = total[
                    r * GRID_W : (r + 1) * GRID_W, block * 128 : (block + 1) * 128
                ]
    for r in range(4 * chunk, 4 * chunk + 4):
        for block in range(feat // 128):
            out_v[r, :, block * 128 : (block + 1) * 128] = acc_v[r, block].astype(BF16)
    rows = pl.ds(4 * chunk, 4)
    store = pltpu.make_async_copy(out_v.at[rows], joined.at[rows], sems.at[chunk])
    store.start()
    return store


def rest_kernel(places, w2, b2, *refs):
    arrived, (up_two, same, rows_v, acc_v, out_v, same_v, sems, same_sem) = refs[:-8], refs[-8:]
    gather_rows(arrived, rows_v)
    tok_dev = rows_v.shape[0]
    c2 = w2.shape[0]
    row_count = tok_dev // GRID_W
    place = places[places.shape[0] - tok_dev :]
    same_v[...] = matmul(place, rows_v[:, c2:]).astype(BF16)
    stores = [pltpu.make_async_copy(same_v, same, same_sem)]
    stores[0].start()
    tile = matmul(place, rows_v[:, 0:c2]).astype(BF16)
    bias = b2[...]
    for a in range(2):
        for b in range(2):
            part = matmul(tile, w2[:, (a * 2 + b) * c2 : (a * 2 + b + 1) * c2]) + bias
            for i in range(row_count):
                for block in range(c2 // 128):
                    acc_v[2 * i + a, block, pl.ds(b, GRID_W, 2), :] = part[
                        i * GRID_W : (i + 1) * GRID_W, block * 128 : (block + 1) * 128
                    ]
        for i in range(row_count):
            r = 2 * i + a
            for block in range(c2 // 128):
                out_v[r, :, block * 128 : (block + 1) * 128] = acc_v[r, block].astype(BF16)
            store = pltpu.make_async_copy(out_v.at[r], up_two.at[r], sems.at[r])
            store.start()
            stores.append(store)
    for store in stores:
        store.wait()


def body(
    hidden_states,
    cell_of,
    proj_four_weight,
    proj_four_bias,
    proj_two_weight,
    proj_two_bias,
    proj_same_weight,
    proj_same_bias,
    up4_weight,
    up4_bias,
    up2_weight,
    up2_bias,
    join_weight,
):
    _, tok_dev, hid = hidden_states.shape
    shards = lax.axis_size("rows")
    per_peer = tok_dev // shards
    row_count = tok_dev // GRID_W
    c4, c2, cs = proj_four_weight.shape[1], proj_two_weight.shape[1], proj_same_weight.shape[1]
    feat = join_weight.shape[3]
    table = cell_of.reshape(shards, tok_dev)
    place_rows = 4 * tok_dev + 6 * GRID_W
    shape = jax.ShapeDtypeStruct

    low = low_part(shards)
    high = shards // low
    biases = [bias.reshape(1, -1) for bias in (proj_four_bias, proj_two_bias, proj_same_bias)]
    inputs = (
        hidden_states,
        table,
        proj_four_weight,
        biases[0],
        proj_two_weight,
        biases[1],
        proj_same_weight,
        biases[2],
    )
    four_shape = (low * per_peer, 3 * c4)
    rest_shape = (high * per_peer, c2 + cs)
    places, *sent = pl.pallas_call(
        functools.partial(project_kernel, low),
        out_shape=(pltpu.VMEM((place_rows, tok_dev), BF16),)
        + (pltpu.VMEM(four_shape, BF16),) * high
        + (pltpu.VMEM(rest_shape, BF16),) * low,
        in_specs=[ANY] * 8,
        out_specs=(VMEM,) * (1 + high + low),
        scratch_shapes=[
            pltpu.VMEM(hidden_states.shape, BF16),
            pltpu.VMEM(table.shape, jnp.int32),
            pltpu.VMEM((hid, c4), BF16),
            pltpu.VMEM((hid, c2), BF16),
            pltpu.VMEM((cs // CHUNK, hid, CHUNK), BF16),
            pltpu.VMEM((1, c4), F32),
            pltpu.VMEM((1, c2), F32),
            pltpu.VMEM((1, cs), F32),
            pltpu.SemaphoreType.DMA((9 + cs // CHUNK,)),
        ],
        compiler_params=pltpu.CompilerParams(vmem_limit_bytes=10 << 20),
        cost_estimate=pl.CostEstimate(flops=2 * tok_dev * hid * (c4 + c2 + cs), bytes_accessed=5 << 20, transcendentals=0),
        name="project",
    )(*(in_hbm(x) for x in inputs))

    def swap(pieces, unit):
        return [pieces[0]] + [
            lax.ppermute(piece, "rows", [(i, i ^ (step * unit)) for i in range(shards)])
            for step, piece in enumerate(pieces[1:], 1)
        ]

    def turn(pieces, out_shape, count):
        return pl.pallas_call(
            functools.partial(turn_kernel, len(pieces)),
            out_shape=(pltpu.VMEM(out_shape, BF16),) * count,
            in_specs=[VMEM] * len(pieces),
            out_specs=(VMEM,) * count,
            compiler_params=pltpu.CompilerParams(vmem_limit_bytes=4 << 20),
            cost_estimate=pl.CostEstimate(flops=1 << 26, bytes_accessed=1 << 20, transcendentals=0),
            name="turn",
        )(*pieces)

    rest = swap(sent[high:], 1)
    four = swap(sent[:high], low)
    rest = turn(rest, (low * per_peer, c2 + cs), high)
    rest = swap(rest, low)
    four = turn(four, (high * per_peer, 3 * c4), low)
    four = swap(four, 1)

    weights = (
        up4_weight,
        up4_bias.reshape(1, -1),
        join_weight.reshape(3, 3 * c4, feat),
        up2_weight,
        up2_bias.reshape(1, -1),
    )
    w4, b4, wj, w2, b2 = pl.pallas_call(
        fetch_kernel,
        out_shape=tuple(pltpu.VMEM(w.shape, w.dtype) for w in weights),
        in_specs=[ANY] * 5,
        out_specs=(VMEM,) * 5,
        scratch_shapes=[pltpu.SemaphoreType.DMA((5,))],
        cost_estimate=pl.CostEstimate(flops=1 << 30, bytes_accessed=5 << 20, transcendentals=0),
        compiler_params=pltpu.CompilerParams(vmem_limit_bytes=8 << 20),
        name="fetch",
    )(*(in_hbm(w) for w in weights))

    out_rows = 4 * row_count
    joined = pl.pallas_call(
        join_kernel,
        out_shape=shape((out_rows, 4 * GRID_W, feat), BF16),
        in_specs=[VMEM] * (4 + low),
        out_specs=ANY,
        scratch_shapes=[
            pltpu.VMEM((tok_dev, 3 * c4), BF16),
            pltpu.VMEM((place_rows, c4), BF16),
            pltpu.VMEM(((out_rows + 2) * GRID_W, 6 * c4), BF16),
            pltpu.VMEM((out_rows, feat // 128, 4 * GRID_W, 128), F32),
            pltpu.VMEM((out_rows, 4 * GRID_W, feat), BF16),
            pltpu.SemaphoreType.DMA((row_count,)),
        ],
        compiler_params=pltpu.CompilerParams(vmem_limit_bytes=20 << 20),
        cost_estimate=pl.CostEstimate(flops=4 << 30, bytes_accessed=4 << 20, transcendentals=0),
        name="join",
    )(places, w4, b4, wj, *four)
    upsampled_two, same_scale = pl.pallas_call(
        rest_kernel,
        out_shape=(shape((2 * row_count, 2 * GRID_W, c2), BF16), shape((tok_dev, cs), BF16)),
        in_specs=[VMEM] * (3 + len(rest)),
        out_specs=(ANY, ANY),
        scratch_shapes=[
            pltpu.VMEM((tok_dev, c2 + cs), BF16),
            pltpu.VMEM((2 * row_count, c2 // 128, 2 * GRID_W, 128), F32),
            pltpu.VMEM((2 * row_count, 2 * GRID_W, c2), BF16),
            pltpu.VMEM((tok_dev, cs), BF16),
            pltpu.SemaphoreType.DMA((2 * row_count,)),
            pltpu.SemaphoreType.DMA,
        ],
        compiler_params=pltpu.CompilerParams(vmem_limit_bytes=8 << 20),
        cost_estimate=pl.CostEstimate(flops=1 << 30, bytes_accessed=4 << 20, transcendentals=0),
        name="rest",
    )(places, w2, b2, *rest)
    return (joined, upsampled_two, same_scale.reshape(row_count, GRID_W, cs))


def solution(mesh):
    return jax.shard_map(
        body,
        mesh=mesh,
        in_specs=(P(None, ("img", "rows"), None),) + (P(),) * 12,
        out_specs=(P(("img", "rows"), None, None),) * 3,
        check_vma=False,
    )
```

```python
import functools

import jax
import jax.numpy as jnp
from jax import lax
from jax.experimental import pallas as pl
from jax.experimental.pallas import tpu as pltpu
from jax.sharding import PartitionSpec as P


GRID_W = 64
CHUNK = 512
F32 = jnp.float32
BF16 = jnp.bfloat16
ANY = pl.BlockSpec(memory_space=pl.ANY)
VMEM = pl.BlockSpec(memory_space=pltpu.VMEM)


def in_hbm(x):
    return pltpu.with_memory_space_constraint(x, pltpu.HBM)


def one_hot(mask):
    return jnp.where(mask, 1.0, 0.0).astype(BF16)


def iota(shape, dim):
    return lax.broadcasted_iota(jnp.int32, shape, dim)


def matmul(left, right):
    return jnp.dot(left, right, preferred_element_type=F32)


def column(row, size):
    same = iota((size, size), 0) == iota((size, size), 1)
    return jnp.sum(jnp.where(same, jnp.broadcast_to(row, (size, size)), 0.0), axis=1, keepdims=True)


def low_part(shards):
    return 1 << ((shards.bit_length()) // 2)


def landing(table, block, tok_dev, per_peer, seat):
    shards = table.shape[0]
    start = block * tok_dev
    inside = jnp.logical_and(table >= start, table < start + tok_dev)
    before = one_hot(iota((tok_dev, tok_dev), 0) < iota((tok_dev, tok_dev), 1))
    rank = matmul(one_hot(inside), before)
    place = (table - start).astype(F32)
    lane = iota((shards, tok_dev), 1)
    spread = jnp.zeros((shards, tok_dev), F32)
    for k in range(per_peer):
        hit = jnp.logical_and(inside, rank == float(k))
        found = jnp.sum(jnp.where(hit, place, 0.0), axis=1, keepdims=True)
        spread = spread + jnp.where(lax.rem(lane, per_peer) == k, found, 0.0)
    own = lax.div(lane, per_peer) == seat
    return jnp.sum(jnp.where(own, spread, 0.0), axis=0, keepdims=True).astype(jnp.int32)


def start_all(pairs, sems):
    copies = [pltpu.make_async_copy(src, dst, sems.at[i]) for i, (src, dst) in enumerate(pairs)]
    for copy in copies:
        copy.start()
    return copies


def project_kernel(low, hidden, table_hbm, w4, b4, w2, b2, ws, bs, places_v, *refs):
    high = (len(refs) - 9) - low
    sent_four, sent = refs[:high], refs[high : high + low]
    hidden_v, table_v, w4_v, w2_v, ws_v, b4_v, b2_v, bs_v, sems = refs[high + low :]
    chunks = ws.shape[1] // CHUNK
    copies = start_all(
        [
            (table_hbm, table_v),
            (hidden.at[0], hidden_v.at[0]),
            (b4, b4_v),
            (w4, w4_v),
            (hidden.at[1], hidden_v.at[1]),
            (b2, b2_v),
            (w2, w2_v),
            (hidden.at[2], hidden_v.at[2]),
            (bs, bs_v),
        ]
        + [(ws.at[:, pl.ds(i * CHUNK, CHUNK)], ws_v.at[i]) for i in range(chunks)],
        sems,
    )
    shards, tok_dev = table_v.shape
    per_peer = tok_dev // shards
    me = lax.axis_index("rows")
    copies[0].wait()
    table = table_v[...]
    mine = table_v[pl.ds(me, 1), :]
    block_row = lax.div(mine, tok_dev)
    block_col = column(block_row.astype(F32), tok_dev).astype(jnp.int32)
    square = (tok_dev, tok_dev)
    earlier = jnp.logical_and(block_col == jnp.broadcast_to(block_row, square), iota(square, 0) < iota(square, 1))
    within = jnp.sum(jnp.where(earlier, 1.0, 0.0), axis=0, keepdims=True).astype(jnp.int32)
    row = iota(square, 0)
    apart = jnp.bitwise_xor(block_row, me)
    order_low = one_hot(row == (lax.rem(apart, low) * high + lax.div(apart, low)) * per_peer + within)
    orders = [one_hot(row == jnp.bitwise_xor(block_row + step, me) * per_peer + within) for step in (0, 1, -1)]
    order_high = jnp.concatenate(orders, axis=0)

    seat_low = jnp.bitwise_xor(iota((shards, tok_dev), 0), me)
    seat_high = lax.rem(seat_low, low) * high + lax.div(seat_low, low)
    own = landing(table, me, tok_dev, per_peer, seat_high)
    above = landing(table, me - 1, tok_dev, per_peer, seat_high)
    below = landing(table, me + 1, tok_dev, per_peer, seat_high)
    cell = iota(square, 0)
    col = lax.rem(cell, GRID_W)
    edge_col = iota((GRID_W, tok_dev), 0)
    base = 0
    for source, target, at in ((own, cell, col), (above, edge_col + (tok_dev - GRID_W), edge_col), (below, edge_col, edge_col)):
        size = target.shape[0]
        places_v[base : base + size] = one_hot(jnp.logical_and(target == source + 1, at != 0))
        places_v[base + size : base + 2 * size] = one_hot(target == source)
        places_v[base + 2 * size : base + 3 * size] = one_hot(jnp.logical_and(target == source - 1, at != GRID_W - 1))
        base += 3 * size
    places_v[base : base + tok_dev] = one_hot(cell == landing(table, me, tok_dev, per_peer, seat_low))

    c4, c2 = w4_v.shape[1], w2_v.shape[1]
    for copy in copies[1:4]:
        copy.wait()
    four = (matmul(hidden_v[0], w4_v[...]) + b4_v[...]).astype(BF16)
    moved = matmul(order_high, four)
    for i in range(3):
        hand_out(moved[i * tok_dev : (i + 1) * tok_dev], sent_four, i * c4)
    copies[4].wait()
    rows_two = matmul(order_low, hidden_v[1]).astype(BF16)
    copies[5].wait()
    copies[6].wait()
    hand_out(matmul(rows_two, w2_v[...]) + b2_v[...], sent, 0)
    copies[7].wait()
    rows_same = matmul(order_low, hidden_v[2]).astype(BF16)
    copies[8].wait()
    for i in range(chunks):
        copies[9 + i].wait()
        same = matmul(rows_same, ws_v[i]) + bs_v[:, i * CHUNK : (i + 1) * CHUNK]
        hand_out(same, sent, c2 + i * CHUNK)


def hand_out(projected, sent, at):
    moved = projected.astype(BF16)
    rows = sent[0].shape[0]
    for k, out in enumerate(sent):
        out[:, at : at + moved.shape[1]] = moved[k * rows : (k + 1) * rows]


def turn_kernel(count, *refs):
    arrived, leaving = refs[:count], refs[count:]
    rows = arrived[0].shape[0] // len(leaving)
    for to, message in enumerate(leaving):
        for come, piece in enumerate(arrived):
            message[come * rows : (come + 1) * rows] = piece[to * rows : (to + 1) * rows]


def fetch_kernel(*refs):
    count = len(refs) // 2
    for copy in start_all(list(zip(refs[:count], refs[count:-1])), refs[-1]):
        copy.wait()


def join_kernel(places, w4, b4, wj, *refs):
    pieces, (begun, wide_v, rows_v, tiles_v, acc_v) = refs[:-5], refs[-5:]
    gather_rows(pieces, rows_v)
    widen(rows_v, places, w4, b4, tiles_v, wide_v)
    for chunk in range(begun.shape[0] // 4):
        convolve(chunk, wide_v, wj, acc_v, begun, 4 * chunk)


def gather_rows(pieces, rows_v):
    rows = pieces[0].shape[0]
    for i, piece in enumerate(pieces):
        rows_v[i * rows : (i + 1) * rows] = piece[...]


def widen(arrived, places, w4, b4, tiles_v, wide_v):
    tok_dev, c4 = arrived.shape[0], w4.shape[0]
    row_count = tok_dev // GRID_W
    me = lax.axis_index("rows")
    top = jnp.where(me > 0, 1.0, 0.0)
    bottom = jnp.where(me < lax.axis_size("rows") - 1, 1.0, 0.0)
    bias = b4[...]
    feat = c4

    base = 3 * tok_dev
    tiles_v[0:base] = matmul(places[0:base], arrived[:, 0:c4]).astype(BF16)
    tiles_v[base : base + 3 * GRID_W] = matmul(places[base : base + 3 * GRID_W], arrived[:, c4 : 2 * c4]).astype(BF16)
    base += 3 * GRID_W
    tiles_v[base : base + 3 * GRID_W] = matmul(places[base : base + 3 * GRID_W], arrived[:, 2 * c4 : 3 * c4]).astype(BF16)

    left = jnp.where(iota((GRID_W, 1), 0) == 0, 0.0, 1.0)
    right = jnp.where(iota((GRID_W, 1), 0) == GRID_W - 1, 0.0, 1.0)

    def fill(first, rows, tap, to, scale):
        size = rows * GRID_W
        for b in range(4):
            start = first + (0 if b == 3 else size)
            stop = first + (3 if b == 0 else 2) * size
            part = matmul(tiles_v[start:stop], w4[:, (tap * 4 + b) * feat : (tap * 4 + b + 1) * feat]) + bias
            if scale is not None:
                part = part * scale
            blocks = {0: ((1, None), (5, right)), 3: ((0, left), (4, None))}.get(b, ((b + 1, None),))
            for place, (block, edge) in enumerate(blocks):
                for i in range(rows):
                    piece = part[(place * rows + i) * GRID_W : (place * rows + i + 1) * GRID_W]
                    if edge is not None:
                        piece = piece * edge
                    wide_v[pl.ds(to(i) * GRID_W, GRID_W), block * feat : (block + 1) * feat] = piece.astype(BF16)

    for tap in range(4):
        fill(0, row_count, tap, lambda i, tap=tap: 4 * i + tap + 1, None)
    fill(3 * tok_dev, 1, 3, lambda i: 0, top)
    fill(3 * tok_dev + 3 * GRID_W, 1, 0, lambda i: 4 * row_count + 1, bottom)


def convolve(chunk, wide_v, wj, acc_v, out_v, at):
    feat = wj.shape[2]
    for b in range(4):
        total = None
        for row_tap in range(3):
            first = (4 * chunk + row_tap) * GRID_W
            term = matmul(wide_v[first : first + 4 * GRID_W, b * feat : (b + 3) * feat], wj[row_tap])
            total = term if total is None else total + term
        for r in range(4):
            for block in range(feat // 128):
                acc_v[r, block, pl.ds(b, GRID_W, 4), :] = total[
                    r * GRID_W : (r + 1) * GRID_W, block * 128 : (block + 1) * 128
                ]
    for r in range(4):
        for block in range(feat // 128):
            out_v[at + r, :, block * 128 : (block + 1) * 128] = acc_v[r, block].astype(BF16)


def rest_kernel(begun, wide, wj, places, w2, b2, *refs):
    arrived, outs = refs[:-12], refs[-12:]
    joined, up_two, same, rows_v, acc_v, out_v, same_v, acc_join_v, join_v, sems, same_sem, join_sems = outs
    cut = begun.shape[0]
    joins = [
        pltpu.make_async_copy(begun, joined.at[pl.ds(0, cut)], join_sems.at[0]),
        pltpu.make_async_copy(join_v, joined.at[pl.ds(cut, 4)], join_sems.at[1]),
    ]
    joins[0].start()
    gather_rows(arrived, rows_v)
    tok_dev = rows_v.shape[0]
    c2 = w2.shape[0]
    row_count = tok_dev // GRID_W
    place = places[places.shape[0] - tok_dev :]
    same_v[...] = matmul(place, rows_v[:, c2:]).astype(BF16)
    stores = [pltpu.make_async_copy(same_v, same, same_sem), *joins]
    stores[0].start()
    convolve(row_count - 1, wide, wj, acc_join_v, join_v, 0)
    joins[1].start()
    tile = matmul(place, rows_v[:, 0:c2]).astype(BF16)
    bias = b2[...]
    for a in range(2):
        for b in range(2):
            part = matmul(tile, w2[:, (a * 2 + b) * c2 : (a * 2 + b + 1) * c2]) + bias
            for i in range(row_count):
                for block in range(c2 // 128):
                    acc_v[2 * i + a, block, pl.ds(b, GRID_W, 2), :] = part[
                        i * GRID_W : (i + 1) * GRID_W, block * 128 : (block + 1) * 128
                    ]
        for i in range(row_count):
            r = 2 * i + a
            for block in range(c2 // 128):
                out_v[r, :, block * 128 : (block + 1) * 128] = acc_v[r, block].astype(BF16)
            store = pltpu.make_async_copy(out_v.at[r], up_two.at[r], sems.at[r])
            store.start()
            stores.append(store)
    for store in stores:
        store.wait()


def body(
    hidden_states,
    cell_of,
    proj_four_weight,
    proj_four_bias,
    proj_two_weight,
    proj_two_bias,
    proj_same_weight,
    proj_same_bias,
    up4_weight,
    up4_bias,
    up2_weight,
    up2_bias,
    join_weight,
):
    _, tok_dev, hid = hidden_states.shape
    shards = lax.axis_size("rows")
    per_peer = tok_dev // shards
    row_count = tok_dev // GRID_W
    c4, c2, cs = proj_four_weight.shape[1], proj_two_weight.shape[1], proj_same_weight.shape[1]
    feat = join_weight.shape[3]
    table = cell_of.reshape(shards, tok_dev)
    place_rows = 4 * tok_dev + 6 * GRID_W
    shape = jax.ShapeDtypeStruct

    low = low_part(shards)
    high = shards // low
    biases = [bias.reshape(1, -1) for bias in (proj_four_bias, proj_two_bias, proj_same_bias)]
    inputs = (
        hidden_states,
        table,
        proj_four_weight,
        biases[0],
        proj_two_weight,
        biases[1],
        proj_same_weight,
        biases[2],
    )
    four_shape = (low * per_peer, 3 * c4)
    rest_shape = (high * per_peer, c2 + cs)
    places, *sent = pl.pallas_call(
        functools.partial(project_kernel, low),
        out_shape=(pltpu.VMEM((place_rows, tok_dev), BF16),)
        + (pltpu.VMEM(four_shape, BF16),) * high
        + (pltpu.VMEM(rest_shape, BF16),) * low,
        in_specs=[ANY] * 8,
        out_specs=(VMEM,) * (1 + high + low),
        scratch_shapes=[
            pltpu.VMEM(hidden_states.shape, BF16),
            pltpu.VMEM(table.shape, jnp.int32),
            pltpu.VMEM((hid, c4), BF16),
            pltpu.VMEM((hid, c2), BF16),
            pltpu.VMEM((cs // CHUNK, hid, CHUNK), BF16),
            pltpu.VMEM((1, c4), F32),
            pltpu.VMEM((1, c2), F32),
            pltpu.VMEM((1, cs), F32),
            pltpu.SemaphoreType.DMA((9 + cs // CHUNK,)),
        ],
        compiler_params=pltpu.CompilerParams(vmem_limit_bytes=10 << 20),
        cost_estimate=pl.CostEstimate(flops=2 * tok_dev * hid * (c4 + c2 + cs), bytes_accessed=5 << 20, transcendentals=0),
        name="project",
    )(*(in_hbm(x) for x in inputs))

    def swap(pieces, unit):
        return [pieces[0]] + [
            lax.ppermute(piece, "rows", [(i, i ^ (step * unit)) for i in range(shards)])
            for step, piece in enumerate(pieces[1:], 1)
        ]

    def turn(pieces, out_shape, count):
        return pl.pallas_call(
            functools.partial(turn_kernel, len(pieces)),
            out_shape=(pltpu.VMEM(out_shape, BF16),) * count,
            in_specs=[VMEM] * len(pieces),
            out_specs=(VMEM,) * count,
            compiler_params=pltpu.CompilerParams(vmem_limit_bytes=4 << 20),
            cost_estimate=pl.CostEstimate(flops=1 << 26, bytes_accessed=1 << 20, transcendentals=0),
            name="turn",
        )(*pieces)

    rest = swap(sent[high:], 1)
    four = swap(sent[:high], low)
    rest = turn(rest, (low * per_peer, c2 + cs), high)
    rest = swap(rest, low)
    four = turn(four, (high * per_peer, 3 * c4), low)
    four = swap(four, 1)

    weights = (
        up4_weight,
        up4_bias.reshape(1, -1),
        join_weight.reshape(3, 3 * c4, feat),
        up2_weight,
        up2_bias.reshape(1, -1),
    )
    w4, b4, wj, w2, b2 = pl.pallas_call(
        fetch_kernel,
        out_shape=tuple(pltpu.VMEM(w.shape, w.dtype) for w in weights),
        in_specs=[ANY] * 5,
        out_specs=(VMEM,) * 5,
        scratch_shapes=[pltpu.SemaphoreType.DMA((5,))],
        cost_estimate=pl.CostEstimate(flops=1 << 30, bytes_accessed=5 << 20, transcendentals=0),
        compiler_params=pltpu.CompilerParams(vmem_limit_bytes=8 << 20),
        name="fetch",
    )(*(in_hbm(w) for w in weights))

    out_rows = 4 * row_count
    join_shape = (out_rows, 4 * GRID_W, feat)
    wide_shape = ((out_rows + 2) * GRID_W, 6 * c4)

    acc_shape = (4, feat // 128, 4 * GRID_W, 128)

    begun, wide = pl.pallas_call(
        join_kernel,
        out_shape=(pltpu.VMEM((out_rows - 4, 4 * GRID_W, feat), BF16), pltpu.VMEM(wide_shape, BF16)),
        in_specs=[VMEM] * (4 + low),
        out_specs=(VMEM, VMEM),
        scratch_shapes=[
            pltpu.VMEM((tok_dev, 3 * c4), BF16),
            pltpu.VMEM((place_rows, c4), BF16),
            pltpu.VMEM(acc_shape, F32),
        ],
        compiler_params=pltpu.CompilerParams(vmem_limit_bytes=20 << 20),
        cost_estimate=pl.CostEstimate(flops=4 << 30, bytes_accessed=4 << 20, transcendentals=0),
        name="join",
    )(places, w4, b4, wj, *four)
    joined, upsampled_two, same_scale = pl.pallas_call(
        rest_kernel,
        out_shape=(shape(join_shape, BF16), shape((2 * row_count, 2 * GRID_W, c2), BF16), shape((tok_dev, cs), BF16)),
        in_specs=[VMEM] * (6 + len(rest)),
        out_specs=(ANY, ANY, ANY),
        scratch_shapes=[
            pltpu.VMEM((tok_dev, c2 + cs), BF16),
            pltpu.VMEM((2 * row_count, c2 // 128, 2 * GRID_W, 128), F32),
            pltpu.VMEM((2 * row_count, 2 * GRID_W, c2), BF16),
            pltpu.VMEM((tok_dev, cs), BF16),
            pltpu.VMEM(acc_shape, F32),
            pltpu.VMEM((4, 4 * GRID_W, feat), BF16),
            pltpu.SemaphoreType.DMA((2 * row_count,)),
            pltpu.SemaphoreType.DMA,
            pltpu.SemaphoreType.DMA((2,)),
        ],
        compiler_params=pltpu.CompilerParams(vmem_limit_bytes=12 << 20),
        cost_estimate=pl.CostEstimate(flops=2 << 30, bytes_accessed=4 << 20, transcendentals=0),
        name="rest",
    )(begun, wide, wj, places, w2, b2, *rest)
    return (joined, upsampled_two, same_scale.reshape(row_count, GRID_W, cs))


def solution(mesh):
    return jax.shard_map(
        body,
        mesh=mesh,
        in_specs=(P(None, ("img", "rows"), None),) + (P(),) * 12,
        out_specs=(P(("img", "rows"), None, None),) * 3,
        check_vma=False,
    )
```

```python
import functools

import jax
import jax.numpy as jnp
from jax import lax
from jax.experimental import pallas as pl
from jax.experimental.pallas import tpu as pltpu
from jax.sharding import PartitionSpec as P


GRID_W = 64
CHUNK = 1024
F32 = jnp.float32
BF16 = jnp.bfloat16
ANY = pl.BlockSpec(memory_space=pl.ANY)
VMEM = pl.BlockSpec(memory_space=pltpu.VMEM)


def in_hbm(x):
    return pltpu.with_memory_space_constraint(x, pltpu.HBM)


def one_hot(mask):
    return jnp.where(mask, 1.0, 0.0).astype(BF16)


def iota(shape, dim):
    return lax.broadcasted_iota(jnp.int32, shape, dim)


def matmul(left, right):
    return jnp.dot(left, right, preferred_element_type=F32)


def column(row, size):
    same = iota((size, size), 0) == iota((size, size), 1)
    return jnp.sum(jnp.where(same, jnp.broadcast_to(row, (size, size)), 0.0), axis=1, keepdims=True)


def low_part(shards):
    return 1 << ((shards.bit_length()) // 2)


def landing(table, block, tok_dev, per_peer, seat):
    shards = table.shape[0]
    start = block * tok_dev
    inside = jnp.logical_and(table >= start, table < start + tok_dev)
    before = one_hot(iota((tok_dev, tok_dev), 0) < iota((tok_dev, tok_dev), 1))
    rank = matmul(one_hot(inside), before)
    place = (table - start).astype(F32)
    lane = iota((shards, tok_dev), 1)
    spread = jnp.zeros((shards, tok_dev), F32)
    for k in range(per_peer):
        hit = jnp.logical_and(inside, rank == float(k))
        found = jnp.sum(jnp.where(hit, place, 0.0), axis=1, keepdims=True)
        spread = spread + jnp.where(lax.rem(lane, per_peer) == k, found, 0.0)
    own = lax.div(lane, per_peer) == seat
    return jnp.sum(jnp.where(own, spread, 0.0), axis=0, keepdims=True).astype(jnp.int32)


def start_all(pairs, sems):
    copies = [pltpu.make_async_copy(src, dst, sems.at[i]) for i, (src, dst) in enumerate(pairs)]
    for copy in copies:
        copy.start()
    return copies


def project_kernel(low, hidden, table_hbm, w4, b4, w2, b2, ws, bs, places_v, *refs):
    high = (len(refs) - 9) - low
    sent_four, sent = refs[:high], refs[high : high + low]
    hidden_v, table_v, w4_v, w2_v, ws_v, b4_v, b2_v, bs_v, sems = refs[high + low :]
    chunks = ws.shape[1] // CHUNK
    copies = start_all(
        [
            (table_hbm, table_v),
            (hidden.at[0], hidden_v.at[0]),
            (b4, b4_v),
            (w4, w4_v),
            (hidden.at[1], hidden_v.at[1]),
            (b2, b2_v),
            (w2, w2_v),
            (hidden.at[2], hidden_v.at[2]),
            (bs, bs_v),
        ]
        + [(ws.at[:, pl.ds(i * CHUNK, CHUNK)], ws_v.at[i]) for i in range(chunks)],
        sems,
    )
    shards, tok_dev = table_v.shape
    per_peer = tok_dev // shards
    me = lax.axis_index("rows")
    copies[0].wait()
    table = table_v[...]
    mine = table_v[pl.ds(me, 1), :]
    block_row = lax.div(mine, tok_dev)
    block_col = column(block_row.astype(F32), tok_dev).astype(jnp.int32)
    square = (tok_dev, tok_dev)
    earlier = jnp.logical_and(block_col == jnp.broadcast_to(block_row, square), iota(square, 0) < iota(square, 1))
    within = jnp.sum(jnp.where(earlier, 1.0, 0.0), axis=0, keepdims=True).astype(jnp.int32)
    row = iota(square, 0)
    apart = jnp.bitwise_xor(block_row, me)
    order_low = one_hot(row == (lax.rem(apart, low) * high + lax.div(apart, low)) * per_peer + within)
    plane, unit = lax.div(block_row, low), lax.rem(block_row, low)
    my_plane = lax.div(me, low)

    def row_of(to_plane, to_unit):
        return (jnp.bitwise_xor(to_plane, my_plane) * (low + 2) + to_unit) * per_peer + within

    row = iota((high * (low + 2) * per_peer, tok_dev), 0)
    nowhere = jnp.full_like(unit, -1)
    here = row == row_of(plane, unit + 1)
    next_plane = row == jnp.where(unit == low - 1, row_of(plane + 1, 0), nowhere)
    last_plane = row == jnp.where(unit == 0, row_of(plane - 1, low + 1), nowhere)
    order_high = one_hot(jnp.logical_or(here, jnp.logical_or(next_plane, last_plane)))

    seat_low = jnp.bitwise_xor(iota((shards, tok_dev), 0), me)
    seat_high = lax.rem(seat_low, low) * high + lax.div(seat_low, low)
    own = landing(table, me, tok_dev, per_peer, seat_high)
    above = landing(table, me - 1, tok_dev, per_peer, seat_high)
    below = landing(table, me + 1, tok_dev, per_peer, seat_high)
    cell = iota(square, 0)
    col = lax.rem(cell, GRID_W)
    edge_col = iota((GRID_W, tok_dev), 0)
    base = 0
    for source, target, at in ((own, cell, col), (above, edge_col + (tok_dev - GRID_W), edge_col), (below, edge_col, edge_col)):
        size = target.shape[0]
        places_v[base : base + size] = one_hot(jnp.logical_and(target == source + 1, at != 0))
        places_v[base + size : base + 2 * size] = one_hot(target == source)
        places_v[base + 2 * size : base + 3 * size] = one_hot(jnp.logical_and(target == source - 1, at != GRID_W - 1))
        base += 3 * size
    places_v[base : base + tok_dev] = one_hot(cell == landing(table, me, tok_dev, per_peer, seat_low))

    c2 = w2_v.shape[1]
    for copy in copies[1:4]:
        copy.wait()
    four = (matmul(hidden_v[0], w4_v[...]) + b4_v[...]).astype(BF16)
    hand_out(matmul(order_high, four), sent_four, 0)
    copies[4].wait()
    rows_two = matmul(order_low, hidden_v[1]).astype(BF16)
    copies[5].wait()
    copies[6].wait()
    hand_out(matmul(rows_two, w2_v[...]) + b2_v[...], sent, 0)
    copies[7].wait()
    rows_same = matmul(order_low, hidden_v[2]).astype(BF16)
    copies[8].wait()
    for i in range(chunks):
        copies[9 + i].wait()
        same = matmul(rows_same, ws_v[i]) + bs_v[:, i * CHUNK : (i + 1) * CHUNK]
        hand_out(same, sent, c2 + i * CHUNK)


def hand_out(projected, sent, at):
    moved = projected.astype(BF16)
    rows = sent[0].shape[0]
    for k, out in enumerate(sent):
        out[:, at : at + moved.shape[1]] = moved[k * rows : (k + 1) * rows]


def turn_kernel(count, *refs):
    arrived, leaving = refs[:count], refs[count:]
    rows = arrived[0].shape[0] // len(leaving)
    for to, message in enumerate(leaving):
        for come, piece in enumerate(arrived):
            message[come * rows : (come + 1) * rows] = piece[to * rows : (to + 1) * rows]


def turn_four_kernel(low, per_peer, *refs):
    high = len(refs) - low - 1
    arrived, leaving, rows_v = refs[:high], refs[high:-1], refs[-1]
    mine = lax.rem(lax.axis_index("rows"), low)
    c4 = rows_v.shape[1]
    count = high * per_peer
    if per_peer % 8 == 0:
        for k, message in enumerate(leaving):
            unit = jnp.bitwise_xor(mine, k)
            for h, piece in enumerate(arrived):
                for place, step in enumerate((1, 0, 2)):
                    first = pl.multiple_of((unit + step) * per_peer, per_peer)
                    message[h * per_peer : (h + 1) * per_peer, place * c4 : (place + 1) * c4] = piece[
                        pl.ds(first, per_peer), :
                    ]
        return
    gather_rows(arrived, rows_v)
    total = rows_v.shape[0]
    to = iota((low * count, total), 0)
    h = lax.rem(lax.div(to, per_peer), high)
    unit = jnp.bitwise_xor(lax.div(to, count), mine)
    for place, step in enumerate((1, 0, 2)):
        source = (h * (low + 2) + unit + step) * per_peer + lax.rem(to, per_peer)
        moved = matmul(one_hot(iota(to.shape, 1) == source), rows_v[...]).astype(BF16)
        for k, message in enumerate(leaving):
            message[:, place * c4 : (place + 1) * c4] = moved[k * count : (k + 1) * count]


def fetch_kernel(*refs):
    count = len(refs) // 2
    for copy in start_all(list(zip(refs[:count], refs[count:-1])), refs[-1]):
        copy.wait()


def join_kernel(places, w4, b4, wj, *refs):
    pieces, (begun, last, rows_v, tiles_v, wide_v, acc_v, out_v, sems) = refs[:-8], refs[-8:]
    gather_rows(pieces, rows_v)
    widen(rows_v, places, w4, b4, tiles_v, wide_v)
    stores = []
    for chunk in range(out_v.shape[0] // 4):
        rows = pl.ds(4 * chunk, 4)
        convolve(chunk, wide_v, wj, acc_v, out_v, 4 * chunk)
        stores.append(pltpu.make_async_copy(out_v.at[rows], begun.at[rows], sems.at[chunk]))
        stores[-1].start()
    convolve(out_v.shape[0] // 4, wide_v, wj, acc_v, last, 0)
    for store in stores:
        store.wait()


def gather_rows(pieces, rows_v):
    rows = pieces[0].shape[0]
    for i, piece in enumerate(pieces):
        rows_v[i * rows : (i + 1) * rows] = piece[...]


def widen(arrived, places, w4, b4, tiles_v, wide_v):
    tok_dev, c4 = arrived.shape[0], w4.shape[0]
    row_count = tok_dev // GRID_W
    me = lax.axis_index("rows")
    top = jnp.where(me > 0, 1.0, 0.0)
    bottom = jnp.where(me < lax.axis_size("rows") - 1, 1.0, 0.0)
    bias = b4[...]
    feat = c4

    base = 3 * tok_dev
    tiles_v[0:base] = matmul(places[0:base], arrived[:, 0:c4]).astype(BF16)
    tiles_v[base : base + 3 * GRID_W] = matmul(places[base : base + 3 * GRID_W], arrived[:, c4 : 2 * c4]).astype(BF16)
    base += 3 * GRID_W
    tiles_v[base : base + 3 * GRID_W] = matmul(places[base : base + 3 * GRID_W], arrived[:, 2 * c4 : 3 * c4]).astype(BF16)

    left = jnp.where(iota((GRID_W, 1), 0) == 0, 0.0, 1.0)
    right = jnp.where(iota((GRID_W, 1), 0) == GRID_W - 1, 0.0, 1.0)

    def fill(first, rows, tap, to, scale):
        size = rows * GRID_W
        for b in range(4):
            start = first + (0 if b == 3 else size)
            stop = first + (3 if b == 0 else 2) * size
            part = matmul(tiles_v[start:stop], w4[:, (tap * 4 + b) * feat : (tap * 4 + b + 1) * feat]) + bias
            if scale is not None:
                part = part * scale
            blocks = {0: ((1, None), (5, right)), 3: ((0, left), (4, None))}.get(b, ((b + 1, None),))
            for place, (block, edge) in enumerate(blocks):
                for i in range(rows):
                    piece = part[(place * rows + i) * GRID_W : (place * rows + i + 1) * GRID_W]
                    if edge is not None:
                        piece = piece * edge
                    wide_v[pl.ds(to(i) * GRID_W, GRID_W), block * feat : (block + 1) * feat] = piece.astype(BF16)

    for tap in range(4):
        fill(0, row_count, tap, lambda i, tap=tap: 4 * i + tap + 1, None)
    fill(3 * tok_dev, 1, 3, lambda i: 0, top)
    fill(3 * tok_dev + 3 * GRID_W, 1, 0, lambda i: 4 * row_count + 1, bottom)


def convolve(chunk, wide_v, wj, acc_v, out_v, at):
    feat = wj.shape[2]
    slot = chunk % 2
    for b in range(4):
        total = None
        for row_tap in range(3):
            first = (4 * chunk + row_tap) * GRID_W
            term = matmul(wide_v[first : first + 4 * GRID_W, b * feat : (b + 3) * feat], wj[row_tap])
            total = term if total is None else total + term
        for r in range(4):
            for block in range(feat // 128):
                acc_v[4 * slot + r, block, pl.ds(b, GRID_W, 4), :] = total[
                    r * GRID_W : (r + 1) * GRID_W, block * 128 : (block + 1) * 128
                ]
    for r in range(4):
        for block in range(feat // 128):
            out_v[at + r, :, block * 128 : (block + 1) * 128] = acc_v[4 * slot + r, block].astype(BF16)


def rest_kernel(begun, last, places, w2, b2, *refs):
    del begun
    arrived, outs = refs[:-9], refs[-9:]
    joined, up_two, same, rows_v, acc_v, out_v, same_v, sems, end_sems = outs
    tail = joined.shape[0] - last.shape[0]
    ends = [
        pltpu.make_async_copy(last, joined.at[pl.ds(tail, last.shape[0])], end_sems.at[0]),
        pltpu.make_async_copy(same_v, same, end_sems.at[1]),
    ]
    ends[0].start()
    gather_rows(arrived, rows_v)
    tok_dev = rows_v.shape[0]
    c2 = w2.shape[0]
    row_count = tok_dev // GRID_W
    place = places[places.shape[0] - tok_dev :]
    same_v[...] = matmul(place, rows_v[:, c2:]).astype(BF16)
    ends[1].start()
    stores = [*ends]
    tile = matmul(place, rows_v[:, 0:c2]).astype(BF16)
    bias = b2[...]
    for a in range(2):
        for b in range(2):
            part = matmul(tile, w2[:, (a * 2 + b) * c2 : (a * 2 + b + 1) * c2]) + bias
            for i in range(row_count):
                for block in range(c2 // 128):
                    acc_v[2 * i + a, block, pl.ds(b, GRID_W, 2), :] = part[
                        i * GRID_W : (i + 1) * GRID_W, block * 128 : (block + 1) * 128
                    ]
        for i in range(row_count):
            r = 2 * i + a
            for block in range(c2 // 128):
                out_v[r, :, block * 128 : (block + 1) * 128] = acc_v[r, block].astype(BF16)
            store = pltpu.make_async_copy(out_v.at[r], up_two.at[r], sems.at[r])
            store.start()
            stores.append(store)
    for store in stores:
        store.wait()


def body(
    hidden_states,
    cell_of,
    proj_four_weight,
    proj_four_bias,
    proj_two_weight,
    proj_two_bias,
    proj_same_weight,
    proj_same_bias,
    up4_weight,
    up4_bias,
    up2_weight,
    up2_bias,
    join_weight,
):
    _, tok_dev, hid = hidden_states.shape
    shards = lax.axis_size("rows")
    per_peer = tok_dev // shards
    row_count = tok_dev // GRID_W
    c4, c2, cs = proj_four_weight.shape[1], proj_two_weight.shape[1], proj_same_weight.shape[1]
    feat = join_weight.shape[3]
    table = cell_of.reshape(shards, tok_dev)
    place_rows = 4 * tok_dev + 6 * GRID_W
    shape = jax.ShapeDtypeStruct

    low = low_part(shards)
    high = shards // low
    biases = [bias.reshape(1, -1) for bias in (proj_four_bias, proj_two_bias, proj_same_bias)]
    inputs = (
        hidden_states,
        table,
        proj_four_weight,
        biases[0],
        proj_two_weight,
        biases[1],
        proj_same_weight,
        biases[2],
    )
    four_shape = ((low + 2) * per_peer, c4)
    rest_shape = (high * per_peer, c2 + cs)
    places, *sent = pl.pallas_call(
        functools.partial(project_kernel, low),
        out_shape=(pltpu.VMEM((place_rows, tok_dev), BF16),)
        + (pltpu.VMEM(four_shape, BF16),) * high
        + (pltpu.VMEM(rest_shape, BF16),) * low,
        in_specs=[ANY] * 8,
        out_specs=(VMEM,) * (1 + high + low),
        scratch_shapes=[
            pltpu.VMEM(hidden_states.shape, BF16),
            pltpu.VMEM(table.shape, jnp.int32),
            pltpu.VMEM((hid, c4), BF16),
            pltpu.VMEM((hid, c2), BF16),
            pltpu.VMEM((cs // CHUNK, hid, CHUNK), BF16),
            pltpu.VMEM((1, c4), F32),
            pltpu.VMEM((1, c2), F32),
            pltpu.VMEM((1, cs), F32),
            pltpu.SemaphoreType.DMA((9 + cs // CHUNK,)),
        ],
        compiler_params=pltpu.CompilerParams(vmem_limit_bytes=10 << 20),
        cost_estimate=pl.CostEstimate(flops=2 * tok_dev * hid * (c4 + c2 + cs), bytes_accessed=5 << 20, transcendentals=0),
        name="project",
    )(*(in_hbm(x) for x in inputs))

    def swap(pieces, unit):
        moved = [pieces[0]]
        for step, piece in enumerate(pieces[1:], 1):
            moved.append(lax.ppermute(piece, "rows", [(i, i ^ (step * unit)) for i in range(shards)]))
        return moved

    def turn(kernel, pieces, out_shape, count, scratch=()):
        return pl.pallas_call(
            kernel,
            out_shape=(pltpu.VMEM(out_shape, BF16),) * count,
            in_specs=[VMEM] * len(pieces),
            out_specs=(VMEM,) * count,
            scratch_shapes=scratch,
            compiler_params=pltpu.CompilerParams(vmem_limit_bytes=4 << 20),
            cost_estimate=pl.CostEstimate(flops=1 << 26, bytes_accessed=1 << 20, transcendentals=0),
            name="turn",
        )(*pieces)

    rest = swap(sent[high:], 1)
    four = swap(sent[:high], low)
    rest = turn(functools.partial(turn_kernel, low), rest, (low * per_peer, c2 + cs), high)
    rest = swap(rest, low)
    four = turn(
        functools.partial(turn_four_kernel, low, per_peer),
        four,
        (high * per_peer, 3 * c4),
        low,
        [pltpu.VMEM((high * (low + 2) * per_peer, c4), BF16)],
    )
    four = swap(four, 1)

    weights = (
        up4_weight,
        up4_bias.reshape(1, -1),
        join_weight.reshape(3, 3 * c4, feat),
        up2_weight,
        up2_bias.reshape(1, -1),
    )
    w4, b4, wj, w2, b2 = pl.pallas_call(
        fetch_kernel,
        out_shape=tuple(pltpu.VMEM(w.shape, w.dtype) for w in weights),
        in_specs=[ANY] * 5,
        out_specs=(VMEM,) * 5,
        scratch_shapes=[pltpu.SemaphoreType.DMA((5,))],
        cost_estimate=pl.CostEstimate(flops=1 << 30, bytes_accessed=5 << 20, transcendentals=0),
        compiler_params=pltpu.CompilerParams(vmem_limit_bytes=8 << 20),
        name="fetch",
    )(*(in_hbm(w) for w in weights))

    out_rows = 4 * row_count
    join_shape = (out_rows, 4 * GRID_W, feat)
    begun, last = pl.pallas_call(
        join_kernel,
        out_shape=(pltpu.HBM(join_shape, BF16), pltpu.VMEM((4, 4 * GRID_W, feat), BF16)),
        in_specs=[VMEM] * (4 + low),
        out_specs=(ANY, VMEM),
        scratch_shapes=[
            pltpu.VMEM((tok_dev, 3 * c4), BF16),
            pltpu.VMEM((place_rows, c4), BF16),
            pltpu.VMEM(((out_rows + 2) * GRID_W, 6 * c4), BF16),
            pltpu.VMEM((8, feat // 128, 4 * GRID_W, 128), F32),
            pltpu.VMEM((out_rows - 4, 4 * GRID_W, feat), BF16),
            pltpu.SemaphoreType.DMA((row_count - 1,)),
        ],
        compiler_params=pltpu.CompilerParams(vmem_limit_bytes=20 << 20),
        cost_estimate=pl.CostEstimate(flops=4 << 30, bytes_accessed=4 << 20, transcendentals=0),
        name="join",
    )(places, w4, b4, wj, *four)
    joined, upsampled_two, same_scale = pl.pallas_call(
        rest_kernel,
        out_shape=(shape(join_shape, BF16), shape((2 * row_count, 2 * GRID_W, c2), BF16), shape((tok_dev, cs), BF16)),
        in_specs=[ANY] + [VMEM] * (4 + len(rest)),
        out_specs=(ANY, ANY, ANY),
        scratch_shapes=[
            pltpu.VMEM((tok_dev, c2 + cs), BF16),
            pltpu.VMEM((2 * row_count, c2 // 128, 2 * GRID_W, 128), F32),
            pltpu.VMEM((2 * row_count, 2 * GRID_W, c2), BF16),
            pltpu.VMEM((tok_dev, cs), BF16),
            pltpu.SemaphoreType.DMA((2 * row_count,)),
            pltpu.SemaphoreType.DMA((2,)),
        ],
        input_output_aliases={0: 0},
        compiler_params=pltpu.CompilerParams(vmem_limit_bytes=12 << 20),
        cost_estimate=pl.CostEstimate(flops=2 << 30, bytes_accessed=4 << 20, transcendentals=0),
        name="rest",
    )(begun, last, places, w2, b2, *rest)
    return (joined, upsampled_two, same_scale.reshape(row_count, GRID_W, cs))


def solution(mesh):
    return jax.shard_map(
        body,
        mesh=mesh,
        in_specs=(P(None, ("img", "rows"), None),) + (P(),) * 12,
        out_specs=(P(("img", "rows"), None, None),) * 3,
        check_vma=False,
    )
```

```python
import functools

import jax
import jax.numpy as jnp
from jax import lax
from jax.experimental import pallas as pl
from jax.experimental.pallas import tpu as pltpu
from jax.sharding import PartitionSpec as P


GRID_W = 64
CHUNK = 1024
F32 = jnp.float32
BF16 = jnp.bfloat16
ANY = pl.BlockSpec(memory_space=pl.ANY)
VMEM = pl.BlockSpec(memory_space=pltpu.VMEM)


def in_hbm(x):
    return pltpu.with_memory_space_constraint(x, pltpu.HBM)


def one_hot(mask):
    return jnp.where(mask, 1.0, 0.0).astype(BF16)


def iota(shape, dim):
    return lax.broadcasted_iota(jnp.int32, shape, dim)


def matmul(left, right):
    return jnp.dot(left, right, preferred_element_type=F32)


def column(row, size):
    same = iota((size, size), 0) == iota((size, size), 1)
    return jnp.sum(jnp.where(same, jnp.broadcast_to(row, (size, size)), 0.0), axis=1, keepdims=True)


def low_part(shards):
    return 1 << ((shards.bit_length()) // 2)


def landing(table, block, tok_dev, per_peer, seat):
    shards = table.shape[0]
    start = block * tok_dev
    inside = jnp.logical_and(table >= start, table < start + tok_dev)
    before = one_hot(iota((tok_dev, tok_dev), 0) < iota((tok_dev, tok_dev), 1))
    rank = matmul(one_hot(inside), before)
    place = (table - start).astype(F32)
    lane = iota((shards, tok_dev), 1)
    spread = jnp.zeros((shards, tok_dev), F32)
    for k in range(per_peer):
        hit = jnp.logical_and(inside, rank == float(k))
        found = jnp.sum(jnp.where(hit, place, 0.0), axis=1, keepdims=True)
        spread = spread + jnp.where(lax.rem(lane, per_peer) == k, found, 0.0)
    own = lax.div(lane, per_peer) == seat
    return jnp.sum(jnp.where(own, spread, 0.0), axis=0, keepdims=True).astype(jnp.int32)


def start_all(pairs, sems):
    copies = [pltpu.make_async_copy(src, dst, sems.at[i]) for i, (src, dst) in enumerate(pairs)]
    for copy in copies:
        copy.start()
    return copies


def project_kernel(low, hidden, table_hbm, w4, b4, w2, b2, ws, bs, places_v, *refs):
    high = (len(refs) - 9) - low
    sent_four, sent = refs[:high], refs[high : high + low]
    hidden_v, table_v, w4_v, w2_v, ws_v, b4_v, b2_v, bs_v, sems = refs[high + low :]
    chunks = ws.shape[1] // CHUNK
    copies = start_all(
        [
            (table_hbm, table_v),
            (hidden.at[0], hidden_v.at[0]),
            (b4, b4_v),
            (w4, w4_v),
            (hidden.at[1], hidden_v.at[1]),
            (b2, b2_v),
            (w2, w2_v),
            (hidden.at[2], hidden_v.at[2]),
            (bs, bs_v),
        ]
        + [(ws.at[:, pl.ds(i * CHUNK, CHUNK)], ws_v.at[i]) for i in range(chunks)],
        sems,
    )
    shards, tok_dev = table_v.shape
    per_peer = tok_dev // shards
    me = lax.axis_index("rows")
    copies[0].wait()
    table = table_v[...]
    mine = table_v[pl.ds(me, 1), :]
    block_row = lax.div(mine, tok_dev)
    block_col = column(block_row.astype(F32), tok_dev).astype(jnp.int32)
    square = (tok_dev, tok_dev)
    earlier = jnp.logical_and(block_col == jnp.broadcast_to(block_row, square), iota(square, 0) < iota(square, 1))
    within = jnp.sum(jnp.where(earlier, 1.0, 0.0), axis=0, keepdims=True).astype(jnp.int32)
    row = iota(square, 0)
    apart = jnp.bitwise_xor(block_row, me)
    order_low = one_hot(row == (lax.rem(apart, low) * high + lax.div(apart, low)) * per_peer + within)
    plane, unit = lax.div(block_row, low), lax.rem(block_row, low)
    my_plane = lax.div(me, low)

    def row_of(to_plane, to_unit):
        return (jnp.bitwise_xor(to_plane, my_plane) * (low + 2) + to_unit) * per_peer + within

    row = iota((high * (low + 2) * per_peer, tok_dev), 0)
    nowhere = jnp.full_like(unit, -1)
    here = row == row_of(plane, unit + 1)
    next_plane = row == jnp.where(unit == low - 1, row_of(plane + 1, 0), nowhere)
    last_plane = row == jnp.where(unit == 0, row_of(plane - 1, low + 1), nowhere)
    order_high = one_hot(jnp.logical_or(here, jnp.logical_or(next_plane, last_plane)))

    seat_low = jnp.bitwise_xor(iota((shards, tok_dev), 0), me)
    seat_high = lax.rem(seat_low, low) * high + lax.div(seat_low, low)
    own = landing(table, me, tok_dev, per_peer, seat_high)
    above = landing(table, me - 1, tok_dev, per_peer, seat_high)
    below = landing(table, me + 1, tok_dev, per_peer, seat_high)
    cell = iota(square, 0)
    col = lax.rem(cell, GRID_W)
    edge_col = iota((GRID_W, tok_dev), 0)
    base = 0
    for source, target, at in ((own, cell, col), (above, edge_col + (tok_dev - GRID_W), edge_col), (below, edge_col, edge_col)):
        size = target.shape[0]
        places_v[base : base + size] = one_hot(jnp.logical_and(target == source + 1, at != 0))
        places_v[base + size : base + 2 * size] = one_hot(target == source)
        places_v[base + 2 * size : base + 3 * size] = one_hot(jnp.logical_and(target == source - 1, at != GRID_W - 1))
        base += 3 * size
    places_v[base : base + tok_dev] = one_hot(cell == landing(table, me, tok_dev, per_peer, seat_low))

    c2 = w2_v.shape[1]
    for copy in copies[1:4]:
        copy.wait()
    four = (matmul(hidden_v[0], w4_v[...]) + b4_v[...]).astype(BF16)
    hand_out(matmul(order_high, four), sent_four, 0)
    copies[4].wait()
    rows_two = matmul(order_low, hidden_v[1]).astype(BF16)
    copies[5].wait()
    copies[6].wait()
    hand_out(matmul(rows_two, w2_v[...]) + b2_v[...], sent, 0)
    copies[7].wait()
    rows_same = matmul(order_low, hidden_v[2]).astype(BF16)
    copies[8].wait()
    for i in range(chunks):
        copies[9 + i].wait()
        same = matmul(rows_same, ws_v[i]) + bs_v[:, i * CHUNK : (i + 1) * CHUNK]
        hand_out(same, sent, c2 + i * CHUNK)


def hand_out(projected, sent, at):
    moved = projected.astype(BF16)
    rows = sent[0].shape[0]
    for k, out in enumerate(sent):
        out[:, at : at + moved.shape[1]] = moved[k * rows : (k + 1) * rows]


def turn_kernel(count, *refs):
    arrived, leaving = refs[:count], refs[count:]
    rows = arrived[0].shape[0] // len(leaving)
    for to, message in enumerate(leaving):
        for come, piece in enumerate(arrived):
            message[come * rows : (come + 1) * rows] = piece[to * rows : (to + 1) * rows]


def turn_four_kernel(low, per_peer, *refs):
    high = len(refs) - low - 1
    arrived, leaving, rows_v = refs[:high], refs[high:-1], refs[-1]
    mine = lax.rem(lax.axis_index("rows"), low)
    c4 = rows_v.shape[1]
    count = high * per_peer
    if per_peer % 8 == 0:
        for k, message in enumerate(leaving):
            unit = jnp.bitwise_xor(mine, k)
            for h, piece in enumerate(arrived):
                for place, step in enumerate((1, 0, 2)):
                    first = pl.multiple_of((unit + step) * per_peer, per_peer)
                    message[h * per_peer : (h + 1) * per_peer, place * c4 : (place + 1) * c4] = piece[
                        pl.ds(first, per_peer), :
                    ]
        return
    gather_rows(arrived, rows_v)
    total = rows_v.shape[0]
    to = iota((low * count, total), 0)
    h = lax.rem(lax.div(to, per_peer), high)
    unit = jnp.bitwise_xor(lax.div(to, count), mine)
    for place, step in enumerate((1, 0, 2)):
        source = (h * (low + 2) + unit + step) * per_peer + lax.rem(to, per_peer)
        moved = matmul(one_hot(iota(to.shape, 1) == source), rows_v[...]).astype(BF16)
        for k, message in enumerate(leaving):
            message[:, place * c4 : (place + 1) * c4] = moved[k * count : (k + 1) * count]


def fetch_kernel(*refs):
    count = len(refs) // 2
    for copy in start_all(list(zip(refs[:count], refs[count:-1])), refs[-1]):
        copy.wait()


def join_kernel(places, w4, b4, wj, *refs):
    pieces, (joined, rows_v, tiles_v, wide_v, acc_v) = refs[:-5], refs[-5:]
    gather_rows(pieces, rows_v)
    widen(rows_v, places, w4, b4, tiles_v, wide_v)
    convolve(wide_v, wj, acc_v, joined)


def gather_rows(pieces, rows_v):
    rows = pieces[0].shape[0]
    for i, piece in enumerate(pieces):
        rows_v[i * rows : (i + 1) * rows] = piece[...]


def widen(arrived, places, w4, b4, tiles_v, wide_v):
    tok_dev, c4 = arrived.shape[0], w4.shape[0]
    row_count = tok_dev // GRID_W
    me = lax.axis_index("rows")
    top = jnp.where(me > 0, 1.0, 0.0)
    bottom = jnp.where(me < lax.axis_size("rows") - 1, 1.0, 0.0)
    bias = b4[...]
    feat = c4

    base = 3 * tok_dev
    tiles_v[0:base] = matmul(places[0:base], arrived[:, 0:c4]).astype(BF16)
    tiles_v[base : base + 3 * GRID_W] = matmul(places[base : base + 3 * GRID_W], arrived[:, c4 : 2 * c4]).astype(BF16)
    base += 3 * GRID_W
    tiles_v[base : base + 3 * GRID_W] = matmul(places[base : base + 3 * GRID_W], arrived[:, 2 * c4 : 3 * c4]).astype(BF16)

    left = jnp.where(iota((GRID_W, 1), 0) == 0, 0.0, 1.0)
    right = jnp.where(iota((GRID_W, 1), 0) == GRID_W - 1, 0.0, 1.0)

    def fill(first, rows, tap, to, scale):
        size = rows * GRID_W
        for b in range(4):
            start = first + (0 if b == 3 else size)
            stop = first + (3 if b == 0 else 2) * size
            part = matmul(tiles_v[start:stop], w4[:, (tap * 4 + b) * feat : (tap * 4 + b + 1) * feat]) + bias
            if scale is not None:
                part = part * scale
            blocks = {0: ((1, None), (5, right)), 3: ((0, left), (4, None))}.get(b, ((b + 1, None),))
            for place, (block, edge) in enumerate(blocks):
                for i in range(rows):
                    piece = part[(place * rows + i) * GRID_W : (place * rows + i + 1) * GRID_W]
                    if edge is not None:
                        piece = piece * edge
                    wide_v[pl.ds(to(i) * GRID_W, GRID_W), block * feat : (block + 1) * feat] = piece.astype(BF16)

    for tap in range(4):
        fill(0, row_count, tap, lambda i, tap=tap: 4 * i + tap + 1, None)
    fill(3 * tok_dev, 1, 3, lambda i: 0, top)
    fill(3 * tok_dev + 3 * GRID_W, 1, 0, lambda i: 4 * row_count + 1, bottom)


def convolve(wide_v, wj, acc_v, out_v):
    feat = wj.shape[2]
    rows = out_v.shape[0]
    for b in range(4):
        total = None
        for row_tap in range(3):
            first = row_tap * GRID_W
            term = matmul(wide_v[first : first + rows * GRID_W, b * feat : (b + 3) * feat], wj[row_tap])
            total = term if total is None else total + term
        for r in range(rows):
            for block in range(feat // 128):
                acc_v[r, block, pl.ds(b, GRID_W, 4), :] = total[
                    r * GRID_W : (r + 1) * GRID_W, block * 128 : (block + 1) * 128
                ]
    for r in range(rows):
        for block in range(feat // 128):
            out_v[r, :, block * 128 : (block + 1) * 128] = acc_v[r, block].astype(BF16)


def rest_kernel(rows_joined, places, w2, b2, *refs):
    arrived, outs = refs[:-9], refs[-9:]
    joined, up_two, same, rows_v, acc_v, out_v, same_v, sems, end_sems = outs
    ends = [
        pltpu.make_async_copy(rows_joined, joined, end_sems.at[0]),
        pltpu.make_async_copy(same_v, same, end_sems.at[1]),
    ]
    ends[0].start()
    gather_rows(arrived, rows_v)
    tok_dev = rows_v.shape[0]
    c2 = w2.shape[0]
    row_count = tok_dev // GRID_W
    place = places[places.shape[0] - tok_dev :]
    same_v[...] = matmul(place, rows_v[:, c2:]).astype(BF16)
    ends[1].start()
    stores = [*ends]
    tile = matmul(place, rows_v[:, 0:c2]).astype(BF16)
    bias = b2[...]
    for a in range(2):
        for b in range(2):
            part = matmul(tile, w2[:, (a * 2 + b) * c2 : (a * 2 + b + 1) * c2]) + bias
            for i in range(row_count):
                for block in range(c2 // 128):
                    acc_v[2 * i + a, block, pl.ds(b, GRID_W, 2), :] = part[
                        i * GRID_W : (i + 1) * GRID_W, block * 128 : (block + 1) * 128
                    ]
        for i in range(row_count):
            r = 2 * i + a
            for block in range(c2 // 128):
                out_v[r, :, block * 128 : (block + 1) * 128] = acc_v[r, block].astype(BF16)
            store = pltpu.make_async_copy(out_v.at[r], up_two.at[r], sems.at[r])
            store.start()
            stores.append(store)
    for store in stores:
        store.wait()


def body(
    hidden_states,
    cell_of,
    proj_four_weight,
    proj_four_bias,
    proj_two_weight,
    proj_two_bias,
    proj_same_weight,
    proj_same_bias,
    up4_weight,
    up4_bias,
    up2_weight,
    up2_bias,
    join_weight,
):
    _, tok_dev, hid = hidden_states.shape
    shards = lax.axis_size("rows")
    per_peer = tok_dev // shards
    row_count = tok_dev // GRID_W
    c4, c2, cs = proj_four_weight.shape[1], proj_two_weight.shape[1], proj_same_weight.shape[1]
    feat = join_weight.shape[3]
    table = cell_of.reshape(shards, tok_dev)
    place_rows = 4 * tok_dev + 6 * GRID_W
    shape = jax.ShapeDtypeStruct

    low = low_part(shards)
    high = shards // low
    biases = [bias.reshape(1, -1) for bias in (proj_four_bias, proj_two_bias, proj_same_bias)]
    inputs = (
        hidden_states,
        table,
        proj_four_weight,
        biases[0],
        proj_two_weight,
        biases[1],
        proj_same_weight,
        biases[2],
    )
    four_shape = ((low + 2) * per_peer, c4)
    rest_shape = (high * per_peer, c2 + cs)
    places, *sent = pl.pallas_call(
        functools.partial(project_kernel, low),
        out_shape=(pltpu.VMEM((place_rows, tok_dev), BF16),)
        + (pltpu.VMEM(four_shape, BF16),) * high
        + (pltpu.VMEM(rest_shape, BF16),) * low,
        in_specs=[ANY] * 8,
        out_specs=(VMEM,) * (1 + high + low),
        scratch_shapes=[
            pltpu.VMEM(hidden_states.shape, BF16),
            pltpu.VMEM(table.shape, jnp.int32),
            pltpu.VMEM((hid, c4), BF16),
            pltpu.VMEM((hid, c2), BF16),
            pltpu.VMEM((cs // CHUNK, hid, CHUNK), BF16),
            pltpu.VMEM((1, c4), F32),
            pltpu.VMEM((1, c2), F32),
            pltpu.VMEM((1, cs), F32),
            pltpu.SemaphoreType.DMA((9 + cs // CHUNK,)),
        ],
        compiler_params=pltpu.CompilerParams(vmem_limit_bytes=10 << 20),
        cost_estimate=pl.CostEstimate(flops=2 * tok_dev * hid * (c4 + c2 + cs), bytes_accessed=5 << 20, transcendentals=0),
        name="project",
    )(*(in_hbm(x) for x in inputs))

    def swap(pieces, unit):
        moved = [pieces[0]]
        for step, piece in enumerate(pieces[1:], 1):
            moved.append(lax.ppermute(piece, "rows", [(i, i ^ (step * unit)) for i in range(shards)]))
        return moved

    def turn(kernel, pieces, out_shape, count, scratch=()):
        return pl.pallas_call(
            kernel,
            out_shape=(pltpu.VMEM(out_shape, BF16),) * count,
            in_specs=[VMEM] * len(pieces),
            out_specs=(VMEM,) * count,
            scratch_shapes=scratch,
            compiler_params=pltpu.CompilerParams(vmem_limit_bytes=4 << 20),
            cost_estimate=pl.CostEstimate(flops=1 << 26, bytes_accessed=1 << 20, transcendentals=0),
            name="turn",
        )(*pieces)

    rest = swap(sent[high:], 1)
    four = swap(sent[:high], low)
    rest = turn(functools.partial(turn_kernel, low), rest, (low * per_peer, c2 + cs), high)
    rest = swap(rest, low)
    four = turn(
        functools.partial(turn_four_kernel, low, per_peer),
        four,
        (high * per_peer, 3 * c4),
        low,
        [pltpu.VMEM((high * (low + 2) * per_peer, c4), BF16)],
    )
    four = swap(four, 1)

    weights = (
        up4_weight,
        up4_bias.reshape(1, -1),
        join_weight.reshape(3, 3 * c4, feat),
        up2_weight,
        up2_bias.reshape(1, -1),
    )
    w4, b4, wj, w2, b2 = pl.pallas_call(
        fetch_kernel,
        out_shape=tuple(pltpu.VMEM(w.shape, w.dtype) for w in weights),
        in_specs=[ANY] * 5,
        out_specs=(VMEM,) * 5,
        scratch_shapes=[pltpu.SemaphoreType.DMA((5,))],
        cost_estimate=pl.CostEstimate(flops=1 << 30, bytes_accessed=5 << 20, transcendentals=0),
        compiler_params=pltpu.CompilerParams(vmem_limit_bytes=8 << 20),
        name="fetch",
    )(*(in_hbm(w) for w in weights))

    out_rows = 4 * row_count
    join_shape = (out_rows, 4 * GRID_W, feat)
    rows_joined = pl.pallas_call(
        join_kernel,
        out_shape=pltpu.VMEM(join_shape, BF16),
        in_specs=[VMEM] * (4 + low),
        out_specs=VMEM,
        scratch_shapes=[
            pltpu.VMEM((tok_dev, 3 * c4), BF16),
            pltpu.VMEM((place_rows, c4), BF16),
            pltpu.VMEM(((out_rows + 2) * GRID_W, 6 * c4), BF16),
            pltpu.VMEM((out_rows, feat // 128, 4 * GRID_W, 128), F32),
        ],
        compiler_params=pltpu.CompilerParams(vmem_limit_bytes=20 << 20),
        cost_estimate=pl.CostEstimate(flops=4 << 30, bytes_accessed=4 << 20, transcendentals=0),
        name="join",
    )(places, w4, b4, wj, *four)
    joined, upsampled_two, same_scale = pl.pallas_call(
        rest_kernel,
        out_shape=(shape(join_shape, BF16), shape((2 * row_count, 2 * GRID_W, c2), BF16), shape((tok_dev, cs), BF16)),
        in_specs=[VMEM] * (4 + len(rest)),
        out_specs=(ANY, ANY, ANY),
        scratch_shapes=[
            pltpu.VMEM((tok_dev, c2 + cs), BF16),
            pltpu.VMEM((2 * row_count, c2 // 128, 2 * GRID_W, 128), F32),
            pltpu.VMEM((2 * row_count, 2 * GRID_W, c2), BF16),
            pltpu.VMEM((tok_dev, cs), BF16),
            pltpu.SemaphoreType.DMA((2 * row_count,)),
            pltpu.SemaphoreType.DMA((2,)),
        ],
        compiler_params=pltpu.CompilerParams(vmem_limit_bytes=12 << 20),
        cost_estimate=pl.CostEstimate(flops=2 << 30, bytes_accessed=4 << 20, transcendentals=0),
        name="rest",
    )(rows_joined, places, w2, b2, *rest)
    return (joined, upsampled_two, same_scale.reshape(row_count, GRID_W, cs))


def solution(mesh):
    return jax.shard_map(
        body,
        mesh=mesh,
        in_specs=(P(None, ("img", "rows"), None),) + (P(),) * 12,
        out_specs=(P(("img", "rows"), None, None),) * 3,
        check_vma=False,
    )
```

```python
import functools

import jax
import jax.numpy as jnp
from jax import lax
from jax.experimental import pallas as pl
from jax.experimental.pallas import tpu as pltpu
from jax.sharding import PartitionSpec as P


GRID_W = 64
CHUNK = 1024
F32 = jnp.float32
BF16 = jnp.bfloat16
ANY = pl.BlockSpec(memory_space=pl.ANY)
VMEM = pl.BlockSpec(memory_space=pltpu.VMEM)


def in_hbm(x):
    return pltpu.with_memory_space_constraint(x, pltpu.HBM)


def one_hot(mask):
    return jnp.where(mask, 1.0, 0.0).astype(BF16)


def iota(shape, dim):
    return lax.broadcasted_iota(jnp.int32, shape, dim)


def matmul(left, right):
    return jnp.dot(left, right, preferred_element_type=F32)


def column(row, size):
    same = iota((size, size), 0) == iota((size, size), 1)
    return jnp.sum(jnp.where(same, jnp.broadcast_to(row, (size, size)), 0.0), axis=1, keepdims=True)


def low_part(shards):
    return 1 << ((shards.bit_length()) // 2)


def landing(table, block, tok_dev, per_peer, seat):
    shards = table.shape[0]
    start = block * tok_dev
    inside = jnp.logical_and(table >= start, table < start + tok_dev)
    before = one_hot(iota((tok_dev, tok_dev), 0) < iota((tok_dev, tok_dev), 1))
    rank = matmul(one_hot(inside), before)
    place = (table - start).astype(F32)
    lane = iota((shards, tok_dev), 1)
    spread = jnp.zeros((shards, tok_dev), F32)
    for k in range(per_peer):
        hit = jnp.logical_and(inside, rank == float(k))
        found = jnp.sum(jnp.where(hit, place, 0.0), axis=1, keepdims=True)
        spread = spread + jnp.where(lax.rem(lane, per_peer) == k, found, 0.0)
    own = lax.div(lane, per_peer) == seat
    return jnp.sum(jnp.where(own, spread, 0.0), axis=0, keepdims=True).astype(jnp.int32)


def start_all(pairs, sems):
    copies = [pltpu.make_async_copy(src, dst, sems.at[i]) for i, (src, dst) in enumerate(pairs)]
    for copy in copies:
        copy.start()
    return copies


def project_kernel(low, hidden, table_hbm, w4, b4, w2, b2, ws, bs, places_v, *refs):
    high = (len(refs) - 9) - low
    sent_four, sent = refs[:high], refs[high : high + low]
    hidden_v, table_v, w4_v, w2_v, ws_v, b4_v, b2_v, bs_v, sems = refs[high + low :]
    chunks = ws.shape[1] // CHUNK
    copies = start_all(
        [
            (table_hbm, table_v),
            (hidden.at[0], hidden_v.at[0]),
            (b4, b4_v),
            (w4, w4_v),
            (hidden.at[1], hidden_v.at[1]),
            (b2, b2_v),
            (w2, w2_v),
            (hidden.at[2], hidden_v.at[2]),
            (bs, bs_v),
        ]
        + [(ws.at[:, pl.ds(i * CHUNK, CHUNK)], ws_v.at[i]) for i in range(chunks)],
        sems,
    )
    shards, tok_dev = table_v.shape
    per_peer = tok_dev // shards
    me = lax.axis_index("rows")
    copies[0].wait()
    table = table_v[...]
    mine = table_v[pl.ds(me, 1), :]
    block_row = lax.div(mine, tok_dev)
    block_col = column(block_row.astype(F32), tok_dev).astype(jnp.int32)
    square = (tok_dev, tok_dev)
    earlier = jnp.logical_and(block_col == jnp.broadcast_to(block_row, square), iota(square, 0) < iota(square, 1))
    within = jnp.sum(jnp.where(earlier, 1.0, 0.0), axis=0, keepdims=True).astype(jnp.int32)
    row = iota(square, 0)
    apart = jnp.bitwise_xor(block_row, me)
    order_low = one_hot(row == (lax.rem(apart, low) * high + lax.div(apart, low)) * per_peer + within)
    plane, unit = lax.div(block_row, low), lax.rem(block_row, low)
    my_plane = lax.div(me, low)

    def row_of(to_plane, to_unit):
        return (jnp.bitwise_xor(to_plane, my_plane) * (low + 2) + to_unit) * per_peer + within

    row = iota((high * (low + 2) * per_peer, tok_dev), 0)
    nowhere = jnp.full_like(unit, -1)
    here = row == row_of(plane, unit + 1)
    next_plane = row == jnp.where(unit == low - 1, row_of(plane + 1, 0), nowhere)
    last_plane = row == jnp.where(unit == 0, row_of(plane - 1, low + 1), nowhere)
    order_high = one_hot(jnp.logical_or(here, jnp.logical_or(next_plane, last_plane)))

    seat_low = jnp.bitwise_xor(iota((shards, tok_dev), 0), me)
    seat_high = lax.rem(seat_low, low) * high + lax.div(seat_low, low)
    own = landing(table, me, tok_dev, per_peer, seat_high)
    above = landing(table, me - 1, tok_dev, per_peer, seat_high)
    below = landing(table, me + 1, tok_dev, per_peer, seat_high)
    cell = iota(square, 0)
    col = lax.rem(cell, GRID_W)
    edge_col = iota((GRID_W, tok_dev), 0)
    base = 0
    for source, target, at in ((own, cell, col), (above, edge_col + (tok_dev - GRID_W), edge_col), (below, edge_col, edge_col)):
        size = target.shape[0]
        places_v[base : base + size] = one_hot(jnp.logical_and(target == source + 1, at != 0))
        places_v[base + size : base + 2 * size] = one_hot(target == source)
        places_v[base + 2 * size : base + 3 * size] = one_hot(jnp.logical_and(target == source - 1, at != GRID_W - 1))
        base += 3 * size
    places_v[base : base + tok_dev] = one_hot(cell == landing(table, me, tok_dev, per_peer, seat_low))

    c2 = w2_v.shape[1]
    for copy in copies[1:4]:
        copy.wait()
    four = (matmul(hidden_v[0], w4_v[...]) + b4_v[...]).astype(BF16)
    hand_out(matmul(order_high, four), sent_four, 0)
    copies[4].wait()
    rows_two = matmul(order_low, hidden_v[1]).astype(BF16)
    copies[5].wait()
    copies[6].wait()
    hand_out(matmul(rows_two, w2_v[...]) + b2_v[...], sent, 0)
    copies[7].wait()
    rows_same = matmul(order_low, hidden_v[2]).astype(BF16)
    copies[8].wait()
    for i in range(chunks):
        copies[9 + i].wait()
        same = matmul(rows_same, ws_v[i]) + bs_v[:, i * CHUNK : (i + 1) * CHUNK]
        hand_out(same, sent, c2 + i * CHUNK)


def hand_out(projected, sent, at):
    moved = projected.astype(BF16)
    rows = sent[0].shape[0]
    for k, out in enumerate(sent):
        out[:, at : at + moved.shape[1]] = moved[k * rows : (k + 1) * rows]


def turn_kernel(count, *refs):
    arrived, leaving = refs[:count], refs[count:]
    rows = arrived[0].shape[0] // len(leaving)
    for to, message in enumerate(leaving):
        for come, piece in enumerate(arrived):
            message[come * rows : (come + 1) * rows] = piece[to * rows : (to + 1) * rows]


def turn_four_kernel(low, per_peer, *refs):
    high = len(refs) - low - 1
    arrived, leaving, rows_v = refs[:high], refs[high:-1], refs[-1]
    mine = lax.rem(lax.axis_index("rows"), low)
    c4 = rows_v.shape[1]
    count = high * per_peer
    if per_peer % 8 == 0:
        for k, message in enumerate(leaving):
            unit = jnp.bitwise_xor(mine, k)
            for h, piece in enumerate(arrived):
                for place, step in enumerate((1, 0, 2)):
                    first = pl.multiple_of((unit + step) * per_peer, per_peer)
                    message[h * per_peer : (h + 1) * per_peer, place * c4 : (place + 1) * c4] = piece[
                        pl.ds(first, per_peer), :
                    ]
        return
    gather_rows(arrived, rows_v)
    total = rows_v.shape[0]
    to = iota((low * count, total), 0)
    h = lax.rem(lax.div(to, per_peer), high)
    unit = jnp.bitwise_xor(lax.div(to, count), mine)
    for place, step in enumerate((1, 0, 2)):
        source = (h * (low + 2) + unit + step) * per_peer + lax.rem(to, per_peer)
        moved = matmul(one_hot(iota(to.shape, 1) == source), rows_v[...]).astype(BF16)
        for k, message in enumerate(leaving):
            message[:, place * c4 : (place + 1) * c4] = moved[k * count : (k + 1) * count]


def fetch_kernel(*refs):
    count = len(refs) // 2
    for copy in start_all(list(zip(refs[:count], refs[count:-1])), refs[-1]):
        copy.wait()


def join_kernel(places, w4, b4, wj, *refs):
    pieces, (joined, rows_v, tiles_v, wide_v, acc_v) = refs[:-5], refs[-5:]
    gather_rows(pieces, rows_v)
    widen(rows_v, places, w4, b4, tiles_v, wide_v)
    convolve(wide_v, wj, acc_v, joined)


def gather_rows(pieces, rows_v):
    rows = pieces[0].shape[0]
    for i, piece in enumerate(pieces):
        rows_v[i * rows : (i + 1) * rows] = piece[...]


def widen(arrived, places, w4, b4, tiles_v, wide_v):
    tok_dev, c4 = arrived.shape[0], w4.shape[0]
    row_count = tok_dev // GRID_W
    me = lax.axis_index("rows")
    top = jnp.where(me > 0, 1.0, 0.0)
    bottom = jnp.where(me < lax.axis_size("rows") - 1, 1.0, 0.0)
    bias = b4[...]
    feat = c4

    base = 3 * tok_dev
    tiles_v[0:base] = matmul(places[0:base], arrived[:, 0:c4]).astype(BF16)
    tiles_v[base : base + 3 * GRID_W] = matmul(places[base : base + 3 * GRID_W], arrived[:, c4 : 2 * c4]).astype(BF16)
    base += 3 * GRID_W
    tiles_v[base : base + 3 * GRID_W] = matmul(places[base : base + 3 * GRID_W], arrived[:, 2 * c4 : 3 * c4]).astype(BF16)

    left = jnp.where(iota((GRID_W, 1), 0) == 0, 0.0, 1.0)
    right = jnp.where(iota((GRID_W, 1), 0) == GRID_W - 1, 0.0, 1.0)

    def fill(first, rows, tap, to, scale):
        size = rows * GRID_W
        for b in range(4):
            start = first + (0 if b == 3 else size)
            stop = first + (3 if b == 0 else 2) * size
            part = matmul(tiles_v[start:stop], w4[:, (tap * 4 + b) * feat : (tap * 4 + b + 1) * feat]) + bias
            if scale is not None:
                part = part * scale
            blocks = {0: ((1, None), (5, right)), 3: ((0, left), (4, None))}.get(b, ((b + 1, None),))
            for place, (block, edge) in enumerate(blocks):
                for i in range(rows):
                    piece = part[(place * rows + i) * GRID_W : (place * rows + i + 1) * GRID_W]
                    if edge is not None:
                        piece = piece * edge
                    wide_v[pl.ds(to(i) * GRID_W, GRID_W), block * feat : (block + 1) * feat] = piece.astype(BF16)

    for tap in range(4):
        fill(0, row_count, tap, lambda i, tap=tap: 4 * i + tap + 1, None)
    fill(3 * tok_dev, 1, 3, lambda i: 0, top)
    fill(3 * tok_dev + 3 * GRID_W, 1, 0, lambda i: 4 * row_count + 1, bottom)


def convolve(wide_v, wj, acc_v, out_v):
    feat = wj.shape[2]
    rows = out_v.shape[0]
    for b in range(4):
        total = None
        for row_tap in range(3):
            first = row_tap * GRID_W
            term = matmul(wide_v[first : first + rows * GRID_W, b * feat : (b + 3) * feat], wj[row_tap])
            total = term if total is None else total + term
        for r in range(rows):
            for block in range(feat // 128):
                acc_v[r, block, pl.ds(b, GRID_W, 4), :] = total[
                    r * GRID_W : (r + 1) * GRID_W, block * 128 : (block + 1) * 128
                ]
    for r in range(rows):
        for block in range(feat // 128):
            out_v[r, :, block * 128 : (block + 1) * 128] = acc_v[r, block].astype(BF16)


def rest_kernel(rows_joined, places, w2, b2, *refs):
    arrived, outs = refs[:-9], refs[-9:]
    joined, up_two, same, rows_v, acc_v, out_v, same_v, sems, end_sems = outs
    ends = [
        pltpu.make_async_copy(rows_joined, joined, end_sems.at[0]),
        pltpu.make_async_copy(same_v, same, end_sems.at[1]),
    ]
    ends[0].start()
    gather_rows(arrived, rows_v)
    tok_dev = rows_v.shape[0]
    c2 = w2.shape[0]
    row_count = tok_dev // GRID_W
    place = places[places.shape[0] - tok_dev :]
    placed = matmul(place, rows_v[...]).astype(BF16)
    same_v[...] = placed[:, c2:]
    ends[1].start()
    stores = [*ends]
    tile = placed[:, 0:c2]
    bias = b2[...]
    for a in range(2):
        for b in range(2):
            part = matmul(tile, w2[:, (a * 2 + b) * c2 : (a * 2 + b + 1) * c2]) + bias
            for i in range(row_count):
                for block in range(c2 // 128):
                    acc_v[2 * i + a, block, pl.ds(b, GRID_W, 2), :] = part[
                        i * GRID_W : (i + 1) * GRID_W, block * 128 : (block + 1) * 128
                    ]
        for i in range(row_count):
            r = 2 * i + a
            for block in range(c2 // 128):
                out_v[r, :, block * 128 : (block + 1) * 128] = acc_v[r, block].astype(BF16)
            store = pltpu.make_async_copy(out_v.at[r], up_two.at[r], sems.at[r])
            store.start()
            stores.append(store)
    for store in stores:
        store.wait()


def body(
    hidden_states,
    cell_of,
    proj_four_weight,
    proj_four_bias,
    proj_two_weight,
    proj_two_bias,
    proj_same_weight,
    proj_same_bias,
    up4_weight,
    up4_bias,
    up2_weight,
    up2_bias,
    join_weight,
):
    _, tok_dev, hid = hidden_states.shape
    shards = lax.axis_size("rows")
    per_peer = tok_dev // shards
    row_count = tok_dev // GRID_W
    c4, c2, cs = proj_four_weight.shape[1], proj_two_weight.shape[1], proj_same_weight.shape[1]
    feat = join_weight.shape[3]
    table = cell_of.reshape(shards, tok_dev)
    place_rows = 4 * tok_dev + 6 * GRID_W
    shape = jax.ShapeDtypeStruct

    low = low_part(shards)
    high = shards // low
    biases = [bias.reshape(1, -1) for bias in (proj_four_bias, proj_two_bias, proj_same_bias)]
    inputs = (
        hidden_states,
        table,
        proj_four_weight,
        biases[0],
        proj_two_weight,
        biases[1],
        proj_same_weight,
        biases[2],
    )
    four_shape = ((low + 2) * per_peer, c4)
    rest_shape = (high * per_peer, c2 + cs)
    places, *sent = pl.pallas_call(
        functools.partial(project_kernel, low),
        out_shape=(pltpu.VMEM((place_rows, tok_dev), BF16),)
        + (pltpu.VMEM(four_shape, BF16),) * high
        + (pltpu.VMEM(rest_shape, BF16),) * low,
        in_specs=[ANY] * 8,
        out_specs=(VMEM,) * (1 + high + low),
        scratch_shapes=[
            pltpu.VMEM(hidden_states.shape, BF16),
            pltpu.VMEM(table.shape, jnp.int32),
            pltpu.VMEM((hid, c4), BF16),
            pltpu.VMEM((hid, c2), BF16),
            pltpu.VMEM((cs // CHUNK, hid, CHUNK), BF16),
            pltpu.VMEM((1, c4), F32),
            pltpu.VMEM((1, c2), F32),
            pltpu.VMEM((1, cs), F32),
            pltpu.SemaphoreType.DMA((9 + cs // CHUNK,)),
        ],
        compiler_params=pltpu.CompilerParams(vmem_limit_bytes=10 << 20),
        cost_estimate=pl.CostEstimate(flops=2 * tok_dev * hid * (c4 + c2 + cs), bytes_accessed=5 << 20, transcendentals=0),
        name="project",
    )(*(in_hbm(x) for x in inputs))

    def swap(pieces, unit):
        moved = [pieces[0]]
        for step, piece in enumerate(pieces[1:], 1):
            moved.append(lax.ppermute(piece, "rows", [(i, i ^ (step * unit)) for i in range(shards)]))
        return moved

    def turn(kernel, pieces, out_shape, count, scratch=()):
        return pl.pallas_call(
            kernel,
            out_shape=(pltpu.VMEM(out_shape, BF16),) * count,
            in_specs=[VMEM] * len(pieces),
            out_specs=(VMEM,) * count,
            scratch_shapes=scratch,
            compiler_params=pltpu.CompilerParams(vmem_limit_bytes=4 << 20),
            cost_estimate=pl.CostEstimate(flops=1 << 26, bytes_accessed=1 << 20, transcendentals=0),
            name="turn",
        )(*pieces)

    rest = swap(sent[high:], 1)
    four = swap(sent[:high], low)
    rest = turn(functools.partial(turn_kernel, low), rest, (low * per_peer, c2 + cs), high)
    rest = swap(rest, low)
    four = turn(
        functools.partial(turn_four_kernel, low, per_peer),
        four,
        (high * per_peer, 3 * c4),
        low,
        [pltpu.VMEM((high * (low + 2) * per_peer, c4), BF16)],
    )
    four = swap(four, 1)

    weights = (
        up4_weight,
        up4_bias.reshape(1, -1),
        join_weight.reshape(3, 3 * c4, feat),
        up2_weight,
        up2_bias.reshape(1, -1),
    )
    w4, b4, wj, w2, b2 = pl.pallas_call(
        fetch_kernel,
        out_shape=tuple(pltpu.VMEM(w.shape, w.dtype) for w in weights),
        in_specs=[ANY] * 5,
        out_specs=(VMEM,) * 5,
        scratch_shapes=[pltpu.SemaphoreType.DMA((5,))],
        cost_estimate=pl.CostEstimate(flops=1 << 30, bytes_accessed=5 << 20, transcendentals=0),
        compiler_params=pltpu.CompilerParams(vmem_limit_bytes=8 << 20),
        name="fetch",
    )(*(in_hbm(w) for w in weights))

    out_rows = 4 * row_count
    join_shape = (out_rows, 4 * GRID_W, feat)
    rows_joined = pl.pallas_call(
        join_kernel,
        out_shape=pltpu.VMEM(join_shape, BF16),
        in_specs=[VMEM] * (4 + low),
        out_specs=VMEM,
        scratch_shapes=[
            pltpu.VMEM((tok_dev, 3 * c4), BF16),
            pltpu.VMEM((place_rows, c4), BF16),
            pltpu.VMEM(((out_rows + 2) * GRID_W, 6 * c4), BF16),
            pltpu.VMEM((out_rows, feat // 128, 4 * GRID_W, 128), F32),
        ],
        compiler_params=pltpu.CompilerParams(vmem_limit_bytes=20 << 20),
        cost_estimate=pl.CostEstimate(flops=4 << 30, bytes_accessed=4 << 20, transcendentals=0),
        name="join",
    )(places, w4, b4, wj, *four)
    joined, upsampled_two, same_scale = pl.pallas_call(
        rest_kernel,
        out_shape=(shape(join_shape, BF16), shape((2 * row_count, 2 * GRID_W, c2), BF16), shape((tok_dev, cs), BF16)),
        in_specs=[VMEM] * (4 + len(rest)),
        out_specs=(ANY, ANY, ANY),
        scratch_shapes=[
            pltpu.VMEM((tok_dev, c2 + cs), BF16),
            pltpu.VMEM((2 * row_count, c2 // 128, 2 * GRID_W, 128), F32),
            pltpu.VMEM((2 * row_count, 2 * GRID_W, c2), BF16),
            pltpu.VMEM((tok_dev, cs), BF16),
            pltpu.SemaphoreType.DMA((2 * row_count,)),
            pltpu.SemaphoreType.DMA((2,)),
        ],
        compiler_params=pltpu.CompilerParams(vmem_limit_bytes=12 << 20),
        cost_estimate=pl.CostEstimate(flops=2 << 30, bytes_accessed=4 << 20, transcendentals=0),
        name="rest",
    )(rows_joined, places, w2, b2, *rest)
    return (joined, upsampled_two, same_scale.reshape(row_count, GRID_W, cs))


def solution(mesh):
    return jax.shard_map(
        body,
        mesh=mesh,
        in_specs=(P(None, ("img", "rows"), None),) + (P(),) * 12,
        out_specs=(P(("img", "rows"), None, None),) * 3,
        check_vma=False,
    )
```
